32 devices in a mesh: slab: 8 (over z, x), tile: 4 (over y, core).
Axes of the slice: x: 2, y: 2, z: 4, core: 2. Of those that a mesh axis runs over, the one named last changes fastest.
Arguments:
- tiles: bfloat16 [32, 20, 256, 128], P(('slab', 'tile')), may hold values from -6 to 6
- offsets: int32 [32, 2], replicated, may hold values from -3 to 690, as said below
- fracs: int32 [32, 3], replicated, may hold values from 0 to 15
Outputs:
- joined: bfloat16 [128, 946, 128], P(('slab', 'tile'))
The draws below stay inside these ranges and needn't reach their ends.
Inputs may be any that keep to these rules, and one draw needn't show every extreme that they name: offsets[g, 0] lies within 1 of (g // 4) * 16 - 2, and offsets[g, 1] within 4 of (g % 4) * 230, clipped to 0 .. 690; some tile reaches each end of the plane shift.
All inputs are finite; a program needn't handle non-finite values.
Results may differ from the reference program's by a relative error of at most 0.0038.
Values may be sent and summed in bfloat16 or wider, within the bound.
A program may use at most 64 MiB of HBM per device.

```python
import jax
import jax.numpy as jnp
from jax import lax

GROUPZ = 16
MARGIN = 2
JIT = 1
TY = 256
TX = 128
STEPY = 230
JITY = 4
RY = 26
RX = 16
QUANT = 16
TZ = 20
TILES_GROUP = 4
TILES = 32
MY = 946
NZ = 128


def draw_offsets(key, part):
    key_plane = jax.random.fold_in(key, 11)
    key_row = jax.random.fold_in(key, 12)
    key_lowest = jax.random.fold_in(key, 13)
    key_highest = jax.random.fold_in(key, 14)
    position = jnp.arange(TILES, dtype=jnp.int32)
    group_of = position // TILES_GROUP
    within = position % TILES_GROUP
    shift_plane = jax.random.randint(key_plane, (TILES,), -JIT, JIT + 1)
    lowest_tile = jax.random.randint(key_lowest, (), 0, TILES)
    highest_tile = (lowest_tile + 1 + jax.random.randint(key_highest, (), 0, TILES - 1)) % TILES
    shift_plane = jnp.where(position == lowest_tile, -JIT, shift_plane)
    shift_plane = jnp.where(position == highest_tile, JIT, shift_plane)
    first_plane = group_of * GROUPZ - MARGIN + shift_plane
    shift_row = jax.random.randint(key_row, (TILES,), -JITY, JITY + 1)
    first_row = jnp.clip(within * STEPY + shift_row, 0, MY - TY)
    return jnp.stack([first_plane, first_row], axis=1).astype(jnp.int32)


def set_ends(drawn, key, low, largest):
    shape = drawn.shape
    index_at = [jax.random.randint(jax.random.fold_in(key, axis), (), 0, shape[axis]) for axis in range(len(shape))]
    drawn = drawn.at[tuple(index_at)].set(low)
    longest = shape.index(max(shape))
    index_at[longest] = (index_at[longest] + 1) % shape[longest]
    return drawn.at[tuple(index_at)].set(largest)


def levels(key, shape, pieces, least, top_value):
    def one(dim, shards_of):
        draws = jax.random.uniform(jax.random.fold_in(jax.random.fold_in(key, 6), dim), (shards_of,), jnp.float32, least / len(pieces), top_value / len(pieces))
        return jnp.repeat(jnp.exp(draws), shape[dim] // shards_of).reshape((-1,) + (1,) * (len(shape) - dim - 1))

    level = one(*pieces[0])
    for cut in pieces[1:]:
        level = level * one(*cut)
    return level


def centred(own_key, shape, scale, most, shards=(), held_as=jnp.bfloat16):
    entries = scale * jax.random.normal(own_key, shape, jnp.float32)
    if shards:
        entries = entries * levels(own_key, shape, shards, -0.22, 0.18)
    return jnp.clip(entries, -most, most).astype(held_as)


def setup_inputs(seed: int = 0) -> dict:
    splits = jax.random.split(jax.random.key(seed), 4)
    tiles = centred(splits[0], (TILES, TZ, TY, TX), 1.0, 6.0, ((0, 32),))
    offsets = draw_offsets(jax.random.fold_in(splits[3], 71), 0)
    fracs = set_ends(jax.random.randint(splits[2], (TILES, 3), 0, QUANT), jax.random.fold_in(splits[2], 1), 0, QUANT - 1).astype(jnp.int32)
    return {"tiles": tiles, "offsets": offsets, "fracs": fracs}


weight_floor = 0.05


def ramp(length, ramp_width):
    position = jnp.arange(length, dtype=jnp.float32)
    rising = 0.5 - 0.5 * jnp.cos(jnp.pi * (position + 1.0) / (ramp_width + 1.0))
    rising = jnp.where(position < ramp_width, rising, jnp.ones_like(rising))
    return jnp.minimum(rising, rising[::-1])


def resample(raw_tile, fraction_row):
    volume_field = raw_tile.astype(jnp.float32)
    for direction in range(3):
        fraction = fraction_row[direction].astype(jnp.float32) / QUANT
        extent = volume_field.shape[direction]
        shifted = jnp.concatenate([lax.slice_in_dim(volume_field, 1, extent, axis=direction), jnp.zeros_like(lax.slice_in_dim(volume_field, 0, 1, axis=direction))], axis=direction)
        volume_field = (1.0 - fraction) * volume_field + fraction * shifted
    return volume_field


def reference(tiles, offsets, fracs):
    ramp_z = ramp(TZ, 2 * MARGIN)
    ramp_y = ramp(TY, RY)
    ramp_x = ramp(TX, RX)
    weight = ramp_z[:, None, None] * ramp_y[None, :, None] * ramp_x[None, None, :]
    border = MARGIN + JIT
    numer_init = jnp.zeros((NZ + 2 * border, MY, TX), jnp.float32)
    weight_init = jnp.zeros((NZ + 2 * border, MY, TX), jnp.float32)

    def place(totals, element):
        numer, weight_sum = totals
        one_tile, corner, fraction_row = element
        blended = (resample(one_tile, fraction_row) * weight).astype(jnp.bfloat16)
        start_at = ((corner[0] + border).astype(jnp.int32), corner[1].astype(jnp.int32), jnp.zeros((), jnp.int32))
        current = lax.dynamic_slice(numer, start_at, (TZ, TY, TX))
        numer = lax.dynamic_update_slice(numer, current + blended.astype(jnp.float32), start_at)
        current = lax.dynamic_slice(weight_sum, start_at, (TZ, TY, TX))
        weight_sum = lax.dynamic_update_slice(weight_sum, current + weight, start_at)
        return (numer, weight_sum), None

    (numer, weight_sum), _ = lax.scan(place, (numer_init, weight_init), (tiles, offsets, fracs))
    numer = numer[border:border + NZ]
    weight_sum = weight_sum[border:border + NZ]
    return (numer / jnp.maximum(weight_sum, weight_floor)).astype(jnp.bfloat16)
```

```python
import functools

import jax
import jax.numpy as jnp
import numpy as np
from jax import lax
from jax.experimental import pallas as pl
from jax.experimental.pallas import tpu as pltpu
from jax.sharding import PartitionSpec as P

GROUPZ = 16
MARGIN = 2
JIT = 1
STEPY = 230
JITY = 4
RY = 26
RX = 16
QUANT = 16
EDGE = MARGIN + JIT
PADY = 32
PADZ = 24
PIECES = 4

weight_floor = 0.05
MESH = pl.DeviceIdType.MESH


def ramp(length, ramp_width):
    position = np.arange(length, dtype=np.float64)
    rising = 0.5 - 0.5 * np.cos(np.pi * (position + 1.0) / (ramp_width + 1.0))
    rising = np.where(position < ramp_width, rising, 1.0)
    return np.minimum(rising, rising[::-1])


def round_up(value, step):
    return -(-value // step) * step


SOLO = STEPY // 8 * 8
PIECE = SOLO // PIECES


def pair_start(pair):
    if isinstance(pair, int):
        return max(2 * pair * STEPY - JITY, 0) // 8 * 8
    return jnp.maximum(2 * pair * STEPY - JITY, 0) // 8 * 8


def frame_start(rank):
    return pair_start(rank // 2) + SOLO * (rank % 2)


def kernel(
    groups, n, per, depth, tile_rows, shared,
    offs_ref, fracs_ref, rampz_ref, table_ref, tile_ref, out_ref,
    head, raw, coef, wa, wb, blend, blend_sh, own_sh, give, got,
    edge_send, edge_send_sh, edge_recv, edge_recv_sh, recv, recv_sh, rec,
    offs, fracs, rampz, table,
    small_sem, load_sem, give_sem, got_sem, es_sem, er_sem, s_sem, r_sem, above_sem,
):
    g = lax.axis_index("slab")
    r = lax.axis_index("tile")
    me = g * n + r
    low = r < n // 2
    odd = r % 2 == 1
    partner = r + 1 - 2 * (r % 2)
    cols = raw.shape[2]
    last = n - 1
    frame = SOLO + 2 * shared
    rows = out_ref.shape[0]

    barrier = pltpu.get_barrier_semaphore()
    has_below = g > 0
    has_above = g < groups - 1
    for i in range(1, n):
        pl.semaphore_signal(
            barrier, inc=1, device_id=(g, lax.rem(r + i, n)), device_id_type=MESH
        )

    @pl.when(has_above)
    def _():
        pl.semaphore_signal(barrier, inc=1, device_id=(g + 1, r), device_id_type=MESH)

    far_side = jnp.where(low, 1, 0)
    near_side = 1 - far_side

    def sends_to(side):
        return jnp.where(side == 0, g < groups - 1, g > 0)

    def gets_from(side):
        return jnp.where(side == 0, g > 0, g < groups - 1)

    gets_far = gets_from(far_side)
    gets_near = gets_from(near_side)

    def mirrored(owner):
        return jnp.where(low, owner, last - owner)

    edge_planes = list(range(EDGE)) + list(range(GROUPZ - EDGE, GROUPZ))
    bound = sorted({q // per for q in edge_planes}, reverse=True)
    free = [o for o in range(last, -1, -1) if o not in bound]
    far_free = [o for o in free if o >= n // 2]
    far_bound = [o for o in bound if o >= n // 2]
    near_free = [o for o in free if o < n // 2]
    near_bound = [o for o in bound if o < n // 2]
    far_list = far_free + far_bound

    def far_owner(i):
        return mirrored(jnp.where(gets_far, far_list[i], far_list[-1 - i]))

    smalls = [
        pltpu.make_async_copy(source, target, small_sem.at[i])
        for i, (source, target) in enumerate(
            [(offs_ref, offs), (fracs_ref, fracs), (rampz_ref, rampz), (table_ref, table)]
        )
    ]
    for small in smalls:
        small.start()
    first_owner = far_owner(0)
    head_planes = head.shape[0]
    head_start = jnp.minimum(first_owner * per + MARGIN - JIT, depth - head_planes)
    head_load = pltpu.make_async_copy(
        tile_ref.at[0, pl.ds(head_start, head_planes)], head, load_sem.at[0]
    )
    head_load.start()
    load = pltpu.make_async_copy(tile_ref.at[0], raw.at[pl.ds(0, depth)], load_sem.at[1])
    load.start()
    raw[depth] = jnp.zeros(raw.shape[1:], raw.dtype)

    def rampz_at(z):
        return rampz[jnp.clip(z + PADZ, 0, rampz.shape[0] - 1)]

    smalls[0].wait()
    smalls[1].wait()
    corner = offs[0, me]
    shift = jnp.clip(offs[1, me] - frame_start(r), 0, frame - tile_rows)
    base = g * GROUPZ - corner
    fz = fracs[0, me].astype(jnp.float32) / QUANT
    fy = fracs[1, me].astype(jnp.float32) / QUANT
    fx = fracs[2, me].astype(jnp.float32) / QUANT
    start_solo = jnp.where(odd, 2 * shared, 0)
    start_own = jnp.where(odd, shared, SOLO)
    start_give = jnp.where(odd, 0, SOLO + shared)
    parts = [(0, SOLO, start_solo), (SOLO, shared, start_own), (SOLO + shared, shared, start_give)]
    for at, count, start in parts:
        row = lax.broadcasted_iota(jnp.int32, (count, tile_rows), 0)
        col = lax.broadcasted_iota(jnp.int32, (count, tile_rows), 1)
        behind = col - row + (shift - start)
        lerp_y = jnp.where(behind == 0, 1.0 - fy, jnp.where(behind == 1, fy, 0.0))
        coef[at : at + count, :tile_rows] = ((1.0 - fz) * lerp_y).astype(jnp.bfloat16)
        coef[at : at + count, tile_rows:] = (fz * lerp_y).astype(jnp.bfloat16)
    smalls[2].wait()
    smalls[3].wait()
    for at, count, start in parts:
        weight = table[pl.ds(PADY + start - shift, count), :]
        lane = lax.broadcasted_iota(jnp.int32, (count, cols), 1)
        wa[at : at + count] = weight * (1.0 - fx)
        wb[at : at + count] = jnp.where(lane < cols - 1, weight * fx, 0.0)

    def planes(store, source, source_start, limit, first, count, lo, hi):
        at = [jnp.clip(first + j, 0, depth - 1) - source_start for j in range(count)]
        at = [jnp.clip(z, 0, limit) for z in at]
        top = jnp.concatenate([source[z] for z in at], axis=1)
        bottom = jnp.concatenate([source[z + 1] for z in at], axis=1)
        mixed = jnp.dot(
            coef[lo:hi], jnp.concatenate([top, bottom], axis=0),
            preferred_element_type=jnp.float32,
        )
        for j in range(count):
            part = mixed[:, j * cols : (j + 1) * cols]
            value = part * wa[lo:hi] + pltpu.roll(part, cols - 1, 1) * wb[lo:hi]
            store(j, value * rampz_at(first + j))

    def blend_rows(to_solo, slot, source, source_start, limit, first, count, lo, hi):
        def store(j, value):
            top = min(hi, SOLO)
            if lo < top:
                to_solo(j, lo, top, value[: top - lo].astype(jnp.bfloat16))
            if hi > SOLO:
                own_sh[slot + j] = value[SOLO - lo : SOLO + shared - lo]
                give[slot + j] = value[SOLO + shared - lo :].astype(jnp.bfloat16)

        planes(store, source, source_start, limit, first, count, lo, hi)

    def blend_owner(owner, lo=0, hi=frame, from_head=False):
        def to_solo(j, a, b, value):
            blend[owner, j, a:b] = value

        first = base + owner * per
        if from_head:
            blend_rows(
                to_solo, owner * per, head, head_start, head_planes - 2, first, per, lo, hi
            )
        else:
            blend_rows(to_solo, owner * per, raw, 0, depth - 1, first, per, lo, hi)

    def edge_slot(side):
        return GROUPZ + side * EDGE

    def blend_edge(side):
        def to_solo(j, a, b, value):
            edge_send[side, j, a:b] = value

        first = base + jnp.where(side == 0, GROUPZ, -EDGE)
        blend_rows(to_solo, edge_slot(side), raw, 0, depth - 1, first, EDGE, 0, frame)

    def swap_copy(at, slot, count):
        part = pl.ds(slot, count)
        return pltpu.make_async_remote_copy(
            src_ref=give.at[part], dst_ref=got.at[part],
            send_sem=give_sem.at[at], recv_sem=got_sem.at[at],
            device_id=(g, partner), device_id_type=MESH,
        )

    def swap_owner(owner):
        return swap_copy(owner, owner * per, per)

    def swap_edge(side):
        return swap_copy(n + side, edge_slot(side), EDGE)

    def join_owner(owner):
        swap_owner(owner).wait_recv()
        for j in range(per):
            slot = owner * per + j
            blend_sh[owner, j] = (own_sh[slot] + got[slot].astype(jnp.float32)).astype(jnp.bfloat16)

    def join_edge(side):
        swap_edge(side).wait_recv()
        for p in range(EDGE):
            slot = edge_slot(side) + p
            edge_send_sh[side, p] = (own_sh[slot] + got[slot].astype(jnp.float32)).astype(
                jnp.bfloat16
            )

    def of(solo, sh, at, i):
        if i == PIECES:
            return sh.at[at]
        return solo.at[at, :, pl.ds(i * PIECE, PIECE)]

    def owner_copy(owner, source, i):
        return pltpu.make_async_remote_copy(
            src_ref=of(blend, blend_sh, owner, i), dst_ref=of(recv, recv_sh, source, i),
            send_sem=s_sem.at[owner, i], recv_sem=r_sem.at[source, i],
            device_id=(g, owner), device_id_type=MESH,
        )

    def own_copy(i):
        return pltpu.make_async_copy(
            of(blend, blend_sh, r, i), of(recv, recv_sh, r, i), r_sem.at[r, i]
        )

    def send(owner, i, when=True):
        @pl.when(jnp.logical_and(when, owner != r))
        def _():
            owner_copy(owner, r, i).start()

        @pl.when(jnp.logical_and(when, owner == r))
        def _():
            own_copy(i).start()

    def edge_copy(side, i):
        return pltpu.make_async_remote_copy(
            src_ref=of(edge_send, edge_send_sh, side, i),
            dst_ref=of(edge_recv, edge_recv_sh, side, i),
            send_sem=es_sem.at[side, i], recv_sem=er_sem.at[side, i],
            device_id=(g + 1 - 2 * side, r), device_id_type=MESH,
        )

    def send_edge(side, i):
        @pl.when(sends_to(side))
        def _():
            edge_copy(side, i).start()

    def add_edge(side, i):
        edge_copy(side, i).wait_recv()
        for p in range(EDGE):
            q = p + jnp.where(side == 0, 0, GROUPZ - EDGE)
            owner, j = q // per, q % per
            if i == PIECES:
                blend_sh[owner, j] = (
                    blend_sh[owner, j].astype(jnp.float32)
                    + edge_recv_sh[side, p].astype(jnp.float32)
                ).astype(jnp.bfloat16)
            else:
                a, b = i * PIECE, (i + 1) * PIECE
                blend[owner, j, a:b] = (
                    blend[owner, j, a:b].astype(jnp.float32)
                    + edge_recv[side, p, a:b].astype(jnp.float32)
                ).astype(jnp.bfloat16)

    head_load.wait()
    blend_owner(first_owner, 0, PIECE, True)
    pl.semaphore_wait(barrier, n - 1 + jnp.where(has_below, 1, 0))
    first_free = len(far_free) > 0
    first_when = True if first_free else jnp.logical_not(gets_far)
    send(first_owner, 0, first_when)

    @pl.when(has_below)
    def _():
        pl.semaphore_signal(above_sem, inc=1, device_id=(g - 1, r), device_id_type=MESH)

    blend_owner(first_owner, PIECE, frame, True)
    for i in range(1, PIECES):
        send(first_owner, i, first_when)
    swap_owner(first_owner).start()

    load.wait()
    blend_edge(far_side)

    @pl.when(jnp.logical_and(has_above, jnp.logical_not(low)))
    def _():
        pl.semaphore_wait(above_sem, 1)

    for i in range(PIECES):
        send_edge(far_side, i)
    swap_edge(far_side).start()

    for at in range(1, len(far_list)):
        owner = far_owner(at)
        blend_owner(owner)
        for i in range(PIECES):
            send(owner, i, True if at < len(far_free) else jnp.logical_not(gets_far))
        swap_owner(owner).start()
    join_edge(far_side)
    send_edge(far_side, PIECES)
    for at in range(len(far_list)):
        owner = far_owner(at)
        join_owner(owner)
        send(owner, PIECES, True if at < len(far_free) else jnp.logical_not(gets_far))

    blend_edge(near_side)

    @pl.when(jnp.logical_and(has_above, low))
    def _():
        pl.semaphore_wait(above_sem, 1)

    for i in range(PIECES):
        send_edge(near_side, i)
    swap_edge(near_side).start()
    for o in near_free + near_bound:
        owner = mirrored(o)
        blend_owner(owner)
        for i in range(PIECES):
            send(owner, i, True if o in near_free else jnp.logical_not(gets_near))
        swap_owner(owner).start()
    join_edge(near_side)
    send_edge(near_side, PIECES)
    for o in near_free + near_bound:
        owner = mirrored(o)
        join_owner(owner)
        send(owner, PIECES, True if o in near_free else jnp.logical_not(gets_near))

    rec[...] = jnp.zeros_like(rec)
    for k in range(n):
        s = frame_start(k)
        totals = [0.0] * per
        for delta in (-1, 0, 1):
            group = jnp.clip(g + delta, 0, groups - 1)
            exists = jnp.where(group == g + delta, 1.0, 0.0)
            z0 = offs[0, group * n + k]
            ahead = jnp.clip(offs[1, group * n + k] - s, 0, frame - tile_rows)
            wy = table[pl.ds(PADY - ahead, frame), :]
            for j in range(per):
                z = g * GROUPZ + r * per + j - z0
                totals[j] = totals[j] + wy * (rampz_at(z) * exists)
        for j in range(per):
            rec[j, s : s + frame] = rec[j, s : s + frame] + totals[j]
    rec[...] = 1.0 / jnp.maximum(rec[...], weight_floor)

    @pl.when(gets_far)
    def _():
        for i in range(PIECES + 1):
            add_edge(far_side, i)
            for o in far_bound:
                send(mirrored(o), i)

    @pl.when(gets_near)
    def _():
        for i in range(PIECES + 1):
            add_edge(near_side, i)
            for o in near_bound:
                send(mirrored(o), i)

    def span(k, i):
        at = pair_start(k // 2) + (k % 2) * (SOLO + 2 * shared)
        if i < PIECES:
            return at + i * PIECE, at + (i + 1) * PIECE
        at = pair_start(k // 2) + SOLO + (k % 2) * shared
        return at, at + shared

    def taken(k, i, a, b):
        lo, _ = span(k, i)
        if i < PIECES:
            lo -= i * PIECE
            return recv[k, :, a - lo : b - lo].astype(jnp.float32)
        return recv_sh[k, :, a - lo : b - lo].astype(jnp.float32)

    every = [(k, i) for k in range(n) for i in range(PIECES + 1)]
    cuts = sorted({min(end, rows) for piece in every for end in span(*piece)})

    def finish(order):
        here = []
        left = [
            (a, b, [p for p in every if span(*p)[0] < b and span(*p)[1] > a])
            for a, b in zip(cuts[:-1], cuts[1:])
        ]
        for k, i in order:
            owner_copy(r, k, i).wait_recv()
            here.append((k, i))
            ready = [item for item in left if all(p in here for p in item[2])]
            left = [item for item in left if item not in ready]
            for a, b, pieces in ready:
                total = sum(taken(*p, a, b) for p in pieces)
                value = (total * rec[:, a:b]).astype(jnp.bfloat16)
                out_ref[a:b] = jnp.swapaxes(value, 0, 1)

    for is_low in (True, False):
        near = [k for k in range(n) if (k < n // 2) == is_low]
        far = [k for k in range(n) if (k < n // 2) != is_low]
        order = [(k, i) for i in range(PIECES - 1) for k in far]
        order += [(k, i) for i in range(PIECES + 1) for k in near]
        order += [(k, i) for i in (PIECES - 1, PIECES) for k in far]

        @pl.when(low == is_low)
        def _():
            finish(order)

    for o in range(n):
        swap_owner(o).wait_send()

        @pl.when(r != o)
        def _():
            for i in range(PIECES + 1):
                owner_copy(o, r, i).wait_send()

    for side in range(2):
        swap_edge(side).wait_send()

        @pl.when(sends_to(side))
        def _():
            for i in range(PIECES + 1):
                edge_copy(side, i).wait_send()


def solution(mesh):
    groups, n = mesh.shape["slab"], mesh.shape["tile"]

    def shards(tiles, offsets, fracs):
        _, depth, tile_rows, cols = tiles.shape
        per = GROUPZ // n
        rows = (n - 1) * STEPY + tile_rows
        reach = max(
            min(k * STEPY + JITY, rows - tile_rows) + tile_rows - frame_start(k) for k in range(n)
        )
        shared = round_up(max(reach - SOLO, 16), 16) // 2
        frame = SOLO + 2 * shared
        acc_rows = round_up(max(rows, frame_start(n - 1) + frame), 16)
        head = per + 2 * JIT + 1
        plane = ramp(tile_rows, RY)[:, None] * ramp(cols, RX)[None, :]
        table = np.zeros((round_up(PADY + frame + 8, 8), cols), np.float32)
        table[PADY : PADY + tile_rows] = plane
        rampz = np.zeros((depth + 2 * PADZ,), np.float32)
        rampz[PADZ : PADZ + depth] = ramp(depth, 2 * MARGIN)
        bf16, f32 = jnp.bfloat16, jnp.float32
        dma = pltpu.SemaphoreType.DMA
        slots = GROUPZ + 2 * EDGE
        joined = pl.pallas_call(
            functools.partial(kernel, groups, n, per, depth, tile_rows, shared),
            out_shape=pltpu.VMEM((rows, per, cols), bf16),
            in_specs=[pl.BlockSpec(memory_space=pl.ANY)] * 5,
            out_specs=pl.BlockSpec(memory_space=pltpu.VMEM),
            scratch_shapes=[
                pltpu.VMEM((head, tile_rows, cols), bf16),
                pltpu.VMEM((depth + 1, tile_rows, cols), bf16),
                pltpu.VMEM((frame, 2 * tile_rows), bf16),
                pltpu.VMEM((frame, cols), f32),
                pltpu.VMEM((frame, cols), f32),
                pltpu.VMEM((n, per, SOLO, cols), bf16),
                pltpu.VMEM((n, per, shared, cols), bf16),
                pltpu.VMEM((slots, shared, cols), f32),
                pltpu.VMEM((slots, shared, cols), bf16),
                pltpu.VMEM((slots, shared, cols), bf16),
                pltpu.VMEM((2, EDGE, SOLO, cols), bf16),
                pltpu.VMEM((2, EDGE, shared, cols), bf16),
                pltpu.VMEM((2, EDGE, SOLO, cols), bf16),
                pltpu.VMEM((2, EDGE, shared, cols), bf16),
                pltpu.VMEM((n, per, SOLO, cols), bf16),
                pltpu.VMEM((n, per, shared, cols), bf16),
                pltpu.VMEM((per, acc_rows, cols), f32),
                pltpu.SMEM((offsets.shape[1], offsets.shape[0]), jnp.int32),
                pltpu.SMEM((fracs.shape[1], fracs.shape[0]), jnp.int32),
                pltpu.SMEM(rampz.shape, f32),
                pltpu.VMEM(table.shape, f32),
                dma((4,)), dma((2,)), dma((n + 2,)), dma((n + 2,)),
                dma((2, PIECES + 1)), dma((2, PIECES + 1)),
                dma((n, PIECES + 1)), dma((n, PIECES + 1)),
                pltpu.SemaphoreType.REGULAR,
            ],
            compiler_params=pltpu.CompilerParams(collective_id=0, has_side_effects=True),
        )(offsets.T, fracs.T, jnp.asarray(rampz), jnp.asarray(table), tiles)
        return jnp.transpose(joined, (1, 0, 2))

    in_specs = (P(("slab", "tile"), None, None, None), P(), P())
    out_specs = P(("slab", "tile"), None, None)
    return jax.shard_map(shards, mesh=mesh, in_specs=in_specs, out_specs=out_specs, check_vma=False)
```

```python
import functools

import jax
import jax.numpy as jnp
import numpy as np
from jax import lax
from jax.experimental import pallas as pl
from jax.experimental.pallas import tpu as pltpu
from jax.sharding import PartitionSpec as P

GROUPZ = 16
MARGIN = 2
JIT = 1
STEPY = 230
JITY = 4
RY = 26
RX = 16
QUANT = 16
EDGE = MARGIN + JIT
PADY = 32
PADZ = 24
PIECES = 4

weight_floor = 0.05
MESH = pl.DeviceIdType.MESH


def ramp(length, ramp_width):
    position = np.arange(length, dtype=np.float64)
    rising = 0.5 - 0.5 * np.cos(np.pi * (position + 1.0) / (ramp_width + 1.0))
    rising = np.where(position < ramp_width, rising, 1.0)
    return np.minimum(rising, rising[::-1])


def round_up(value, step):
    return -(-value // step) * step


SOLO = STEPY // 8 * 8


def pair_start(pair):
    if isinstance(pair, int):
        return max(2 * pair * STEPY - JITY, 0) // 8 * 8
    return jnp.maximum(2 * pair * STEPY - JITY, 0) // 8 * 8


def frame_start(rank):
    return pair_start(rank // 2) + SOLO * (rank % 2)


def kernel(
    groups, n, per, depth, tile_rows, shared,
    offs_ref, fracs_ref, rampz_ref, table_ref, tile_ref, out_ref,
    head, raw, coef, wa, wb, blend, own_sh, give, got,
    edge_send, far_recv, near_recv, recv, rec,
    offs, fracs, rampz, table,
    small_sem, load_sem, give_sem, got_sem, es_sem, far_sem, near_sem, s_sem, r_sem,
    above_sem, below_sem,
):
    g = lax.axis_index("slab")
    r = lax.axis_index("tile")
    me = g * n + r
    chip = r // 2
    pairs = n // 2
    low = r < n // 2
    high = jnp.logical_not(low)
    odd = r % 2 == 1
    partner = r + 1 - 2 * (r % 2)
    cols = raw.shape[2]
    last = n - 1
    frame = SOLO + 2 * shared
    half = SOLO + shared
    rows = out_ref.shape[0]
    steps = half // 8
    cut = [steps * i // PIECES * 8 for i in range(PIECES + 1)]
    direct = pairs == 2

    barrier = pltpu.get_barrier_semaphore()
    has_below = g > 0
    has_above = g < groups - 1
    for i in range(1, n):
        pl.semaphore_signal(
            barrier, inc=1, device_id=(g, lax.rem(r + i, n)), device_id_type=MESH
        )

    @pl.when(has_above)
    def _():
        pl.semaphore_signal(barrier, inc=1, device_id=(g + 1, r), device_id_type=MESH)

    far_side = jnp.where(low, 1, 0)
    near_side = 1 - far_side

    def sends_to(side):
        return jnp.where(side == 0, g < groups - 1, g > 0)

    def gets_from(side):
        return jnp.where(side == 0, g > 0, g < groups - 1)

    gets_far = gets_from(far_side)
    gets_near = gets_from(near_side)

    def mirrored(owner):
        return jnp.where(low, owner, last - owner)

    edge_planes = list(range(EDGE)) + list(range(GROUPZ - EDGE, GROUPZ))
    bound = sorted({q // per for q in edge_planes}, reverse=True)
    free = [o for o in range(last, -1, -1) if o not in bound]
    far_free = [o for o in free if o >= n // 2]
    far_bound = [o for o in bound if o >= n // 2]
    near_free = [o for o in free if o < n // 2]
    near_bound = [o for o in bound if o < n // 2]
    far_list = far_free + far_bound
    near_list = near_free + near_bound
    near_owner = mirrored(near_bound[-1])
    takes_near = jnp.logical_and(gets_near, r == near_owner)

    def far_owner(i):
        return mirrored(jnp.where(gets_far, far_list[i], far_list[-1 - i]))

    smalls = [
        pltpu.make_async_copy(source, target, small_sem.at[i])
        for i, (source, target) in enumerate(
            [(offs_ref, offs), (fracs_ref, fracs), (rampz_ref, rampz), (table_ref, table)]
        )
    ]
    for small in smalls:
        small.start()
    first_owner = far_owner(0)
    head_planes = head.shape[0]
    head_start = jnp.minimum(first_owner * per + MARGIN - JIT, depth - head_planes)
    head_load = pltpu.make_async_copy(
        tile_ref.at[0, pl.ds(head_start, head_planes)], head, load_sem.at[0]
    )
    head_load.start()
    load = pltpu.make_async_copy(tile_ref.at[0], raw.at[pl.ds(0, depth)], load_sem.at[1])
    load.start()
    raw[depth] = jnp.zeros(raw.shape[1:], raw.dtype)

    def rampz_at(z):
        return rampz[jnp.clip(z + PADZ, 0, rampz.shape[0] - 1)]

    smalls[0].wait()
    smalls[1].wait()
    corner = offs[0, me]
    shift = jnp.clip(offs[1, me] - frame_start(r), 0, frame - tile_rows)
    base = g * GROUPZ - corner
    fz = fracs[0, me].astype(jnp.float32) / QUANT
    fy = fracs[1, me].astype(jnp.float32) / QUANT
    fx = fracs[2, me].astype(jnp.float32) / QUANT
    start_solo = jnp.where(odd, 2 * shared, 0)
    start_own = jnp.where(odd, shared, SOLO)
    start_give = jnp.where(odd, 0, half)
    parts = [(0, SOLO, start_solo), (SOLO, shared, start_own), (half, shared, start_give)]
    for at, count, start in parts:
        row = lax.broadcasted_iota(jnp.int32, (count, tile_rows), 0)
        col = lax.broadcasted_iota(jnp.int32, (count, tile_rows), 1)
        behind = col - row + (shift - start)
        lerp_y = jnp.where(behind == 0, 1.0 - fy, jnp.where(behind == 1, fy, 0.0))
        coef[at : at + count, :tile_rows] = ((1.0 - fz) * lerp_y).astype(jnp.bfloat16)
        coef[at : at + count, tile_rows:] = (fz * lerp_y).astype(jnp.bfloat16)
    smalls[2].wait()
    smalls[3].wait()
    for at, count, start in parts:
        weight = table[pl.ds(PADY + start - shift, count), :]
        lane = lax.broadcasted_iota(jnp.int32, (count, cols), 1)
        wa[at : at + count] = weight * (1.0 - fx)
        wb[at : at + count] = jnp.where(lane < cols - 1, weight * fx, 0.0)

    def planes(store, source, source_start, limit, first, count, lo, hi):
        at = [jnp.clip(first + j, 0, depth - 1) - source_start for j in range(count)]
        at = [jnp.clip(z, 0, limit) for z in at]
        top = jnp.concatenate([source[z] for z in at], axis=1)
        bottom = jnp.concatenate([source[z + 1] for z in at], axis=1)
        mixed = jnp.dot(
            coef[lo:hi], jnp.concatenate([top, bottom], axis=0),
            preferred_element_type=jnp.float32,
        )
        for j in range(count):
            part = mixed[:, j * cols : (j + 1) * cols]
            value = part * wa[lo:hi] + pltpu.roll(part, cols - 1, 1) * wb[lo:hi]
            store(j, value * rampz_at(first + j))

    def blend_rows(target, at, slot, where_from, first, count, lo, hi):
        def store(j, value):
            top = min(hi, SOLO)
            if lo < top:
                target[at, j, lo:top] = value[: top - lo].astype(jnp.bfloat16)
            if hi > SOLO:
                own_sh[slot + j] = value[SOLO - lo : half - lo]
                give[slot + j] = value[half - lo :].astype(jnp.bfloat16)

        planes(store, *where_from, first, count, lo, hi)

    whole = (raw, 0, depth - 1)

    def blend_owner(owner, lo=0, hi=frame, where_from=whole):
        blend_rows(blend, owner, owner * per, where_from, base + owner * per, per, lo, hi)

    def edge_slot(side):
        return GROUPZ + side * EDGE

    def blend_edge(side):
        first = base + jnp.where(side == 0, GROUPZ, -EDGE)
        blend_rows(edge_send, side, edge_slot(side), whole, first, EDGE, 0, frame)

    def swap_copy(slot, count, at):
        part = pl.ds(slot, count)
        return pltpu.make_async_remote_copy(
            src_ref=give.at[part], dst_ref=got.at[part],
            send_sem=give_sem, recv_sem=got_sem.at[at],
            device_id=(g, partner), device_id_type=MESH,
        )

    def joined_rows(slot):
        return (own_sh[slot] + got[slot].astype(jnp.float32)).astype(jnp.bfloat16)

    def join_owner(owner):
        for j in range(per):
            blend[owner, j, SOLO:half] = joined_rows(owner * per + j)

    def join_edge(side):
        for p in range(EDGE):
            edge_send[side, p, SOLO:half] = joined_rows(edge_slot(side) + p)

    def rows_of(i):
        return pl.ds(cut[i], cut[i + 1] - cut[i])

    def came(source_chip, i):
        away = lax.rem(source_chip - chip + pairs, pairs)
        return jnp.where(away == 0, 0, 1 + (away - 1) * PIECES + i)

    def send(owner, i, when=True):
        there = owner // 2
        away = lax.rem(chip - there + pairs, pairs)
        at = jnp.where(away == 0, 0, 1 + (away - 1) * PIECES + i)

        @pl.when(jnp.logical_and(when, owner != r))
        def _():
            pltpu.make_async_remote_copy(
                src_ref=blend.at[owner, :, rows_of(i)], dst_ref=recv.at[r, :, rows_of(i)],
                send_sem=s_sem, recv_sem=r_sem.at[at],
                device_id=(g, owner), device_id_type=MESH,
            ).start()

        @pl.when(jnp.logical_and(when, owner == r))
        def _():
            pltpu.make_async_copy(
                blend.at[owner, :, rows_of(i)], recv.at[r, :, rows_of(i)], r_sem.at[at]
            ).start()

    def await_far(source_chip, i):
        part = recv.at[pl.ds(2 * source_chip, 2), :, rows_of(i)]
        pltpu.make_async_copy(part, part, r_sem.at[came(source_chip, i)]).wait()

    def await_own():
        part = recv.at[pl.ds(2 * chip, 2)]
        pltpu.make_async_copy(part, part, r_sem.at[0]).wait()

    def send_far(i):
        @pl.when(sends_to(far_side))
        def _():
            pltpu.make_async_remote_copy(
                src_ref=edge_send.at[far_side, :, rows_of(i)], dst_ref=far_recv.at[:, rows_of(i)],
                send_sem=es_sem.at[0], recv_sem=far_sem.at[i],
                device_id=(g + 1 - 2 * far_side, r), device_id_type=MESH,
            ).start()

    near_slot = r % 2 if direct else 0
    near_target = near_owner if direct else r

    def send_near(i):
        @pl.when(sends_to(near_side))
        def _():
            pltpu.make_async_remote_copy(
                src_ref=edge_send.at[near_side, :, rows_of(i)],
                dst_ref=near_recv.at[near_slot, :, rows_of(i)],
                send_sem=es_sem.at[1], recv_sem=near_sem.at[i],
                device_id=(g + 1 - 2 * near_side, near_target), device_id_type=MESH,
            ).start()

    def await_piece(part, sem):
        pltpu.make_async_copy(part, part, sem).wait()

    def add_edge(side, source, i):
        for p in range(EDGE):
            q = p + jnp.where(side == 0, 0, GROUPZ - EDGE)
            owner, j = q // per, q % per
            a, b = cut[i], cut[i + 1]
            blend[owner, j, a:b] = (
                blend[owner, j, a:b].astype(jnp.float32) + source[p, a:b].astype(jnp.float32)
            ).astype(jnp.bfloat16)

    near_head = (head, head_start, head_planes - 2)
    head_load.wait()
    blend_owner(first_owner, 0, cut[1], near_head)
    pl.semaphore_wait(barrier, n - 1 + jnp.where(has_below, 1, 0))
    not_far = jnp.logical_not(gets_far)
    send(first_owner, 0, True if far_free else not_far)

    @pl.when(has_below)
    def _():
        pl.semaphore_signal(above_sem, inc=1, device_id=(g - 1, r), device_id_type=MESH)

    blend_owner(first_owner, cut[1], frame, near_head)
    for i in range(1, PIECES - 1):
        send(first_owner, i, True if far_free else not_far)
    swap_copy(first_owner * per, per, 0).start()

    load.wait()
    blend_edge(far_side)
    swap_copy(edge_slot(far_side), EDGE, 0).start()

    @pl.when(low)
    def _():
        for i in range(PIECES - 1):
            send_far(i)

    for at in range(1, len(far_list)):
        owner = far_owner(at)
        blend_owner(owner)
        swap_copy(owner * per, per, 1).start()

    @pl.when(jnp.logical_and(has_above, high))
    def _():
        pl.semaphore_wait(above_sem, 1)
        if direct:
            pl.semaphore_signal(below_sem, inc=1, device_id=(g + 1, r), device_id_type=MESH)
        for i in range(PIECES - 1):
            send_far(i)

    await_piece(got.at[pl.ds(0, per + EDGE)], got_sem.at[0])
    join_owner(first_owner)
    send(first_owner, PIECES - 1, True if far_free else not_far)
    join_edge(far_side)
    send_far(PIECES - 1)
    for at in range(1, len(far_list)):
        owner = far_owner(at)
        for i in range(PIECES - 1):
            send(owner, i, True if at < len(far_free) else not_far)

    for o in near_list:
        owner = mirrored(o)
        blend_owner(owner)
        swap_copy(owner * per, per, 1).start()
    blend_edge(near_side)
    swap_copy(edge_slot(near_side), EDGE, 1).start()
    if direct:
        @pl.when(jnp.logical_not(takes_near))
        def _():
            near_recv[...] = jnp.zeros_like(near_recv)

    await_piece(got.at[pl.ds(0, GROUPZ - per + EDGE)], got_sem.at[1])
    for at in range(1, len(far_list)):
        owner = far_owner(at)
        join_owner(owner)
        send(owner, PIECES - 1, True if at < len(far_free) else not_far)
    for o in near_list:
        owner = mirrored(o)
        join_owner(owner)
        for i in range(PIECES):
            send(owner, i, True if direct or o in near_free else jnp.logical_not(gets_near))
    join_edge(near_side)

    rec[...] = jnp.zeros_like(rec)
    for k in range(n):
        s = frame_start(k)
        totals = [0.0] * per
        for delta in (-1, 0, 1):
            group = jnp.clip(g + delta, 0, groups - 1)
            exists = jnp.where(group == g + delta, 1.0, 0.0)
            z0 = offs[0, group * n + k]
            ahead = jnp.clip(offs[1, group * n + k] - s, 0, frame - tile_rows)
            wy = table[pl.ds(PADY - ahead, frame), :]
            for j in range(per):
                z = g * GROUPZ + r * per + j - z0
                totals[j] = totals[j] + wy * (rampz_at(z) * exists)
        for j in range(per):
            rec[j, s : s + frame] = rec[j, s : s + frame] + totals[j]
    rec[...] = 1.0 / jnp.maximum(rec[...], weight_floor)

    @pl.when(jnp.logical_and(has_above, low))
    def _():
        pl.semaphore_wait(above_sem, 1)

    if direct:
        @pl.when(jnp.logical_and(has_below, high))
        def _():
            pl.semaphore_wait(below_sem, 1)

    for i in range(PIECES):
        @pl.when(gets_far)
        def _():
            await_piece(far_recv.at[:, rows_of(i)], far_sem.at[i])
            add_edge(far_side, far_recv, i)
            for o in far_bound:
                send(mirrored(o), i)

        send_near(i)

    if not direct:
        @pl.when(gets_near)
        def _():
            for i in range(PIECES):
                await_piece(near_recv.at[0, :, rows_of(i)], near_sem.at[i])
                add_edge(near_side, near_recv.at[0], i)
                for o in near_bound:
                    send(mirrored(o), i)

    def spans(k, i):
        solo_at = pair_start(k // 2) + (k % 2) * (SOLO + 2 * shared)
        shared_at = pair_start(k // 2) + SOLO + (k % 2) * shared
        a, b = cut[i], cut[i + 1]
        found = [(solo_at + a, solo_at + min(b, SOLO), solo_at)] if a < SOLO else []
        if b > SOLO:
            a = max(a, SOLO)
            found.append((shared_at + a - SOLO, shared_at + b - SOLO, shared_at - SOLO))
        return found

    segments = [(k, i, *span) for k in range(n) for i in range(PIECES) for span in spans(k, i)]
    marks = sorted({min(end, rows) for item in segments for end in item[2:4]})
    intervals = [
        (a, b, [(k, i, at) for k, i, lo, hi, at in segments if lo < b and hi > a])
        for a, b in zip(marks[:-1], marks[1:])
    ]

    def finish(a, b, pieces, own=None, first=0):
        total = 0.0
        for k, i, at in pieces:
            total = total + recv[k, :, a - at : b - at].astype(jnp.float32)
            if k // 2 == own:
                edge = near_recv[k % 2, :, a - at : b - at].astype(jnp.float32)
                blank = [jnp.zeros((count, b - a, cols), jnp.float32) for count in (first, per - EDGE - first)]
                kept = [part for part in (blank[0], edge, blank[1]) if part.shape[0]]
                total = total + jnp.concatenate(kept, axis=0)
        value = (total * rec[:, a:b]).astype(jnp.bfloat16)
        out_ref[a:b] = jnp.swapaxes(value, 0, 1)

    if direct:
        for own in range(2):
            @pl.when(chip == own)
            def _():
                left = list(intervals)
                here = set()
                await_own()
                for i in range(PIECES):
                    @pl.when(takes_near)
                    def _():
                        await_piece(near_recv.at[:, :, rows_of(i)], near_sem.at[i])

                    for source in (own, 1 - own):
                        if source != own:
                            await_far(source, i)
                        here |= {(2 * source, i), (2 * source + 1, i)}
                        for item in list(left):
                            if all((k, j) in here for k, j, _ in item[2]):
                                left.remove(item)
                                finish(*item, own, 0 if own == 0 else per - EDGE)
    else:
        await_own()
        for away in range(1, pairs):
            for i in range(PIECES):
                await_far(lax.rem(chip + away, pairs), i)
        for item in intervals:
            finish(*item)

    def await_sent(part, sem):
        pltpu.make_async_copy(part, part, sem).wait()

    await_sent(give, give_sem)
    await_sent(blend.at[pl.ds(0, n - 1)], s_sem)
    for at, side in enumerate((far_side, near_side)):
        @pl.when(sends_to(side))
        def _():
            await_sent(far_recv, es_sem.at[at])


def solution(mesh):
    groups, n = mesh.shape["slab"], mesh.shape["tile"]

    def shards(tiles, offsets, fracs):
        _, depth, tile_rows, cols = tiles.shape
        per = GROUPZ // n
        rows = (n - 1) * STEPY + tile_rows
        reach = max(
            min(k * STEPY + JITY, rows - tile_rows) + tile_rows - frame_start(k) for k in range(n)
        )
        shared = round_up(max(reach - SOLO, 16), 16) // 2
        frame, half = SOLO + 2 * shared, SOLO + shared
        acc_rows = round_up(max(rows, frame_start(n - 1) + frame), 16)
        head = per + 2 * JIT + 1
        plane = ramp(tile_rows, RY)[:, None] * ramp(cols, RX)[None, :]
        table = np.zeros((round_up(PADY + frame + 8, 8), cols), np.float32)
        table[PADY : PADY + tile_rows] = plane
        rampz = np.zeros((depth + 2 * PADZ,), np.float32)
        rampz[PADZ : PADZ + depth] = ramp(depth, 2 * MARGIN)
        bf16, f32 = jnp.bfloat16, jnp.float32
        dma, signal = pltpu.SemaphoreType.DMA, pltpu.SemaphoreType.REGULAR
        slots = GROUPZ + 2 * EDGE
        joined = pl.pallas_call(
            functools.partial(kernel, groups, n, per, depth, tile_rows, shared),
            out_shape=pltpu.VMEM((rows, per, cols), bf16),
            in_specs=[pl.BlockSpec(memory_space=pl.ANY)] * 5,
            out_specs=pl.BlockSpec(memory_space=pltpu.VMEM),
            scratch_shapes=[
                pltpu.VMEM((head, tile_rows, cols), bf16),
                pltpu.VMEM((depth + 1, tile_rows, cols), bf16),
                pltpu.VMEM((frame, 2 * tile_rows), bf16),
                pltpu.VMEM((frame, cols), f32),
                pltpu.VMEM((frame, cols), f32),
                pltpu.VMEM((n, per, half, cols), bf16),
                pltpu.VMEM((slots, shared, cols), f32),
                pltpu.VMEM((slots, shared, cols), bf16),
                pltpu.VMEM((slots, shared, cols), bf16),
                pltpu.VMEM((2, EDGE, half, cols), bf16),
                pltpu.VMEM((EDGE, half, cols), bf16),
                pltpu.VMEM((2, EDGE, half, cols), bf16),
                pltpu.VMEM((n, per, half, cols), bf16),
                pltpu.VMEM((per, acc_rows, cols), f32),
                pltpu.SMEM((offsets.shape[1], offsets.shape[0]), jnp.int32),
                pltpu.SMEM((fracs.shape[1], fracs.shape[0]), jnp.int32),
                pltpu.SMEM(rampz.shape, f32),
                pltpu.VMEM(table.shape, f32),
                dma((4,)), dma((2,)), dma, dma((2,)), dma((2,)),
                dma((PIECES,)), dma((PIECES,)), dma, dma(((n // 2 - 1) * PIECES + 1,)),
                signal, signal,
            ],
            compiler_params=pltpu.CompilerParams(collective_id=0, has_side_effects=True),
        )(offsets.T, fracs.T, jnp.asarray(rampz), jnp.asarray(table), tiles)
        return jnp.transpose(joined, (1, 0, 2))

    in_specs = (P(("slab", "tile"), None, None, None), P(), P())
    out_specs = P(("slab", "tile"), None, None)
    return jax.shard_map(shards, mesh=mesh, in_specs=in_specs, out_specs=out_specs, check_vma=False)
```

```python
import functools

import jax
import jax.numpy as jnp
import numpy as np
from jax import lax
from jax.experimental import pallas as pl
from jax.experimental.pallas import tpu as pltpu
from jax.sharding import PartitionSpec as P

GROUPZ = 16
MARGIN = 2
JIT = 1
STEPY = 230
JITY = 4
RY = 26
RX = 16
QUANT = 16
EDGE = MARGIN + JIT
PADY = 32
PIECES = 4
LOADZ = 4

weight_floor = 0.05
MESH = pl.DeviceIdType.MESH


def ramp(length, ramp_width):
    position = np.arange(length, dtype=np.float64)
    rising = 0.5 - 0.5 * np.cos(np.pi * (position + 1.0) / (ramp_width + 1.0))
    rising = np.where(position < ramp_width, rising, 1.0)
    return np.minimum(rising, rising[::-1])


def ramp_at(position, length, ramp_width):
    inward = jnp.minimum(position, length - 1 - position)
    t = (inward + 1).astype(jnp.float32) * float(np.pi / 2 / (ramp_width + 1.0))
    square = t * t
    sine = jnp.full(t.shape, 1.0 / 6227020800.0, jnp.float32)
    for term in (-39916800.0, 362880.0, -5040.0, 120.0, -6.0, 1.0):
        sine = sine * square + 1.0 / term
    sine = sine * t
    value = jnp.where(inward < ramp_width, sine * sine, 1.0)
    return jnp.where(inward < 0, 0.0, value)


def round_up(value, step):
    return -(-value // step) * step


SOLO = STEPY // 8 * 8
MAIN = SOLO - 8


def pair_start(pair):
    if isinstance(pair, int):
        return max(2 * pair * STEPY - JITY, 0) // 8 * 8
    return jnp.maximum(2 * pair * STEPY - JITY, 0) // 8 * 8


def frame_start(rank):
    return pair_start(rank // 2) + SOLO * (rank % 2)


def kernel(
    groups, n, per, depth, tile_rows, shared, trim,
    offs_ref, fracs_ref, tile_ref, out_ref,
    lead, head, raw, coef, coef_lead, wa, wb, blend, own_sh, give, got,
    edge_send, far_recv, near_recv, recv, rec,
    offs, fracs, rampz, table,
    small_sem, load_sem, give_sem, got_sem, es_sem, far_sem, near_sem, s_sem, r_sem,
    above_sem, below_sem, clear_sem,
):
    g = lax.axis_index("slab")
    r = lax.axis_index("tile")
    me = g * n + r
    chip = r // 2
    pairs = n // 2
    low = r < n // 2
    high = jnp.logical_not(low)
    odd = r % 2 == 1
    partner = r + 1 - 2 * (r % 2)
    cols = raw.shape[2]
    last = n - 1
    frame = SOLO + 2 * shared
    half = SOLO + shared
    rows = out_ref.shape[0]
    steps = MAIN // 8
    cut = [steps * i // (PIECES - 1) * 8 for i in range(PIECES)] + [half]
    direct = pairs == 2

    barrier = pltpu.get_barrier_semaphore()
    has_below = g > 0
    has_above = g < groups - 1
    for i in range(1, n):
        pl.semaphore_signal(
            barrier, inc=1, device_id=(g, lax.rem(r + i, n)), device_id_type=MESH
        )

    @pl.when(has_above)
    def _():
        pl.semaphore_signal(barrier, inc=1, device_id=(g + 1, r), device_id_type=MESH)

    @pl.when(jnp.logical_and(has_below, high))
    def _():
        pl.semaphore_signal(barrier, inc=1, device_id=(g - 1, r), device_id_type=MESH)

    greeted = n - 1 + jnp.where(has_below, 1, 0) + jnp.where(jnp.logical_and(has_above, high), 1, 0)
    far_side = jnp.where(low, 1, 0)
    near_side = 1 - far_side

    def sends_to(side):
        return jnp.where(side == 0, g < groups - 1, g > 0)

    def gets_from(side):
        return jnp.where(side == 0, g > 0, g < groups - 1)

    gets_far = gets_from(far_side)
    gets_near = gets_from(near_side)

    def mirrored(owner):
        return jnp.where(low, owner, last - owner)

    edge_planes = list(range(EDGE)) + list(range(GROUPZ - EDGE, GROUPZ))
    bound = sorted({q // per for q in edge_planes}, reverse=True)
    free = [o for o in range(last, -1, -1) if o not in bound]
    far_free = [o for o in free if o >= n // 2]
    far_bound = [o for o in bound if o >= n // 2]
    near_free = [o for o in free if o < n // 2]
    near_bound = [o for o in bound if o < n // 2]
    far_list = far_free + far_bound
    near_list = near_free + near_bound
    near_owner = mirrored(near_bound[-1])
    takes_near = jnp.logical_and(gets_near, r == near_owner)

    def far_owner(i):
        return mirrored(jnp.where(gets_far, far_list[i], far_list[-1 - i]))

    offs_load = pltpu.make_async_copy(offs_ref, offs, small_sem.at[0])
    fracs_load = pltpu.make_async_copy(fracs_ref, fracs, small_sem.at[1])
    first_owner = far_owner(0)
    head_planes = head.shape[0]
    head_start = jnp.minimum(first_owner * per + MARGIN - JIT, depth - head_planes)
    lead_rows = lead.shape[1]
    lead_start = jnp.where(odd, max(2 * shared - (frame - tile_rows), 0) // 8 * 8, 0)
    head_part = pl.ds(head_start, head_planes)
    pltpu.make_async_copy(
        tile_ref.at[0, head_part, pl.ds(pl.multiple_of(lead_start, 8), lead_rows)],
        lead, load_sem.at[2],
    ).start()
    offs_load.start()
    fracs_load.start()
    pltpu.make_async_copy(tile_ref.at[0, head_part], head, load_sem.at[0]).start()

    def await_piece(part, sem):
        pltpu.make_async_copy(part, part, sem).wait()

    raw[depth] = jnp.zeros(raw.shape[1:], raw.dtype)

    for at, value in enumerate([0.0, *ramp(depth, 2 * MARGIN), 0.0]):
        rampz[at] = jnp.float32(value)
    row = lax.broadcasted_iota(jnp.int32, table.shape, 0) - PADY
    col = lax.broadcasted_iota(jnp.int32, (8, cols), 1)
    table[...] = ramp_at(row, tile_rows, RY) * ramp_at(col, cols, RX)[:1]

    def rampz_at(z):
        return rampz[jnp.clip(z, -1, depth) + 1]

    offs_load.wait()
    fracs_load.wait()
    corner = offs[0, me]
    shift = jnp.clip(offs[1, me] - frame_start(r), 0, frame - tile_rows)
    base = g * GROUPZ - corner
    fz = fracs[0, me].astype(jnp.float32) / QUANT
    fy = fracs[1, me].astype(jnp.float32) / QUANT
    fx = fracs[2, me].astype(jnp.float32) / QUANT
    start_solo = jnp.where(odd, 2 * shared, 0)
    start_own = jnp.where(odd, shared, SOLO)
    start_give = jnp.where(odd, 0, half)
    parts = [
        (0, MAIN, start_solo), (MAIN, shared, start_own),
        (MAIN + shared, SOLO - MAIN, start_solo + MAIN), (half, shared, start_give),
    ]
    def lerps(target, at, count, start, first_col, width):
        row = lax.broadcasted_iota(jnp.int32, (count, width), 0)
        col = lax.broadcasted_iota(jnp.int32, (count, width), 1)
        behind = col - row + (shift - start + first_col)
        lerp_y = jnp.where(behind == 0, 1.0 - fy, jnp.where(behind == 1, fy, 0.0))
        target[at : at + count, :width] = ((1.0 - fz) * lerp_y).astype(jnp.bfloat16)
        target[at : at + count, width:] = (fz * lerp_y).astype(jnp.bfloat16)

    def weights(at, count, start):
        weight = table[pl.ds(PADY + start - shift, count), :]
        lane = lax.broadcasted_iota(jnp.int32, (count, cols), 1)
        wa[at : at + count] = weight * (1.0 - fx)
        wb[at : at + count] = jnp.where(lane < cols - 1, weight * fx, 0.0)

    def planes(store, source, source_start, limit, factors, first, count, lo, hi):
        at = [jnp.clip(first + j, 0, depth - 1) - source_start for j in range(count)]
        at = [jnp.clip(z, 0, limit) for z in at]
        top = jnp.concatenate([source[z] for z in at], axis=1)
        bottom = jnp.concatenate([source[z + 1] for z in at], axis=1)
        mixed = jnp.dot(
            factors[lo:hi], jnp.concatenate([top, bottom], axis=0),
            preferred_element_type=jnp.float32,
        )
        for j in range(count):
            part = mixed[:, j * cols : (j + 1) * cols]
            value = part * wa[lo:hi] + pltpu.roll(part, cols - 1, 1) * wb[lo:hi]
            store(j, value * rampz_at(first + j))

    def blend_rows(target, at, start, slot, where_from, first, count, lo, hi):
        def store(j, value):
            top = min(hi, MAIN)
            if lo < top:
                target[at, start + j, lo:top] = value[: top - lo].astype(jnp.bfloat16)
            if hi > MAIN:
                own_sh[slot + j] = value[MAIN - lo : MAIN + shared - lo]
                target[at, start + j, MAIN + shared : half] = value[
                    MAIN + shared - lo : half - lo
                ].astype(jnp.bfloat16)
                give[slot + j] = value[half - lo :].astype(jnp.bfloat16)

        planes(store, *where_from, first, count, lo, hi)

    whole = (raw, 0, depth - 1, coef)

    def blend_owner(owner, lo=0, hi=frame, where_from=whole, j=0, count=per):
        first = owner * per + j
        blend_rows(blend, owner, j, first, where_from, base + first, count, lo, hi)

    def edge_slot(side):
        return GROUPZ + side * EDGE

    def blend_edge(side):
        first = base + jnp.where(side == 0, GROUPZ, -EDGE)
        blend_rows(edge_send, side, 0, edge_slot(side), whole, first, EDGE, 0, frame)

    def swap_copy(slot, count, at):
        part = pl.ds(slot, count)
        return pltpu.make_async_remote_copy(
            src_ref=give.at[part], dst_ref=got.at[part],
            send_sem=give_sem, recv_sem=got_sem.at[at],
            device_id=(g, partner), device_id_type=MESH,
        )

    def joined_rows(slot):
        return (own_sh[slot] + got[slot].astype(jnp.float32)).astype(jnp.bfloat16)

    def join_owner(owner):
        for j in range(per):
            blend[owner, j, MAIN : MAIN + shared] = joined_rows(owner * per + j)

    def join_edge(side):
        for p in range(EDGE):
            edge_send[side, p, MAIN : MAIN + shared] = joined_rows(edge_slot(side) + p)

    def rows_of(i):
        return pl.ds(cut[i], cut[i + 1] - cut[i])

    def came(source_chip, i):
        away = lax.rem(source_chip - chip + pairs, pairs)
        return jnp.where(away == 0, 0, 1 + (away - 1) * PIECES + i)

    def send(owner, i, when=True, start=0, count=per):
        there = owner // 2
        away = lax.rem(chip - there + pairs, pairs)
        at = jnp.where(away == 0, 0, 1 + (away - 1) * PIECES + i)
        shapes = [(when, 0)] if i < PIECES - 1 else [
            (jnp.logical_and(when, jnp.logical_not(odd)), 0), (jnp.logical_and(when, odd), trim)
        ]
        for condition, less in shapes:
            part = pl.ds(cut[i], cut[i + 1] - cut[i] - less)
            source = blend.at[owner, pl.ds(start, count), part]
            target = recv.at[r, pl.ds(start, count), part]

            @pl.when(jnp.logical_and(condition, owner != r))
            def _():
                pltpu.make_async_remote_copy(
                    src_ref=source, dst_ref=target, send_sem=s_sem, recv_sem=r_sem.at[at],
                    device_id=(g, owner), device_id_type=MESH,
                ).start()

            @pl.when(jnp.logical_and(condition, owner == r))
            def _():
                pltpu.make_async_copy(source, target, r_sem.at[at]).start()

    def inner(o):
        taking = sum(o * per + j >= GROUPZ - EDGE for j in range(per))
        free_count = per - taking
        return jnp.where(low, 0, taking), free_count, jnp.where(low, free_count, 0), taking

    def await_far(source_chip, i):
        less = trim // 2 if i == PIECES - 1 else 0
        part = recv.at[pl.ds(2 * source_chip, 2), :, pl.ds(cut[i], cut[i + 1] - cut[i] - less)]
        pltpu.make_async_copy(part, part, r_sem.at[came(source_chip, i)]).wait()

    def await_own():
        part = recv.at[pl.ds(2 * chip, 2), :, pl.ds(0, half - trim // 2)]
        pltpu.make_async_copy(part, part, r_sem.at[0]).wait()

    def send_far(i):
        @pl.when(sends_to(far_side))
        def _():
            pltpu.make_async_remote_copy(
                src_ref=edge_send.at[far_side, :, rows_of(i)], dst_ref=far_recv.at[:, rows_of(i)],
                send_sem=es_sem.at[0], recv_sem=far_sem.at[i],
                device_id=(g + 1 - 2 * far_side, r), device_id_type=MESH,
            ).start()

    near_slot = r % 2 if direct else 0
    near_target = near_owner if direct else r

    def send_near(i):
        @pl.when(sends_to(near_side))
        def _():
            pltpu.make_async_remote_copy(
                src_ref=edge_send.at[near_side, :, rows_of(i)],
                dst_ref=near_recv.at[near_slot, :, rows_of(i)],
                send_sem=es_sem.at[1], recv_sem=near_sem.at[i],
                device_id=(g + 1 - 2 * near_side, near_target), device_id_type=MESH,
            ).start()

    def add_edge(side, source, i):
        for p in range(EDGE):
            q = p + jnp.where(side == 0, 0, GROUPZ - EDGE)
            owner, j = q // per, q % per
            a, b = cut[i], cut[i + 1]
            blend[owner, j, a:b] = (
                blend[owner, j, a:b].astype(jnp.float32) + source[p, a:b].astype(jnp.float32)
            ).astype(jnp.bfloat16)

    lerps(coef_lead, 0, cut[1], start_solo, lead_start, lead_rows)
    weights(0, cut[1], start_solo)
    await_piece(lead, load_sem.at[2])
    for z in range(0, depth, LOADZ):
        part = pl.ds(z, min(LOADZ, depth - z))
        pltpu.make_async_copy(tile_ref.at[0, part], raw.at[part], load_sem.at[1]).start()
    not_far = jnp.logical_not(gets_far)
    first_when = True if far_free else not_far
    blend_owner(first_owner, 0, cut[1], (lead, head_start, head_planes - 2, coef_lead))
    pl.semaphore_wait(barrier, greeted)
    send(first_owner, 0, first_when)

    @pl.when(jnp.logical_and(has_below, low))
    def _():
        pl.semaphore_signal(above_sem, inc=1, device_id=(g - 1, r), device_id_type=MESH)

    if direct:
        @pl.when(jnp.logical_and(has_above, high))
        def _():
            pl.semaphore_signal(below_sem, inc=1, device_id=(g + 1, r), device_id_type=MESH)

    for at, count, start in parts:
        lerps(coef, at, count, start, 0, tile_rows)
    weights(cut[1], MAIN - cut[1], start_solo + cut[1])
    for at, count, start in parts[1:]:
        weights(at, count, start)
    await_piece(head, load_sem.at[0])
    blend_owner(first_owner, cut[1], frame, (head, head_start, head_planes - 2, coef))
    for i in range(1, PIECES - 1):
        send(first_owner, i, first_when)
    swap_copy(first_owner * per, per, 0).start()

    await_piece(raw.at[pl.ds(0, depth)], load_sem.at[1])
    blend_edge(far_side)
    swap_copy(edge_slot(far_side), EDGE, 0).start()
    for i in range(PIECES - 1):
        send_far(i)

    for at in range(1, len(far_list)):
        owner = far_owner(at)
        blend_owner(owner)
        swap_copy(owner * per, per, 1).start()

    await_piece(got.at[pl.ds(0, per + EDGE)], got_sem.at[0])
    join_owner(first_owner)
    send(first_owner, PIECES - 1, first_when)
    join_edge(far_side)
    send_far(PIECES - 1)
    for at in range(1, len(far_list)):
        owner = far_owner(at)
        for i in range(PIECES - 1):
            if at < len(far_free):
                send(owner, i)
            else:
                send(owner, i, not_far)
                start, count, _, _ = inner(far_list[at])
                if count:
                    send(owner, i, gets_far, start, count)

    for o in near_list:
        owner = mirrored(o)
        blend_owner(owner)
        swap_copy(owner * per, per, 1).start()
    blend_edge(near_side)
    swap_copy(edge_slot(near_side), EDGE, 1).start()
    if direct:
        @pl.when(jnp.logical_not(takes_near))
        def _():
            near_recv[...] = jnp.zeros_like(near_recv)

    rec[...] = jnp.zeros_like(rec)
    for k in range(n):
        s = frame_start(k)
        totals = [0.0] * per
        for delta in (-1, 0, 1):
            group = jnp.clip(g + delta, 0, groups - 1)
            exists = jnp.where(group == g + delta, 1.0, 0.0)
            z0 = offs[0, group * n + k]
            ahead = jnp.clip(offs[1, group * n + k] - s, 0, frame - tile_rows)
            wy = table[pl.ds(PADY - ahead, frame), :]
            for j in range(per):
                z = g * GROUPZ + r * per + j - z0
                totals[j] = totals[j] + wy * (rampz_at(z) * exists)
        for j in range(per):
            rec[j, s : s + frame] = rec[j, s : s + frame] + totals[j]
    rec[...] = 1.0 / jnp.maximum(rec[...], weight_floor)

    await_piece(got.at[pl.ds(0, GROUPZ - per + EDGE)], got_sem.at[1])
    for at in range(1, len(far_list)):
        owner = far_owner(at)
        join_owner(owner)
        if at < len(far_free):
            send(owner, PIECES - 1)
        else:
            send(owner, PIECES - 1, not_far)
            start, count, _, _ = inner(far_list[at])
            if count:
                send(owner, PIECES - 1, gets_far, start, count)
    for o in near_list:
        owner = mirrored(o)
        join_owner(owner)
        for i in range(PIECES):
            send(owner, i, True if direct or o in near_free else jnp.logical_not(gets_near))
    join_edge(near_side)

    @pl.when(jnp.logical_and(has_above, low))
    def _():
        pl.semaphore_wait(above_sem, 1)

    if direct:
        @pl.when(jnp.logical_and(has_below, high))
        def _():
            pl.semaphore_wait(below_sem, 1)

    for i in range(PIECES):
        @pl.when(gets_far)
        def _():
            await_piece(far_recv.at[:, rows_of(i)], far_sem.at[i])
            add_edge(far_side, far_recv, i)
            for o in far_bound:
                _, _, start, count = inner(o)
                send(mirrored(o), i, True, start, count)

        if i == 0:
            @pl.when(sends_to(far_side))
            def _():
                await_piece(far_recv, es_sem.at[0])
                pl.semaphore_signal(
                    clear_sem, inc=1, device_id=(g, partner), device_id_type=MESH
                )
                pl.semaphore_wait(clear_sem, 1)

        send_near(i)

    if not direct:
        @pl.when(gets_near)
        def _():
            for i in range(PIECES):
                await_piece(near_recv.at[0, :, rows_of(i)], near_sem.at[i])
                add_edge(near_side, near_recv.at[0], i)
                for o in near_bound:
                    send(mirrored(o), i)

    def spans(k, i):
        solo_at = pair_start(k // 2) + (k % 2) * (SOLO + 2 * shared)
        shared_at = pair_start(k // 2) + SOLO + (k % 2) * shared
        if i < PIECES - 1:
            return [(solo_at + cut[i], solo_at + cut[i + 1], solo_at)]
        end = solo_at + SOLO - (k % 2) * trim
        return [
            (shared_at, shared_at + shared, shared_at - MAIN),
            (solo_at + MAIN, end, solo_at - shared),
        ]

    segments = [(k, i, *span) for k in range(n) for i in range(PIECES) for span in spans(k, i)]
    marks = sorted({min(end, rows) for item in segments for end in item[2:4]})
    intervals = [
        (a, b, [(k, i, at) for k, i, lo, hi, at in segments if lo < b and hi > a])
        for a, b in zip(marks[:-1], marks[1:])
    ]

    def finish(a, b, pieces, own=None, first=0):
        total = 0.0
        for k, i, at in pieces:
            total = total + recv[k, :, a - at : b - at].astype(jnp.float32)
            if k // 2 == own:
                edge = near_recv[k % 2, :, a - at : b - at].astype(jnp.float32)
                blank = [jnp.zeros((count, b - a, cols), jnp.float32) for count in (first, per - EDGE - first)]
                kept = [part for part in (blank[0], edge, blank[1]) if part.shape[0]]
                total = total + jnp.concatenate(kept, axis=0)
        value = (total * rec[:, a:b]).astype(jnp.bfloat16)
        out_ref[a:b] = jnp.swapaxes(value, 0, 1)

    if direct:
        for own in range(2):
            @pl.when(chip == own)
            def _():
                left = list(intervals)
                here = set()
                await_own()
                for i in range(PIECES):
                    @pl.when(takes_near)
                    def _():
                        await_piece(near_recv.at[:, :, rows_of(i)], near_sem.at[i])

                    for source in (own, 1 - own):
                        if source != own:
                            await_far(source, i)
                        here |= {(2 * source, i), (2 * source + 1, i)}
                        for item in list(left):
                            if all((k, j) in here for k, j, _ in item[2]):
                                left.remove(item)
                                finish(*item, own, 0 if own == 0 else per - EDGE)
    else:
        await_own()
        for away in range(1, pairs):
            for i in range(PIECES):
                await_far(lax.rem(chip + away, pairs), i)
        for item in intervals:
            finish(*item)

    await_piece(give, give_sem)
    for is_odd in (False, True):
        @pl.when(odd == is_odd)
        def _():
            await_piece(blend.at[pl.ds(0, n - 1), :, pl.ds(0, half - is_odd * trim)], s_sem)

    @pl.when(sends_to(near_side))
    def _():
        await_piece(far_recv, es_sem.at[1])


def solution(mesh):
    groups, n = mesh.shape["slab"], mesh.shape["tile"]

    def shards(tiles, offsets, fracs):
        _, depth, tile_rows, cols = tiles.shape
        per = GROUPZ // n
        rows = (n - 1) * STEPY + tile_rows
        reach = max(
            min(k * STEPY + JITY, rows - tile_rows) + tile_rows - frame_start(k) for k in range(n)
        )
        shared = round_up(max(reach - SOLO, 16), 16) // 2
        frame, half = SOLO + 2 * shared, SOLO + shared
        trim = min(frame - reach, SOLO - MAIN - 4) // 4 * 4
        acc_rows = round_up(max(rows, frame_start(n - 1) + frame), 16)
        head = per + 2 * JIT + 1
        lead = round_up(MAIN // (PIECES - 1) + frame - tile_rows + 8, 16)
        bf16, f32 = jnp.bfloat16, jnp.float32
        dma, signal = pltpu.SemaphoreType.DMA, pltpu.SemaphoreType.REGULAR
        slots = GROUPZ + 2 * EDGE
        joined = pl.pallas_call(
            functools.partial(kernel, groups, n, per, depth, tile_rows, shared, trim),
            out_shape=pltpu.VMEM((rows, per, cols), bf16),
            in_specs=[pl.BlockSpec(memory_space=pl.ANY)] * 3,
            out_specs=pl.BlockSpec(memory_space=pltpu.VMEM),
            scratch_shapes=[
                pltpu.VMEM((head, lead, cols), bf16),
                pltpu.VMEM((head, tile_rows, cols), bf16),
                pltpu.VMEM((depth + 1, tile_rows, cols), bf16),
                pltpu.VMEM((frame, 2 * tile_rows), bf16),
                pltpu.VMEM((SOLO, 2 * lead), bf16),
                pltpu.VMEM((frame, cols), f32),
                pltpu.VMEM((frame, cols), f32),
                pltpu.VMEM((n, per, half, cols), bf16),
                pltpu.VMEM((slots, shared, cols), f32),
                pltpu.VMEM((slots, shared, cols), bf16),
                pltpu.VMEM((slots, shared, cols), bf16),
                pltpu.VMEM((2, EDGE, half, cols), bf16),
                pltpu.VMEM((EDGE, half, cols), bf16),
                pltpu.VMEM((2, EDGE, half, cols), bf16),
                pltpu.VMEM((n, per, half, cols), bf16),
                pltpu.VMEM((per, acc_rows, cols), f32),
                pltpu.SMEM((offsets.shape[1], offsets.shape[0]), jnp.int32),
                pltpu.SMEM((fracs.shape[1], fracs.shape[0]), jnp.int32),
                pltpu.SMEM((depth + 2,), f32),
                pltpu.VMEM((round_up(PADY + frame + 8, 8), cols), f32),
                dma((2,)), dma((3,)), dma, dma((2,)), dma((2,)),
                dma((PIECES,)), dma((PIECES,)), dma, dma(((n // 2 - 1) * PIECES + 1,)),
                signal, signal, signal,
            ],
            compiler_params=pltpu.CompilerParams(collective_id=0, has_side_effects=True),
        )(offsets.T, fracs.T, tiles)
        return jnp.transpose(joined, (1, 0, 2))

    in_specs = (P(("slab", "tile"), None, None, None), P(), P())
    out_specs = P(("slab", "tile"), None, None)
    return jax.shard_map(shards, mesh=mesh, in_specs=in_specs, out_specs=out_specs, check_vma=False)
```

```python
import functools

import jax
import jax.numpy as jnp
import numpy as np
from jax import lax
from jax.experimental import pallas as pl
from jax.experimental.pallas import tpu as pltpu
from jax.sharding import PartitionSpec as P

GROUPZ = 16
MARGIN = 2
JIT = 1
STEPY = 230
JITY = 4
RY = 26
RX = 16
QUANT = 16
EDGE = MARGIN + JIT
PADY = 32
PIECES = 3
LOADZ = 4

weight_floor = 0.05
MESH = pl.DeviceIdType.MESH


def ramp(length, ramp_width):
    position = np.arange(length, dtype=np.float64)
    rising = 0.5 - 0.5 * np.cos(np.pi * (position + 1.0) / (ramp_width + 1.0))
    rising = np.where(position < ramp_width, rising, 1.0)
    return np.minimum(rising, rising[::-1])


def ramp_at(position, length, ramp_width):
    inward = jnp.minimum(position, length - 1 - position)
    t = (inward + 1).astype(jnp.float32) * float(np.pi / 2 / (ramp_width + 1.0))
    square = t * t
    sine = jnp.full(t.shape, 1.0 / 6227020800.0, jnp.float32)
    for term in (-39916800.0, 362880.0, -5040.0, 120.0, -6.0, 1.0):
        sine = sine * square + 1.0 / term
    sine = sine * t
    value = jnp.where(inward < ramp_width, sine * sine, 1.0)
    return jnp.where(inward < 0, 0.0, value)


def round_up(value, step):
    return -(-value // step) * step


SOLO = STEPY // 8 * 8
MAIN = SOLO - 8
FIRST = MAIN // 24 * 8
DETOUR = 32


def pair_start(pair):
    if isinstance(pair, int):
        return max(2 * pair * STEPY - JITY, 0) // 8 * 8
    return jnp.maximum(2 * pair * STEPY - JITY, 0) // 8 * 8


def frame_start(rank):
    return pair_start(rank // 2) + SOLO * (rank % 2)


def kernel(
    groups, n, per, depth, tile_rows, shared, trim, stride,
    offs_ref, fracs_ref, tile_ref, out_ref,
    lead, head, raw, coef, coef_lead, wa, wb, blend, own_sh, give, got,
    edge_send, far_recv, near_recv, recv, relay, rec,
    offs, fracs, rampz, table,
    small_sem, load_sem, give_sem, got_sem, es_sem, far_sem, near_sem, s_sem, r_sem, relay_sem,
    above_sem, below_sem, clear_sem,
):
    g = lax.axis_index("slab")
    r = lax.axis_index("tile")
    me = g * n + r
    chip = r // 2
    pairs = n // 2
    low = r < n // 2
    high = jnp.logical_not(low)
    odd = r % 2 == 1
    partner = r + 1 - 2 * (r % 2)
    cols = raw.shape[2]
    last = n - 1
    frame = SOLO + 2 * shared
    half = SOLO + shared
    rows = out_ref.shape[0]
    cut = [0, FIRST, MAIN, half]
    direct = pairs == 2

    barrier = pltpu.get_barrier_semaphore()
    has_below = g > 0
    has_above = g < groups - 1
    for i in range(1, n):
        pl.semaphore_signal(
            barrier, inc=1, device_id=(g, lax.rem(r + i, n)), device_id_type=MESH
        )

    @pl.when(has_above)
    def _():
        pl.semaphore_signal(barrier, inc=1, device_id=(g + 1, r), device_id_type=MESH)

    @pl.when(jnp.logical_and(has_below, high))
    def _():
        pl.semaphore_signal(barrier, inc=1, device_id=(g - 1, r), device_id_type=MESH)

    detour = direct and groups > stride
    relays = jnp.logical_and(g == stride, odd)
    source = jnp.logical_and(g == 0, jnp.logical_and(high, odd)) if detour else False
    if detour:
        @pl.when(jnp.logical_and(relays, high))
        def _():
            pl.semaphore_signal(barrier, inc=1, device_id=(0, r), device_id_type=MESH)

    greeted = n - 1 + jnp.where(has_below, 1, 0) + jnp.where(jnp.logical_and(has_above, high), 1, 0)
    if detour:
        greeted = greeted + jnp.where(source, 1, 0)
    far_side = jnp.where(low, 1, 0)
    near_side = 1 - far_side

    def sends_to(side):
        return jnp.where(side == 0, g < groups - 1, g > 0)

    def gets_from(side):
        return jnp.where(side == 0, g > 0, g < groups - 1)

    gets_far = gets_from(far_side)
    gets_near = gets_from(near_side)

    def mirrored(owner):
        return jnp.where(low, owner, last - owner)

    edge_planes = list(range(EDGE)) + list(range(GROUPZ - EDGE, GROUPZ))
    bound = sorted({q // per for q in edge_planes}, reverse=True)
    free = [o for o in range(last, -1, -1) if o not in bound]
    far_free = [o for o in free if o >= n // 2]
    far_bound = [o for o in bound if o >= n // 2]
    near_free = [o for o in free if o < n // 2]
    near_bound = [o for o in bound if o < n // 2]
    far_list = far_free + far_bound
    near_list = near_free + near_bound
    near_owner = mirrored(near_bound[-1])
    takes_near = jnp.logical_and(gets_near, r == near_owner)

    def far_owner(i):
        return mirrored(jnp.where(gets_far, far_list[i], far_list[-1 - i]))

    offs_load = pltpu.make_async_copy(offs_ref, offs, small_sem.at[0])
    fracs_load = pltpu.make_async_copy(fracs_ref, fracs, small_sem.at[1])
    first_owner = far_owner(0)
    head_planes = head.shape[0]
    head_start = jnp.minimum(first_owner * per + MARGIN - JIT, depth - head_planes)
    lead_rows = lead.shape[1]
    lead_start = jnp.where(odd, max(2 * shared - (frame - tile_rows), 0) // 8 * 8, 0)
    head_part = pl.ds(head_start, head_planes)
    pltpu.make_async_copy(
        tile_ref.at[0, head_part, pl.ds(pl.multiple_of(lead_start, 8), lead_rows)],
        lead, load_sem.at[2],
    ).start()
    offs_load.start()
    fracs_load.start()
    pltpu.make_async_copy(tile_ref.at[0, head_part], head, load_sem.at[0]).start()

    def await_piece(part, sem):
        pltpu.make_async_copy(part, part, sem).wait()

    raw[depth] = jnp.zeros(raw.shape[1:], raw.dtype)

    for at, value in enumerate([0.0, *ramp(depth, 2 * MARGIN), 0.0]):
        rampz[at] = jnp.float32(value)
    row = lax.broadcasted_iota(jnp.int32, table.shape, 0) - PADY
    col = lax.broadcasted_iota(jnp.int32, (8, cols), 1)
    table[...] = ramp_at(row, tile_rows, RY) * ramp_at(col, cols, RX)[:1]

    def rampz_at(z):
        return rampz[jnp.clip(z, -1, depth) + 1]

    offs_load.wait()
    fracs_load.wait()
    corner = offs[0, me]
    shift = jnp.clip(offs[1, me] - frame_start(r), 0, frame - tile_rows)
    base = g * GROUPZ - corner
    fz = fracs[0, me].astype(jnp.float32) / QUANT
    fy = fracs[1, me].astype(jnp.float32) / QUANT
    fx = fracs[2, me].astype(jnp.float32) / QUANT
    start_solo = jnp.where(odd, 2 * shared, 0)
    start_own = jnp.where(odd, shared, SOLO)
    start_give = jnp.where(odd, 0, half)
    parts = [
        (0, MAIN, start_solo), (MAIN, shared, start_own),
        (MAIN + shared, SOLO - MAIN, start_solo + MAIN), (half, shared, start_give),
    ]
    def lerps(target, at, count, start, first_col, width):
        row = lax.broadcasted_iota(jnp.int32, (count, width), 0)
        col = lax.broadcasted_iota(jnp.int32, (count, width), 1)
        behind = col - row + (shift - start + first_col)
        lerp_y = jnp.where(behind == 0, 1.0 - fy, jnp.where(behind == 1, fy, 0.0))
        target[at : at + count, :width] = ((1.0 - fz) * lerp_y).astype(jnp.bfloat16)
        target[at : at + count, width:] = (fz * lerp_y).astype(jnp.bfloat16)

    def weights(at, count, start):
        weight = table[pl.ds(PADY + start - shift, count), :]
        lane = lax.broadcasted_iota(jnp.int32, (count, cols), 1)
        wa[at : at + count] = weight * (1.0 - fx)
        wb[at : at + count] = jnp.where(lane < cols - 1, weight * fx, 0.0)

    def planes(store, source, source_start, limit, factors, first, count, lo, hi):
        at = [jnp.clip(first + j, 0, depth - 1) - source_start for j in range(count)]
        at = [jnp.clip(z, 0, limit) for z in at]
        top = jnp.concatenate([source[z] for z in at], axis=1)
        bottom = jnp.concatenate([source[z + 1] for z in at], axis=1)
        mixed = jnp.dot(
            factors[lo:hi], jnp.concatenate([top, bottom], axis=0),
            preferred_element_type=jnp.float32,
        )
        for j in range(count):
            part = mixed[:, j * cols : (j + 1) * cols]
            value = part * wa[lo:hi] + pltpu.roll(part, cols - 1, 1) * wb[lo:hi]
            store(j, value * rampz_at(first + j))

    def blend_rows(target, at, start, slot, where_from, first, count, lo, hi):
        def store(j, value):
            top = min(hi, MAIN)
            if lo < top:
                target[at, start + j, lo:top] = value[: top - lo].astype(jnp.bfloat16)
            if hi > MAIN:
                own_sh[slot + j] = value[MAIN - lo : MAIN + shared - lo]
                target[at, start + j, MAIN + shared : half] = value[
                    MAIN + shared - lo : half - lo
                ].astype(jnp.bfloat16)
                give[slot + j] = value[half - lo :].astype(jnp.bfloat16)

        planes(store, *where_from, first, count, lo, hi)

    whole = (raw, 0, depth - 1, coef)

    def blend_owner(owner, lo=0, hi=frame, where_from=whole, j=0, count=per):
        first = owner * per + j
        blend_rows(blend, owner, j, first, where_from, base + first, count, lo, hi)

    def edge_slot(side):
        return GROUPZ + side * EDGE

    def blend_edge(side):
        first = base + jnp.where(side == 0, GROUPZ, -EDGE)
        blend_rows(edge_send, side, 0, edge_slot(side), whole, first, EDGE, 0, frame)

    def swap_copy(slot, count, at):
        part = pl.ds(slot, count)
        return pltpu.make_async_remote_copy(
            src_ref=give.at[part], dst_ref=got.at[part],
            send_sem=give_sem, recv_sem=got_sem.at[at],
            device_id=(g, partner), device_id_type=MESH,
        )

    def joined_rows(slot):
        return (own_sh[slot] + got[slot].astype(jnp.float32)).astype(jnp.bfloat16)

    def join_owner(owner):
        for j in range(per):
            blend[owner, j, MAIN : MAIN + shared] = joined_rows(owner * per + j)

    def join_edge(side):
        for p in range(EDGE):
            edge_send[side, p, MAIN : MAIN + shared] = joined_rows(edge_slot(side) + p)

    def rows_of(i):
        return pl.ds(cut[i], cut[i + 1] - cut[i])

    def came(source_chip, i):
        away = lax.rem(source_chip - chip + pairs, pairs)
        return jnp.where(away == 0, 0, 1 + (away - 1) * PIECES + i)

    def send(owner, i, when=True, start=0, count=per, less=0):
        there = owner // 2
        away = lax.rem(chip - there + pairs, pairs)
        at = jnp.where(away == 0, 0, 1 + (away - 1) * PIECES + i)
        shapes = [(when, less)] if i < PIECES - 1 else [
            (jnp.logical_and(when, jnp.logical_not(odd)), 0), (jnp.logical_and(when, odd), trim)
        ]
        for condition, fewer in shapes:
            part = pl.ds(cut[i], cut[i + 1] - cut[i] - fewer)
            held = blend.at[owner, pl.ds(start, count), part]
            target = recv.at[r, pl.ds(start, count), part]

            @pl.when(jnp.logical_and(condition, owner != r))
            def _():
                pltpu.make_async_remote_copy(
                    src_ref=held, dst_ref=target, send_sem=s_sem, recv_sem=r_sem.at[at],
                    device_id=(g, owner), device_id_type=MESH,
                ).start()

            @pl.when(jnp.logical_and(condition, owner == r))
            def _():
                pltpu.make_async_copy(held, target, r_sem.at[at]).start()

    def inner(o):
        taking = sum(o * per + j >= GROUPZ - EDGE for j in range(per))
        free_count = per - taking
        return jnp.where(low, 0, taking), free_count, jnp.where(low, free_count, 0), taking

    def await_far(source_chip, i):
        less = trim // 2 if i == PIECES - 1 else 0
        part = recv.at[pl.ds(2 * source_chip, 2), :, pl.ds(cut[i], cut[i + 1] - cut[i] - less)]
        pltpu.make_async_copy(part, part, r_sem.at[came(source_chip, i)]).wait()

    def await_own():
        part = recv.at[pl.ds(2 * chip, 2), :, pl.ds(0, half - trim // 2)]
        pltpu.make_async_copy(part, part, r_sem.at[0]).wait()

    def send_far(i):
        @pl.when(sends_to(far_side))
        def _():
            pltpu.make_async_remote_copy(
                src_ref=edge_send.at[far_side, :, rows_of(i)], dst_ref=far_recv.at[:, rows_of(i)],
                send_sem=es_sem.at[0], recv_sem=far_sem.at[i],
                device_id=(g + 1 - 2 * far_side, r), device_id_type=MESH,
            ).start()

    near_slot = r % 2 if direct else 0
    near_target = near_owner if direct else r

    def send_near(i):
        @pl.when(sends_to(near_side))
        def _():
            pltpu.make_async_remote_copy(
                src_ref=edge_send.at[near_side, :, rows_of(i)],
                dst_ref=near_recv.at[near_slot, :, rows_of(i)],
                send_sem=es_sem.at[1], recv_sem=near_sem.at[i],
                device_id=(g + 1 - 2 * near_side, near_target), device_id_type=MESH,
            ).start()

    def add_edge(side, source, i):
        for p in range(EDGE):
            q = p + jnp.where(side == 0, 0, GROUPZ - EDGE)
            owner, j = q // per, q % per
            a, b = cut[i], cut[i + 1]
            blend[owner, j, a:b] = (
                blend[owner, j, a:b].astype(jnp.float32) + source[p, a:b].astype(jnp.float32)
            ).astype(jnp.bfloat16)

    lerps(coef_lead, 0, cut[1], start_solo, lead_start, lead_rows)
    weights(0, cut[1], start_solo)
    await_piece(lead, load_sem.at[2])
    for z in range(0, depth, LOADZ):
        part = pl.ds(z, min(LOADZ, depth - z))
        pltpu.make_async_copy(tile_ref.at[0, part], raw.at[part], load_sem.at[1]).start()
    not_far = jnp.logical_not(gets_far)
    first_when = True if far_free else not_far
    blend_owner(first_owner, 0, cut[1], (lead, head_start, head_planes - 2, coef_lead))
    pl.semaphore_wait(barrier, greeted)
    send(first_owner, 0, first_when)

    @pl.when(jnp.logical_and(has_below, low))
    def _():
        pl.semaphore_signal(above_sem, inc=1, device_id=(g - 1, r), device_id_type=MESH)

    if direct:
        @pl.when(jnp.logical_and(has_above, high))
        def _():
            pl.semaphore_signal(below_sem, inc=1, device_id=(g + 1, r), device_id_type=MESH)

    for at, count, start in parts:
        lerps(coef, at, count, start, 0, tile_rows)
    weights(cut[1], MAIN - cut[1], start_solo + cut[1])
    for at, count, start in parts[1:]:
        weights(at, count, start)
    await_piece(head, load_sem.at[0])
    blend_owner(first_owner, cut[1], frame, (head, head_start, head_planes - 2, coef))
    if detour:
        @pl.when(source)
        def _():
            pltpu.make_async_remote_copy(
                src_ref=blend.at[first_owner, :, pl.ds(MAIN - DETOUR, DETOUR)], dst_ref=relay,
                send_sem=s_sem, recv_sem=relay_sem.at[0],
                device_id=(stride, r), device_id_type=MESH,
            ).start()

        send(first_owner, 1, source, less=DETOUR)
        send(first_owner, 1, jnp.logical_not(source))
    else:
        for i in range(1, PIECES - 1):
            send(first_owner, i, first_when)
    swap_copy(first_owner * per, per, 0).start()

    await_piece(raw.at[pl.ds(0, depth)], load_sem.at[1])
    blend_edge(far_side)
    swap_copy(edge_slot(far_side), EDGE, 0).start()
    for i in range(PIECES - 1):
        send_far(i)

    for at in range(1, len(far_list)):
        owner = far_owner(at)
        blend_owner(owner)
        swap_copy(owner * per, per, 1).start()

    await_piece(got.at[pl.ds(0, per + EDGE)], got_sem.at[0])
    join_owner(first_owner)
    send(first_owner, PIECES - 1, first_when)
    join_edge(far_side)
    send_far(PIECES - 1)
    for at in range(1, len(far_list)):
        owner = far_owner(at)
        for i in range(PIECES - 1):
            if at < len(far_free):
                send(owner, i)
            else:
                send(owner, i, not_far)
                start, count, _, _ = inner(far_list[at])
                if count:
                    send(owner, i, gets_far, start, count)

    for o in near_list:
        owner = mirrored(o)
        blend_owner(owner)
        swap_copy(owner * per, per, 1).start()
    blend_edge(near_side)
    swap_copy(edge_slot(near_side), EDGE, 1).start()
    if direct:
        @pl.when(jnp.logical_not(takes_near))
        def _():
            near_recv[...] = jnp.zeros_like(near_recv)

    if detour:
        @pl.when(jnp.logical_and(relays, high))
        def _():
            await_piece(relay, relay_sem.at[0])
            pltpu.make_async_remote_copy(
                src_ref=relay, dst_ref=relay, send_sem=relay_sem.at[1], recv_sem=relay_sem.at[0],
                device_id=(g, r - n // 2), device_id_type=MESH,
            ).start()

    rec[...] = jnp.zeros_like(rec)
    for k in range(n):
        s = frame_start(k)
        totals = [0.0] * per
        for delta in (-1, 0, 1):
            group = jnp.clip(g + delta, 0, groups - 1)
            exists = jnp.where(group == g + delta, 1.0, 0.0)
            z0 = offs[0, group * n + k]
            ahead = jnp.clip(offs[1, group * n + k] - s, 0, frame - tile_rows)
            wy = table[pl.ds(PADY - ahead, frame), :]
            for j in range(per):
                z = g * GROUPZ + r * per + j - z0
                totals[j] = totals[j] + wy * (rampz_at(z) * exists)
        for j in range(per):
            rec[j, s : s + frame] = rec[j, s : s + frame] + totals[j]
    rec[...] = 1.0 / jnp.maximum(rec[...], weight_floor)

    await_piece(got.at[pl.ds(0, GROUPZ - per + EDGE)], got_sem.at[1])
    for at in range(1, len(far_list)):
        owner = far_owner(at)
        join_owner(owner)
        if at < len(far_free):
            send(owner, PIECES - 1)
        else:
            send(owner, PIECES - 1, not_far)
            start, count, _, _ = inner(far_list[at])
            if count:
                send(owner, PIECES - 1, gets_far, start, count)
    for o in near_list:
        owner = mirrored(o)
        join_owner(owner)
        for i in range(PIECES):
            send(owner, i, True if direct or o in near_free else jnp.logical_not(gets_near))
    join_edge(near_side)

    @pl.when(jnp.logical_and(has_above, low))
    def _():
        pl.semaphore_wait(above_sem, 1)

    if direct:
        @pl.when(jnp.logical_and(has_below, high))
        def _():
            pl.semaphore_wait(below_sem, 1)

    for i in range(PIECES):
        @pl.when(gets_far)
        def _():
            await_piece(far_recv.at[:, rows_of(i)], far_sem.at[i])
            add_edge(far_side, far_recv, i)
            for o in far_bound:
                _, _, start, count = inner(o)
                send(mirrored(o), i, True, start, count)

        if i == 0:
            @pl.when(sends_to(far_side))
            def _():
                await_piece(far_recv, es_sem.at[0])
                pl.semaphore_signal(
                    clear_sem, inc=1, device_id=(g, partner), device_id_type=MESH
                )
                pl.semaphore_wait(clear_sem, 1)

        send_near(i)

    if not direct:
        @pl.when(gets_near)
        def _():
            for i in range(PIECES):
                await_piece(near_recv.at[0, :, rows_of(i)], near_sem.at[i])
                add_edge(near_side, near_recv.at[0], i)
                for o in near_bound:
                    send(mirrored(o), i)

    if detour:
        @pl.when(jnp.logical_and(relays, low))
        def _():
            await_piece(relay, relay_sem.at[0])
            pltpu.make_async_remote_copy(
                src_ref=relay, dst_ref=recv.at[r + n // 2, :, pl.ds(MAIN - DETOUR, DETOUR)],
                send_sem=relay_sem.at[1], recv_sem=r_sem.at[2],
                device_id=(0, 0), device_id_type=MESH,
            ).start()

    def spans(k, i):
        solo_at = pair_start(k // 2) + (k % 2) * (SOLO + 2 * shared)
        shared_at = pair_start(k // 2) + SOLO + (k % 2) * shared
        if i < PIECES - 1:
            return [(solo_at + cut[i], solo_at + cut[i + 1], solo_at)]
        end = solo_at + SOLO - (k % 2) * trim
        return [
            (shared_at, shared_at + shared, shared_at - MAIN),
            (solo_at + MAIN, end, solo_at - shared),
        ]

    segments = [(k, i, *span) for k in range(n) for i in range(PIECES) for span in spans(k, i)]
    marks = sorted({min(end, rows) for item in segments for end in item[2:4]})
    intervals = [
        (a, b, [(k, i, at) for k, i, lo, hi, at in segments if lo < b and hi > a])
        for a, b in zip(marks[:-1], marks[1:])
    ]

    def finish(a, b, pieces, own=None, first=0):
        total = 0.0
        for k, i, at in pieces:
            total = total + recv[k, :, a - at : b - at].astype(jnp.float32)
            if k // 2 == own:
                edge = near_recv[k % 2, :, a - at : b - at].astype(jnp.float32)
                blank = [jnp.zeros((count, b - a, cols), jnp.float32) for count in (first, per - EDGE - first)]
                kept = [part for part in (blank[0], edge, blank[1]) if part.shape[0]]
                total = total + jnp.concatenate(kept, axis=0)
        value = (total * rec[:, a:b]).astype(jnp.bfloat16)
        out_ref[a:b] = jnp.swapaxes(value, 0, 1)

    if direct:
        for own in range(2):
            @pl.when(chip == own)
            def _():
                left = list(intervals)
                here = set()
                await_own()
                for i in range(PIECES):
                    @pl.when(takes_near)
                    def _():
                        await_piece(near_recv.at[:, :, rows_of(i)], near_sem.at[i])

                    for source in (own, 1 - own):
                        if source != own:
                            await_far(source, i)
                        here |= {(2 * source, i), (2 * source + 1, i)}
                        for item in list(left):
                            if all((k, j) in here for k, j, _ in item[2]):
                                left.remove(item)
                                finish(*item, own, 0 if own == 0 else per - EDGE)
    else:
        await_own()
        for away in range(1, pairs):
            for i in range(PIECES):
                await_far(lax.rem(chip + away, pairs), i)
        for item in intervals:
            finish(*item)

    if detour:
        @pl.when(relays)
        def _():
            await_piece(relay, relay_sem.at[1])

    await_piece(give, give_sem)
    for is_odd in (False, True):
        @pl.when(odd == is_odd)
        def _():
            await_piece(blend.at[pl.ds(0, n - 1), :, pl.ds(0, half - is_odd * trim)], s_sem)

    @pl.when(sends_to(near_side))
    def _():
        await_piece(far_recv, es_sem.at[1])


def solution(mesh):
    groups, n = mesh.shape["slab"], mesh.shape["tile"]
    stride = len({getattr(d, "coords", (i % 2,))[0] for i, d in enumerate(mesh.devices.flat)})

    def shards(tiles, offsets, fracs):
        _, depth, tile_rows, cols = tiles.shape
        per = GROUPZ // n
        rows = (n - 1) * STEPY + tile_rows
        reach = max(
            min(k * STEPY + JITY, rows - tile_rows) + tile_rows - frame_start(k) for k in range(n)
        )
        shared = round_up(max(reach - SOLO, 16), 16) // 2
        frame, half = SOLO + 2 * shared, SOLO + shared
        trim = min(frame - reach, SOLO - MAIN - 4) // 4 * 4
        acc_rows = round_up(max(rows, frame_start(n - 1) + frame), 16)
        head = per + 2 * JIT + 1
        lead = round_up(FIRST + frame - tile_rows + 8, 16)
        bf16, f32 = jnp.bfloat16, jnp.float32
        dma, signal = pltpu.SemaphoreType.DMA, pltpu.SemaphoreType.REGULAR
        slots = GROUPZ + 2 * EDGE
        joined = pl.pallas_call(
            functools.partial(
                kernel, groups, n, per, depth, tile_rows, shared, trim, stride
            ),
            out_shape=pltpu.VMEM((rows, per, cols), bf16),
            in_specs=[pl.BlockSpec(memory_space=pl.ANY)] * 3,
            out_specs=pl.BlockSpec(memory_space=pltpu.VMEM),
            scratch_shapes=[
                pltpu.VMEM((head, lead, cols), bf16),
                pltpu.VMEM((head, tile_rows, cols), bf16),
                pltpu.VMEM((depth + 1, tile_rows, cols), bf16),
                pltpu.VMEM((frame, 2 * tile_rows), bf16),
                pltpu.VMEM((SOLO, 2 * lead), bf16),
                pltpu.VMEM((frame, cols), f32),
                pltpu.VMEM((frame, cols), f32),
                pltpu.VMEM((n, per, half, cols), bf16),
                pltpu.VMEM((slots, shared, cols), f32),
                pltpu.VMEM((slots, shared, cols), bf16),
                pltpu.VMEM((slots, shared, cols), bf16),
                pltpu.VMEM((2, EDGE, half, cols), bf16),
                pltpu.VMEM((EDGE, half, cols), bf16),
                pltpu.VMEM((2, EDGE, half, cols), bf16),
                pltpu.VMEM((n, per, half, cols), bf16),
                pltpu.VMEM((per, DETOUR, cols), bf16),
                pltpu.VMEM((per, acc_rows, cols), f32),
                pltpu.SMEM((offsets.shape[1], offsets.shape[0]), jnp.int32),
                pltpu.SMEM((fracs.shape[1], fracs.shape[0]), jnp.int32),
                pltpu.SMEM((depth + 2,), f32),
                pltpu.VMEM((round_up(PADY + frame + 8, 8), cols), f32),
                dma((2,)), dma((3,)), dma, dma((2,)), dma((2,)),
                dma((PIECES,)), dma((PIECES,)), dma, dma(((n // 2 - 1) * PIECES + 1,)), dma((2,)),
                signal, signal, signal,
            ],
            compiler_params=pltpu.CompilerParams(collective_id=0, has_side_effects=True),
        )(offsets.T, fracs.T, tiles)
        return jnp.transpose(joined, (1, 0, 2))

    in_specs = (P(("slab", "tile"), None, None, None), P(), P())
    out_specs = P(("slab", "tile"), None, None)
    return jax.shard_map(shards, mesh=mesh, in_specs=in_specs, out_specs=out_specs, check_vma=False)
```

```python
import functools

import jax
import jax.numpy as jnp
import numpy as np
from jax import lax
from jax.experimental import pallas as pl
from jax.experimental.pallas import tpu as pltpu
from jax.sharding import PartitionSpec as P

GROUPZ = 16
MARGIN = 2
JIT = 1
STEPY = 230
JITY = 4
RY = 26
RX = 16
QUANT = 16
EDGE = MARGIN + JIT
PADY = 32
PIECES = 3

weight_floor = 0.05
MESH = pl.DeviceIdType.MESH


def ramp(length, ramp_width):
    position = np.arange(length, dtype=np.float64)
    rising = 0.5 - 0.5 * np.cos(np.pi * (position + 1.0) / (ramp_width + 1.0))
    rising = np.where(position < ramp_width, rising, 1.0)
    return np.minimum(rising, rising[::-1])


def ramp_at(position, length, ramp_width):
    inward = jnp.minimum(position, length - 1 - position)
    t = (inward + 1).astype(jnp.float32) * float(np.pi / 2 / (ramp_width + 1.0))
    square = t * t
    sine = jnp.full(t.shape, 1.0 / 6227020800.0, jnp.float32)
    for term in (-39916800.0, 362880.0, -5040.0, 120.0, -6.0, 1.0):
        sine = sine * square + 1.0 / term
    sine = sine * t
    value = jnp.where(inward < ramp_width, sine * sine, 1.0)
    return jnp.where(inward < 0, 0.0, value)


def round_up(value, step):
    return -(-value // step) * step


SOLO = STEPY // 8 * 8
MAIN = SOLO - 8
FIRST = MAIN // 24 * 8
DETOUR = 40


def pair_start(pair):
    if isinstance(pair, int):
        return max(2 * pair * STEPY - JITY, 0) // 8 * 8
    return jnp.maximum(2 * pair * STEPY - JITY, 0) // 8 * 8


def frame_start(rank):
    return pair_start(rank // 2) + SOLO * (rank % 2)


def kernel(
    groups, n, per, depth, tile_rows, shared, trim, stride,
    offs_ref, fracs_ref, tile_ref, out_ref,
    lead, raw, coef, coef_lead, wa, wb, blend, own_sh, give, got,
    edge_send, far_recv, near_recv, recv, relay, rec,
    offs, fracs, rampz, table,
    small_sem, load_sem, give_sem, got_sem, es_sem, far_sem, near_sem, s_sem, r_sem, relay_sem,
    above_sem, below_sem, clear_sem,
):
    g = lax.axis_index("slab")
    r = lax.axis_index("tile")
    me = g * n + r
    chip = r // 2
    pairs = n // 2
    low = r < n // 2
    high = jnp.logical_not(low)
    odd = r % 2 == 1
    partner = r + 1 - 2 * (r % 2)
    cols = raw.shape[2]
    last = n - 1
    frame = SOLO + 2 * shared
    half = SOLO + shared
    rows = out_ref.shape[0]
    cut = [0, FIRST, MAIN, half]
    direct = pairs == 2

    barrier = pltpu.get_barrier_semaphore()
    has_below = g > 0
    has_above = g < groups - 1
    for i in range(1, n):
        pl.semaphore_signal(
            barrier, inc=1, device_id=(g, lax.rem(r + i, n)), device_id_type=MESH
        )

    @pl.when(has_above)
    def _():
        pl.semaphore_signal(barrier, inc=1, device_id=(g + 1, r), device_id_type=MESH)

    @pl.when(jnp.logical_and(has_below, high))
    def _():
        pl.semaphore_signal(barrier, inc=1, device_id=(g - 1, r), device_id_type=MESH)

    detour = direct and groups > stride
    relays = jnp.logical_and(g == stride, odd)
    source_rank = n // 2
    source = jnp.logical_and(g == 0, r == source_rank) if detour else False
    if detour:
        @pl.when(jnp.logical_and(relays, high))
        def _():
            pl.semaphore_signal(barrier, inc=1, device_id=(0, source_rank), device_id_type=MESH)

    greeted = n - 1 + jnp.where(has_below, 1, 0) + jnp.where(jnp.logical_and(has_above, high), 1, 0)
    if detour:
        greeted = greeted + jnp.where(source, 1, 0)
    far_side = jnp.where(low, 1, 0)
    near_side = 1 - far_side

    def sends_to(side):
        return jnp.where(side == 0, g < groups - 1, g > 0)

    def gets_from(side):
        return jnp.where(side == 0, g > 0, g < groups - 1)

    gets_far = gets_from(far_side)
    gets_near = gets_from(near_side)

    def mirrored(owner):
        return jnp.where(low, owner, last - owner)

    edge_planes = list(range(EDGE)) + list(range(GROUPZ - EDGE, GROUPZ))
    bound = sorted({q // per for q in edge_planes}, reverse=True)
    free = [o for o in range(last, -1, -1) if o not in bound]
    far_free = [o for o in free if o >= n // 2]
    far_bound = [o for o in bound if o >= n // 2]
    near_free = [o for o in free if o < n // 2]
    near_bound = [o for o in bound if o < n // 2]
    far_list = far_free + far_bound
    near_list = near_free + near_bound
    near_owner = mirrored(near_bound[-1])
    takes_near = jnp.logical_and(gets_near, r == near_owner)

    def far_owner(i):
        return mirrored(jnp.where(gets_far, far_list[i], far_list[-1 - i]))

    offs_load = pltpu.make_async_copy(offs_ref, offs, small_sem.at[0])
    fracs_load = pltpu.make_async_copy(fracs_ref, fracs, small_sem.at[1])
    first_owner = far_owner(0)
    head_planes = lead.shape[0]
    head_start = jnp.minimum(first_owner * per + MARGIN - JIT, depth - head_planes)
    lead_rows = lead.shape[1]
    lead_start = jnp.where(odd, max(2 * shared - (frame - tile_rows), 0) // 8 * 8, 0)
    head_part = pl.ds(head_start, head_planes)
    pltpu.make_async_copy(
        tile_ref.at[0, head_part, pl.ds(pl.multiple_of(lead_start, 8), lead_rows)],
        lead, load_sem.at[0],
    ).start()
    offs_load.start()
    fracs_load.start()
    pltpu.make_async_copy(tile_ref.at[0], raw.at[pl.ds(0, depth)], load_sem.at[1]).start()

    def await_piece(part, sem):
        pltpu.make_async_copy(part, part, sem).wait()

    raw[depth] = jnp.zeros(raw.shape[1:], raw.dtype)

    for at, value in enumerate([0.0, *ramp(depth, 2 * MARGIN), 0.0]):
        rampz[at] = jnp.float32(value)
    row = lax.broadcasted_iota(jnp.int32, table.shape, 0) - PADY
    col = lax.broadcasted_iota(jnp.int32, (8, cols), 1)
    table[...] = ramp_at(row, tile_rows, RY) * ramp_at(col, cols, RX)[:1]

    def rampz_at(z):
        return rampz[jnp.clip(z, -1, depth) + 1]

    offs_load.wait()
    fracs_load.wait()
    corner = offs[0, me]
    shift = jnp.clip(offs[1, me] - frame_start(r), 0, frame - tile_rows)
    base = g * GROUPZ - corner
    fz = fracs[0, me].astype(jnp.float32) / QUANT
    fy = fracs[1, me].astype(jnp.float32) / QUANT
    fx = fracs[2, me].astype(jnp.float32) / QUANT
    start_solo = jnp.where(odd, 2 * shared, 0)
    start_own = jnp.where(odd, shared, SOLO)
    start_give = jnp.where(odd, 0, half)
    parts = [
        (0, MAIN, start_solo), (MAIN, shared, start_own),
        (MAIN + shared, SOLO - MAIN, start_solo + MAIN), (half, shared, start_give),
    ]
    def lerps(target, at, count, start, first_col, width):
        row = lax.broadcasted_iota(jnp.int32, (count, width), 0)
        col = lax.broadcasted_iota(jnp.int32, (count, width), 1)
        behind = col - row + (shift - start + first_col)
        lerp_y = jnp.where(behind == 0, 1.0 - fy, jnp.where(behind == 1, fy, 0.0))
        target[at : at + count, :width] = ((1.0 - fz) * lerp_y).astype(jnp.bfloat16)
        target[at : at + count, width:] = (fz * lerp_y).astype(jnp.bfloat16)

    def weights(at, count, start):
        weight = table[pl.ds(PADY + start - shift, count), :]
        lane = lax.broadcasted_iota(jnp.int32, (count, cols), 1)
        wa[at : at + count] = weight * (1.0 - fx)
        wb[at : at + count] = jnp.where(lane < cols - 1, weight * fx, 0.0)

    def planes(store, source, source_start, limit, factors, first, count, lo, hi):
        at = [jnp.clip(first + j, 0, depth - 1) - source_start for j in range(count)]
        at = [jnp.clip(z, 0, limit) for z in at]
        top = jnp.concatenate([source[z] for z in at], axis=1)
        bottom = jnp.concatenate([source[z + 1] for z in at], axis=1)
        mixed = jnp.dot(
            factors[lo:hi], jnp.concatenate([top, bottom], axis=0),
            preferred_element_type=jnp.float32,
        )
        for j in range(count):
            part = mixed[:, j * cols : (j + 1) * cols]
            value = part * wa[lo:hi] + pltpu.roll(part, cols - 1, 1) * wb[lo:hi]
            store(j, value * rampz_at(first + j))

    def blend_rows(target, at, start, slot, where_from, first, count, lo, hi):
        def store(j, value):
            top = min(hi, MAIN)
            if lo < top:
                target[at, start + j, lo:top] = value[: top - lo].astype(jnp.bfloat16)
            if hi > MAIN:
                own_sh[slot + j] = value[MAIN - lo : MAIN + shared - lo]
                target[at, start + j, MAIN + shared : half] = value[
                    MAIN + shared - lo : half - lo
                ].astype(jnp.bfloat16)
                give[slot + j] = value[half - lo :].astype(jnp.bfloat16)

        planes(store, *where_from, first, count, lo, hi)

    whole = (raw, 0, depth - 1, coef)

    def blend_owner(owner, lo=0, hi=frame, where_from=whole, j=0, count=per):
        first = owner * per + j
        blend_rows(blend, owner, j, first, where_from, base + first, count, lo, hi)

    def edge_slot(side):
        return GROUPZ + side * EDGE

    def blend_edge(side):
        first = base + jnp.where(side == 0, GROUPZ, -EDGE)
        blend_rows(edge_send, side, 0, edge_slot(side), whole, first, EDGE, 0, frame)

    def swap_copy(slot, count, at):
        part = pl.ds(slot, count)
        return pltpu.make_async_remote_copy(
            src_ref=give.at[part], dst_ref=got.at[part],
            send_sem=give_sem, recv_sem=got_sem.at[at],
            device_id=(g, partner), device_id_type=MESH,
        )

    def joined_rows(slot):
        return (own_sh[slot] + got[slot].astype(jnp.float32)).astype(jnp.bfloat16)

    def join_owner(owner):
        for j in range(per):
            blend[owner, j, MAIN : MAIN + shared] = joined_rows(owner * per + j)

    def join_edge(side):
        for p in range(EDGE):
            edge_send[side, p, MAIN : MAIN + shared] = joined_rows(edge_slot(side) + p)

    def rows_of(i):
        return pl.ds(cut[i], cut[i + 1] - cut[i])

    def came(source_chip, i):
        away = lax.rem(source_chip - chip + pairs, pairs)
        return jnp.where(away == 0, 0, 1 + (away - 1) * PIECES + i)

    def send(owner, i, when=True, start=0, count=per, less=0):
        there = owner // 2
        away = lax.rem(chip - there + pairs, pairs)
        at = jnp.where(away == 0, 0, 1 + (away - 1) * PIECES + i)
        shapes = [(when, less)] if i < PIECES - 1 else [
            (jnp.logical_and(when, jnp.logical_not(odd)), 0), (jnp.logical_and(when, odd), trim)
        ]
        for condition, fewer in shapes:
            part = pl.ds(cut[i], cut[i + 1] - cut[i] - fewer)
            held = blend.at[owner, pl.ds(start, count), part]
            target = recv.at[r, pl.ds(start, count), part]

            @pl.when(jnp.logical_and(condition, owner != r))
            def _():
                pltpu.make_async_remote_copy(
                    src_ref=held, dst_ref=target, send_sem=s_sem, recv_sem=r_sem.at[at],
                    device_id=(g, owner), device_id_type=MESH,
                ).start()

            @pl.when(jnp.logical_and(condition, owner == r))
            def _():
                pltpu.make_async_copy(held, target, r_sem.at[at]).start()

    def inner(o):
        taking = sum(o * per + j >= GROUPZ - EDGE for j in range(per))
        free_count = per - taking
        return jnp.where(low, 0, taking), free_count, jnp.where(low, free_count, 0), taking

    def await_far(source_chip, i):
        less = trim // 2 if i == PIECES - 1 else 0
        part = recv.at[pl.ds(2 * source_chip, 2), :, pl.ds(cut[i], cut[i + 1] - cut[i] - less)]
        pltpu.make_async_copy(part, part, r_sem.at[came(source_chip, i)]).wait()

    def await_own():
        part = recv.at[pl.ds(2 * chip, 2), :, pl.ds(0, half - trim // 2)]
        pltpu.make_async_copy(part, part, r_sem.at[0]).wait()

    def send_far(i):
        @pl.when(sends_to(far_side))
        def _():
            pltpu.make_async_remote_copy(
                src_ref=edge_send.at[far_side, :, rows_of(i)], dst_ref=far_recv.at[:, rows_of(i)],
                send_sem=es_sem.at[0], recv_sem=far_sem.at[i],
                device_id=(g + 1 - 2 * far_side, r), device_id_type=MESH,
            ).start()

    near_slot = r % 2 if direct else 0
    near_target = near_owner if direct else r

    def send_near(i):
        @pl.when(sends_to(near_side))
        def _():
            pltpu.make_async_remote_copy(
                src_ref=edge_send.at[near_side, :, rows_of(i)],
                dst_ref=near_recv.at[near_slot, :, rows_of(i)],
                send_sem=es_sem.at[1], recv_sem=near_sem.at[i],
                device_id=(g + 1 - 2 * near_side, near_target), device_id_type=MESH,
            ).start()

    def add_edge(side, source, i):
        for p in range(EDGE):
            q = p + jnp.where(side == 0, 0, GROUPZ - EDGE)
            owner, j = q // per, q % per
            a, b = cut[i], cut[i + 1]
            blend[owner, j, a:b] = (
                blend[owner, j, a:b].astype(jnp.float32) + source[p, a:b].astype(jnp.float32)
            ).astype(jnp.bfloat16)

    lerps(coef_lead, 0, cut[1], start_solo, lead_start, lead_rows)
    weights(0, cut[1], start_solo)
    await_piece(lead, load_sem.at[0])
    not_far = jnp.logical_not(gets_far)
    first_when = True if far_free else not_far
    held_back = jnp.logical_and(jnp.logical_and(high, odd), gets_far) if direct else False
    blend_owner(first_owner, 0, cut[1], (lead, head_start, head_planes - 2, coef_lead))
    pl.semaphore_wait(barrier, greeted)
    send(first_owner, 0, first_when)

    @pl.when(jnp.logical_and(has_below, low))
    def _():
        pl.semaphore_signal(above_sem, inc=1, device_id=(g - 1, r), device_id_type=MESH)

    if direct:
        @pl.when(jnp.logical_and(has_above, high))
        def _():
            pl.semaphore_signal(below_sem, inc=1, device_id=(g + 1, r), device_id_type=MESH)

    for at, count, start in parts:
        lerps(coef, at, count, start, 0, tile_rows)
    weights(cut[1], MAIN - cut[1], start_solo + cut[1])
    for at, count, start in parts[1:]:
        weights(at, count, start)
    await_piece(raw.at[pl.ds(0, depth)], load_sem.at[1])
    blend_owner(first_owner, cut[1], frame)
    if detour:
        @pl.when(source)
        def _():
            pltpu.make_async_remote_copy(
                src_ref=blend.at[first_owner, :, pl.ds(MAIN - DETOUR, DETOUR)], dst_ref=relay,
                send_sem=s_sem, recv_sem=relay_sem.at[0],
                device_id=(stride, source_rank + 1), device_id_type=MESH,
            ).start()

        send(first_owner, 1, source, less=DETOUR)
        send(first_owner, 1, jnp.logical_not(source))
    else:
        for i in range(1, PIECES - 1):
            send(first_owner, i, first_when)
    swap_copy(first_owner * per, per, 0).start()

    blend_edge(far_side)
    swap_copy(edge_slot(far_side), EDGE, 0).start()
    for i in range(PIECES - 1):
        send_far(i)

    for at in range(1, len(far_list)):
        owner = far_owner(at)
        blend_owner(owner)
        swap_copy(owner * per, per, 1).start()

    await_piece(got.at[pl.ds(0, per + EDGE)], got_sem.at[0])
    join_owner(first_owner)
    send(first_owner, PIECES - 1, jnp.logical_and(first_when, jnp.logical_not(held_back)))
    join_edge(far_side)
    send_far(PIECES - 1)
    for at in range(1, len(far_list)):
        owner = far_owner(at)
        for i in range(PIECES - 1):
            if at < len(far_free):
                send(owner, i)
            else:
                send(owner, i, not_far)
                start, count, _, _ = inner(far_list[at])
                if count:
                    send(owner, i, gets_far, start, count)

    for o in near_list:
        owner = mirrored(o)
        blend_owner(owner)
        swap_copy(owner * per, per, 1).start()
    blend_edge(near_side)
    swap_copy(edge_slot(near_side), EDGE, 1).start()
    if direct:
        @pl.when(jnp.logical_not(takes_near))
        def _():
            near_recv[...] = jnp.zeros_like(near_recv)

    if detour:
        @pl.when(jnp.logical_and(relays, high))
        def _():
            await_piece(relay, relay_sem.at[0])
            pltpu.make_async_remote_copy(
                src_ref=relay, dst_ref=relay, send_sem=relay_sem.at[1], recv_sem=relay_sem.at[0],
                device_id=(g, r - n // 2), device_id_type=MESH,
            ).start()

    rec[...] = jnp.zeros_like(rec)
    for k in range(n):
        s = frame_start(k)
        totals = [0.0] * per
        for delta in (-1, 0, 1):
            group = jnp.clip(g + delta, 0, groups - 1)
            exists = jnp.where(group == g + delta, 1.0, 0.0)
            z0 = offs[0, group * n + k]
            ahead = jnp.clip(offs[1, group * n + k] - s, 0, frame - tile_rows)
            wy = table[pl.ds(PADY - ahead, frame), :]
            for j in range(per):
                z = g * GROUPZ + r * per + j - z0
                totals[j] = totals[j] + wy * (rampz_at(z) * exists)
        for j in range(per):
            rec[j, s : s + frame] = rec[j, s : s + frame] + totals[j]
    rec[...] = 1.0 / jnp.maximum(rec[...], weight_floor)

    await_piece(got.at[pl.ds(0, GROUPZ - per + EDGE)], got_sem.at[1])
    for at in range(1, len(far_list)):
        owner = far_owner(at)
        join_owner(owner)
        if at < len(far_free):
            send(owner, PIECES - 1)
        else:
            send(owner, PIECES - 1, not_far)
            start, count, _, _ = inner(far_list[at])
            if count:
                send(owner, PIECES - 1, gets_far, start, count)
    for o in near_list:
        owner = mirrored(o)
        join_owner(owner)
        for i in range(PIECES):
            send(owner, i, True if direct or o in near_free else jnp.logical_not(gets_near))
    join_edge(near_side)

    @pl.when(jnp.logical_and(has_above, low))
    def _():
        pl.semaphore_wait(above_sem, 1)

    if direct:
        @pl.when(jnp.logical_and(has_below, high))
        def _():
            pl.semaphore_wait(below_sem, 1)

    for i in range(PIECES):
        @pl.when(gets_far)
        def _():
            await_piece(far_recv.at[:, rows_of(i)], far_sem.at[i])
            add_edge(far_side, far_recv, i)
            for o in far_bound:
                _, _, start, count = inner(o)
                send(mirrored(o), i, True, start, count)

        if i == 0:
            @pl.when(sends_to(far_side))
            def _():
                await_piece(far_recv, es_sem.at[0])
                pl.semaphore_signal(
                    clear_sem, inc=1, device_id=(g, partner), device_id_type=MESH
                )
                pl.semaphore_wait(clear_sem, 1)

        send_near(i)

    if direct:
        send(first_owner, PIECES - 1, held_back)
    else:
        @pl.when(gets_near)
        def _():
            for i in range(PIECES):
                await_piece(near_recv.at[0, :, rows_of(i)], near_sem.at[i])
                add_edge(near_side, near_recv.at[0], i)
                for o in near_bound:
                    send(mirrored(o), i)

    if detour:
        @pl.when(jnp.logical_and(relays, low))
        def _():
            await_piece(relay, relay_sem.at[0])
            pltpu.make_async_remote_copy(
                src_ref=relay, dst_ref=recv.at[source_rank, :, pl.ds(MAIN - DETOUR, DETOUR)],
                send_sem=relay_sem.at[1], recv_sem=r_sem.at[2],
                device_id=(0, 0), device_id_type=MESH,
            ).start()

    def spans(k, i):
        solo_at = pair_start(k // 2) + (k % 2) * (SOLO + 2 * shared)
        shared_at = pair_start(k // 2) + SOLO + (k % 2) * shared
        if i < PIECES - 1:
            return [(solo_at + cut[i], solo_at + cut[i + 1], solo_at)]
        end = solo_at + SOLO - (k % 2) * trim
        return [
            (shared_at, shared_at + shared, shared_at - MAIN),
            (solo_at + MAIN, end, solo_at - shared),
        ]

    segments = [(k, i, *span) for k in range(n) for i in range(PIECES) for span in spans(k, i)]
    marks = sorted({min(end, rows) for item in segments for end in item[2:4]})
    intervals = [
        (a, b, [(k, i, at) for k, i, lo, hi, at in segments if lo < b and hi > a])
        for a, b in zip(marks[:-1], marks[1:])
    ]

    def finish(a, b, pieces, own=None, first=0):
        total = 0.0
        for k, i, at in pieces:
            total = total + recv[k, :, a - at : b - at].astype(jnp.float32)
            if k // 2 == own:
                edge = near_recv[k % 2, :, a - at : b - at].astype(jnp.float32)
                blank = [jnp.zeros((count, b - a, cols), jnp.float32) for count in (first, per - EDGE - first)]
                kept = [part for part in (blank[0], edge, blank[1]) if part.shape[0]]
                total = total + jnp.concatenate(kept, axis=0)
        value = (total * rec[:, a:b]).astype(jnp.bfloat16)
        out_ref[a:b] = jnp.swapaxes(value, 0, 1)

    if direct:
        for own in range(2):
            @pl.when(chip == own)
            def _():
                left = list(intervals)
                here = set()
                await_own()
                for i in range(PIECES):
                    @pl.when(takes_near)
                    def _():
                        await_piece(near_recv.at[:, :, rows_of(i)], near_sem.at[i])

                    for source in (own, 1 - own):
                        if source != own:
                            await_far(source, i)
                        here |= {(2 * source, i), (2 * source + 1, i)}
                        for item in list(left):
                            if all((k, j) in here for k, j, _ in item[2]):
                                left.remove(item)
                                finish(*item, own, 0 if own == 0 else per - EDGE)
    else:
        await_own()
        for away in range(1, pairs):
            for i in range(PIECES):
                await_far(lax.rem(chip + away, pairs), i)
        for item in intervals:
            finish(*item)

    if detour:
        @pl.when(relays)
        def _():
            await_piece(relay, relay_sem.at[1])

    await_piece(give, give_sem)
    for is_odd in (False, True):
        @pl.when(odd == is_odd)
        def _():
            await_piece(blend.at[pl.ds(0, n - 1), :, pl.ds(0, half - is_odd * trim)], s_sem)

    @pl.when(sends_to(near_side))
    def _():
        await_piece(far_recv, es_sem.at[1])


def solution(mesh):
    groups, n = mesh.shape["slab"], mesh.shape["tile"]
    stride = len({getattr(d, "coords", (i % 2,))[0] for i, d in enumerate(mesh.devices.flat)})

    def shards(tiles, offsets, fracs):
        _, depth, tile_rows, cols = tiles.shape
        per = GROUPZ // n
        rows = (n - 1) * STEPY + tile_rows
        reach = max(
            min(k * STEPY + JITY, rows - tile_rows) + tile_rows - frame_start(k) for k in range(n)
        )
        shared = round_up(max(reach - SOLO, 16), 16) // 2
        frame, half = SOLO + 2 * shared, SOLO + shared
        trim = min(frame - reach, SOLO - MAIN - 4) // 4 * 4
        acc_rows = round_up(max(rows, frame_start(n - 1) + frame), 16)
        head = per + 2 * JIT + 1
        lead = round_up(FIRST + frame - tile_rows + 8, 16)
        bf16, f32 = jnp.bfloat16, jnp.float32
        dma, signal = pltpu.SemaphoreType.DMA, pltpu.SemaphoreType.REGULAR
        slots = GROUPZ + 2 * EDGE
        joined = pl.pallas_call(
            functools.partial(
                kernel, groups, n, per, depth, tile_rows, shared, trim, stride
            ),
            out_shape=pltpu.VMEM((rows, per, cols), bf16),
            in_specs=[pl.BlockSpec(memory_space=pl.ANY)] * 3,
            out_specs=pl.BlockSpec(memory_space=pltpu.VMEM),
            scratch_shapes=[
                pltpu.VMEM((head, lead, cols), bf16),
                pltpu.VMEM((depth + 1, tile_rows, cols), bf16),
                pltpu.VMEM((frame, 2 * tile_rows), bf16),
                pltpu.VMEM((SOLO, 2 * lead), bf16),
                pltpu.VMEM((frame, cols), f32),
                pltpu.VMEM((frame, cols), f32),
                pltpu.VMEM((n, per, half, cols), bf16),
                pltpu.VMEM((slots, shared, cols), f32),
                pltpu.VMEM((slots, shared, cols), bf16),
                pltpu.VMEM((slots, shared, cols), bf16),
                pltpu.VMEM((2, EDGE, half, cols), bf16),
                pltpu.VMEM((EDGE, half, cols), bf16),
                pltpu.VMEM((2, EDGE, half, cols), bf16),
                pltpu.VMEM((n, per, half, cols), bf16),
                pltpu.VMEM((per, DETOUR, cols), bf16),
                pltpu.VMEM((per, acc_rows, cols), f32),
                pltpu.SMEM((offsets.shape[1], offsets.shape[0]), jnp.int32),
                pltpu.SMEM((fracs.shape[1], fracs.shape[0]), jnp.int32),
                pltpu.SMEM((depth + 2,), f32),
                pltpu.VMEM((round_up(PADY + frame + 8, 8), cols), f32),
                dma((2,)), dma((2,)), dma, dma((2,)), dma((2,)),
                dma((PIECES,)), dma((PIECES,)), dma, dma(((n // 2 - 1) * PIECES + 1,)), dma((2,)),
                signal, signal, signal,
            ],
            compiler_params=pltpu.CompilerParams(collective_id=0, has_side_effects=True),
        )(offsets.T, fracs.T, tiles)
        return jnp.transpose(joined, (1, 0, 2))

    in_specs = (P(("slab", "tile"), None, None, None), P(), P())
    out_specs = P(("slab", "tile"), None, None)
    return jax.shard_map(shards, mesh=mesh, in_specs=in_specs, out_specs=out_specs, check_vma=False)
```

```python
import functools

import jax
import jax.numpy as jnp
import numpy as np
from jax import lax
from jax.experimental import pallas as pl
from jax.experimental.pallas import tpu as pltpu
from jax.sharding import PartitionSpec as P

GROUPZ = 16
MARGIN = 2
JIT = 1
STEPY = 230
JITY = 4
RY = 26
RX = 16
QUANT = 16
EDGE = MARGIN + JIT
PADY = 32
PIECES = 3

weight_floor = 0.05
MESH = pl.DeviceIdType.MESH


def ramp(length, ramp_width):
    position = np.arange(length, dtype=np.float64)
    rising = 0.5 - 0.5 * np.cos(np.pi * (position + 1.0) / (ramp_width + 1.0))
    rising = np.where(position < ramp_width, rising, 1.0)
    return np.minimum(rising, rising[::-1])


def ramp_at(position, length, ramp_width):
    inward = jnp.minimum(position, length - 1 - position)
    t = (inward + 1).astype(jnp.float32) * float(np.pi / 2 / (ramp_width + 1.0))
    square = t * t
    sine = jnp.full(t.shape, 1.0 / 6227020800.0, jnp.float32)
    for term in (-39916800.0, 362880.0, -5040.0, 120.0, -6.0, 1.0):
        sine = sine * square + 1.0 / term
    sine = sine * t
    value = jnp.where(inward < ramp_width, sine * sine, 1.0)
    return jnp.where(inward < 0, 0.0, value)


def round_up(value, step):
    return -(-value // step) * step


SOLO = STEPY // 8 * 8
MAIN = SOLO - 8
FIRST = MAIN // 24 * 8
DETOUR = 24


def pair_start(pair):
    if isinstance(pair, int):
        return max(2 * pair * STEPY - JITY, 0) // 8 * 8
    return jnp.maximum(2 * pair * STEPY - JITY, 0) // 8 * 8


def frame_start(rank):
    return pair_start(rank // 2) + SOLO * (rank % 2)


def kernel(
    groups, n, per, depth, tile_rows, shared, trim, stride,
    offs_ref, fracs_ref, tile_ref, out_ref,
    lead, raw, coef, coef_lead, wa, wb, blend, own_sh, give, got,
    edge_send, far_recv, near_recv, recv, relay, rec,
    offs, fracs, rampz, table,
    small_sem, load_sem, give_sem, got_sem, es_sem, far_sem, near_sem, s_sem, r_sem, relay_sem,
    above_sem, below_sem, clear_sem,
):
    g = lax.axis_index("slab")
    r = lax.axis_index("tile")
    me = g * n + r
    chip = r // 2
    pairs = n // 2
    low = r < n // 2
    high = jnp.logical_not(low)
    odd = r % 2 == 1
    partner = r + 1 - 2 * (r % 2)
    cols = raw.shape[2]
    last = n - 1
    frame = SOLO + 2 * shared
    half = SOLO + shared
    rows = out_ref.shape[0]
    cut = [0, FIRST, MAIN, half]
    direct = pairs == 2

    barrier = pltpu.get_barrier_semaphore()
    has_below = g > 0
    has_above = g < groups - 1
    for i in range(1, n):
        pl.semaphore_signal(
            barrier, inc=1, device_id=(g, lax.rem(r + i, n)), device_id_type=MESH
        )

    @pl.when(has_above)
    def _():
        pl.semaphore_signal(barrier, inc=1, device_id=(g + 1, r), device_id_type=MESH)

    @pl.when(jnp.logical_and(has_below, high))
    def _():
        pl.semaphore_signal(barrier, inc=1, device_id=(g - 1, r), device_id_type=MESH)

    routes = sorted({stride, 1}, reverse=True)
    detour = direct and groups > stride
    relays = jnp.logical_and(functools.reduce(jnp.logical_or, [g == at for at in routes]), odd)
    source_rank = n // 2
    source = jnp.logical_and(g == 0, r == source_rank) if detour else False
    if detour:
        @pl.when(jnp.logical_and(relays, high))
        def _():
            pl.semaphore_signal(barrier, inc=1, device_id=(0, source_rank), device_id_type=MESH)

    greeted = n - 1 + jnp.where(has_below, 1, 0) + jnp.where(jnp.logical_and(has_above, high), 1, 0)
    if detour:
        greeted = greeted + jnp.where(source, len(routes), 0)
    far_side = jnp.where(low, 1, 0)
    near_side = 1 - far_side

    def sends_to(side):
        return jnp.where(side == 0, g < groups - 1, g > 0)

    def gets_from(side):
        return jnp.where(side == 0, g > 0, g < groups - 1)

    gets_far = gets_from(far_side)
    gets_near = gets_from(near_side)

    def mirrored(owner):
        return jnp.where(low, owner, last - owner)

    edge_planes = list(range(EDGE)) + list(range(GROUPZ - EDGE, GROUPZ))
    bound = sorted({q // per for q in edge_planes}, reverse=True)
    free = [o for o in range(last, -1, -1) if o not in bound]
    far_free = [o for o in free if o >= n // 2]
    far_bound = [o for o in bound if o >= n // 2]
    near_free = [o for o in free if o < n // 2]
    near_bound = [o for o in bound if o < n // 2]
    far_list = far_free + far_bound
    near_list = near_free + near_bound
    near_owner = mirrored(near_bound[-1])
    takes_near = jnp.logical_and(gets_near, r == near_owner)

    def far_owner(i):
        return mirrored(jnp.where(gets_far, far_list[i], far_list[-1 - i]))

    offs_load = pltpu.make_async_copy(offs_ref, offs, small_sem.at[0])
    fracs_load = pltpu.make_async_copy(fracs_ref, fracs, small_sem.at[1])
    first_owner = far_owner(0)
    head_planes = lead.shape[0]
    head_start = jnp.minimum(first_owner * per + MARGIN - JIT, depth - head_planes)
    lead_rows = lead.shape[1]
    lead_start = jnp.where(odd, max(2 * shared - (frame - tile_rows), 0) // 8 * 8, 0)
    head_part = pl.ds(head_start, head_planes)
    pltpu.make_async_copy(
        tile_ref.at[0, head_part, pl.ds(pl.multiple_of(lead_start, 8), lead_rows)],
        lead, load_sem.at[0],
    ).start()
    offs_load.start()
    fracs_load.start()
    pltpu.make_async_copy(tile_ref.at[0], raw.at[pl.ds(0, depth)], load_sem.at[1]).start()

    def await_piece(part, sem):
        pltpu.make_async_copy(part, part, sem).wait()

    raw[depth] = jnp.zeros(raw.shape[1:], raw.dtype)

    for at, value in enumerate([0.0, *ramp(depth, 2 * MARGIN), 0.0]):
        rampz[at] = jnp.float32(value)
    row = lax.broadcasted_iota(jnp.int32, table.shape, 0) - PADY
    col = lax.broadcasted_iota(jnp.int32, (8, cols), 1)
    table[...] = ramp_at(row, tile_rows, RY) * ramp_at(col, cols, RX)[:1]

    def rampz_at(z):
        return rampz[jnp.clip(z, -1, depth) + 1]

    offs_load.wait()
    fracs_load.wait()
    corner = offs[0, me]
    shift = jnp.clip(offs[1, me] - frame_start(r), 0, frame - tile_rows)
    base = g * GROUPZ - corner
    fz = fracs[0, me].astype(jnp.float32) / QUANT
    fy = fracs[1, me].astype(jnp.float32) / QUANT
    fx = fracs[2, me].astype(jnp.float32) / QUANT
    start_solo = jnp.where(odd, 2 * shared, 0)
    start_own = jnp.where(odd, shared, SOLO)
    start_give = jnp.where(odd, 0, half)
    parts = [
        (0, MAIN, start_solo), (MAIN, shared, start_own),
        (MAIN + shared, SOLO - MAIN, start_solo + MAIN), (half, shared, start_give),
    ]
    def lerps(target, at, count, start, first_col, width):
        row = lax.broadcasted_iota(jnp.int32, (count, width), 0)
        col = lax.broadcasted_iota(jnp.int32, (count, width), 1)
        behind = col - row + (shift - start + first_col)
        lerp_y = jnp.where(behind == 0, 1.0 - fy, jnp.where(behind == 1, fy, 0.0))
        target[at : at + count, :width] = ((1.0 - fz) * lerp_y).astype(jnp.bfloat16)
        target[at : at + count, width:] = (fz * lerp_y).astype(jnp.bfloat16)

    def weights(at, count, start):
        weight = table[pl.ds(PADY + start - shift, count), :]
        lane = lax.broadcasted_iota(jnp.int32, (count, cols), 1)
        wa[at : at + count] = weight * (1.0 - fx)
        wb[at : at + count] = jnp.where(lane < cols - 1, weight * fx, 0.0)

    def planes(store, source, source_start, limit, factors, first, count, lo, hi):
        at = [jnp.clip(first + j, 0, depth - 1) - source_start for j in range(count)]
        at = [jnp.clip(z, 0, limit) for z in at]
        top = jnp.concatenate([source[z] for z in at], axis=1)
        bottom = jnp.concatenate([source[z + 1] for z in at], axis=1)
        mixed = jnp.dot(
            factors[lo:hi], jnp.concatenate([top, bottom], axis=0),
            preferred_element_type=jnp.float32,
        )
        for j in range(count):
            part = mixed[:, j * cols : (j + 1) * cols]
            value = part * wa[lo:hi] + pltpu.roll(part, cols - 1, 1) * wb[lo:hi]
            store(j, value * rampz_at(first + j))

    def blend_rows(target, at, start, slot, where_from, first, count, lo, hi):
        def store(j, value):
            top = min(hi, MAIN)
            if lo < top:
                target[at, start + j, lo:top] = value[: top - lo].astype(jnp.bfloat16)
            if hi > MAIN:
                own_sh[slot + j] = value[MAIN - lo : MAIN + shared - lo]
                target[at, start + j, MAIN + shared : half] = value[
                    MAIN + shared - lo : half - lo
                ].astype(jnp.bfloat16)
                give[slot + j] = value[half - lo :].astype(jnp.bfloat16)

        planes(store, *where_from, first, count, lo, hi)

    whole = (raw, 0, depth - 1, coef)

    def blend_owner(owner, lo=0, hi=frame, where_from=whole, j=0, count=per):
        first = owner * per + j
        blend_rows(blend, owner, j, first, where_from, base + first, count, lo, hi)

    def edge_slot(side):
        return GROUPZ + side * EDGE

    def blend_edge(side):
        first = base + jnp.where(side == 0, GROUPZ, -EDGE)
        blend_rows(edge_send, side, 0, edge_slot(side), whole, first, EDGE, 0, frame)

    def swap_copy(slot, count, at):
        part = pl.ds(slot, count)
        return pltpu.make_async_remote_copy(
            src_ref=give.at[part], dst_ref=got.at[part],
            send_sem=give_sem, recv_sem=got_sem.at[at],
            device_id=(g, partner), device_id_type=MESH,
        )

    def joined_rows(slot):
        return (own_sh[slot] + got[slot].astype(jnp.float32)).astype(jnp.bfloat16)

    def join_owner(owner):
        for j in range(per):
            blend[owner, j, MAIN : MAIN + shared] = joined_rows(owner * per + j)

    def join_edge(side):
        for p in range(EDGE):
            edge_send[side, p, MAIN : MAIN + shared] = joined_rows(edge_slot(side) + p)

    def rows_of(i):
        return pl.ds(cut[i], cut[i + 1] - cut[i])

    def came(source_chip, i):
        away = lax.rem(source_chip - chip + pairs, pairs)
        return jnp.where(away == 0, 0, 1 + (away - 1) * PIECES + i)

    def send(owner, i, when=True, start=0, count=per, less=0):
        there = owner // 2
        away = lax.rem(chip - there + pairs, pairs)
        at = jnp.where(away == 0, 0, 1 + (away - 1) * PIECES + i)
        shapes = [(when, less)] if i < PIECES - 1 else [
            (jnp.logical_and(when, jnp.logical_not(odd)), 0), (jnp.logical_and(when, odd), trim)
        ]
        for condition, fewer in shapes:
            part = pl.ds(cut[i], cut[i + 1] - cut[i] - fewer)
            held = blend.at[owner, pl.ds(start, count), part]
            target = recv.at[r, pl.ds(start, count), part]

            @pl.when(jnp.logical_and(condition, owner != r))
            def _():
                pltpu.make_async_remote_copy(
                    src_ref=held, dst_ref=target, send_sem=s_sem, recv_sem=r_sem.at[at],
                    device_id=(g, owner), device_id_type=MESH,
                ).start()

            @pl.when(jnp.logical_and(condition, owner == r))
            def _():
                pltpu.make_async_copy(held, target, r_sem.at[at]).start()

    def inner(o):
        taking = sum(o * per + j >= GROUPZ - EDGE for j in range(per))
        free_count = per - taking
        return jnp.where(low, 0, taking), free_count, jnp.where(low, free_count, 0), taking

    def await_far(source_chip, i):
        less = trim // 2 if i == PIECES - 1 else 0
        part = recv.at[pl.ds(2 * source_chip, 2), :, pl.ds(cut[i], cut[i + 1] - cut[i] - less)]
        pltpu.make_async_copy(part, part, r_sem.at[came(source_chip, i)]).wait()

    def await_own():
        part = recv.at[pl.ds(2 * chip, 2), :, pl.ds(0, half - trim // 2)]
        pltpu.make_async_copy(part, part, r_sem.at[0]).wait()

    def send_far(i):
        @pl.when(sends_to(far_side))
        def _():
            pltpu.make_async_remote_copy(
                src_ref=edge_send.at[far_side, :, rows_of(i)], dst_ref=far_recv.at[:, rows_of(i)],
                send_sem=es_sem.at[0], recv_sem=far_sem.at[i],
                device_id=(g + 1 - 2 * far_side, r), device_id_type=MESH,
            ).start()

    near_slot = r % 2 if direct else 0
    near_target = near_owner if direct else r

    def send_near(i):
        @pl.when(sends_to(near_side))
        def _():
            pltpu.make_async_remote_copy(
                src_ref=edge_send.at[near_side, :, rows_of(i)],
                dst_ref=near_recv.at[near_slot, :, rows_of(i)],
                send_sem=es_sem.at[1], recv_sem=near_sem.at[i],
                device_id=(g + 1 - 2 * near_side, near_target), device_id_type=MESH,
            ).start()

    def add_edge(side, source, i):
        for p in range(EDGE):
            q = p + jnp.where(side == 0, 0, GROUPZ - EDGE)
            owner, j = q // per, q % per
            a, b = cut[i], cut[i + 1]
            blend[owner, j, a:b] = (
                blend[owner, j, a:b].astype(jnp.float32) + source[p, a:b].astype(jnp.float32)
            ).astype(jnp.bfloat16)

    lerps(coef_lead, 0, cut[1], start_solo, lead_start, lead_rows)
    weights(0, cut[1], start_solo)
    await_piece(lead, load_sem.at[0])
    not_far = jnp.logical_not(gets_far)
    first_when = True if far_free else not_far
    held_back = jnp.logical_and(jnp.logical_and(high, odd), gets_far) if direct else False
    blend_owner(first_owner, 0, cut[1], (lead, head_start, head_planes - 2, coef_lead))
    pl.semaphore_wait(barrier, greeted)
    send(first_owner, 0, first_when)

    @pl.when(jnp.logical_and(has_below, low))
    def _():
        pl.semaphore_signal(above_sem, inc=1, device_id=(g - 1, r), device_id_type=MESH)

    if direct:
        @pl.when(jnp.logical_and(has_above, high))
        def _():
            pl.semaphore_signal(below_sem, inc=1, device_id=(g + 1, r), device_id_type=MESH)

    for at, count, start in parts:
        lerps(coef, at, count, start, 0, tile_rows)
    weights(cut[1], MAIN - cut[1], start_solo + cut[1])
    for at, count, start in parts[1:]:
        weights(at, count, start)
    await_piece(raw.at[pl.ds(0, depth)], load_sem.at[1])
    blend_owner(first_owner, cut[1], frame)
    if detour:
        @pl.when(source)
        def _():
            for i, at in enumerate(routes):
                part = pl.ds(MAIN - (i + 1) * DETOUR, DETOUR)
                pltpu.make_async_remote_copy(
                    src_ref=blend.at[first_owner, :, part], dst_ref=relay,
                    send_sem=s_sem, recv_sem=relay_sem.at[0],
                    device_id=(at, source_rank + 1), device_id_type=MESH,
                ).start()

        send(first_owner, 1, source, less=len(routes) * DETOUR)
        send(first_owner, 1, jnp.logical_not(source))
    else:
        for i in range(1, PIECES - 1):
            send(first_owner, i, first_when)
    swap_copy(first_owner * per, per, 0).start()

    blend_edge(far_side)
    swap_copy(edge_slot(far_side), EDGE, 0).start()
    for i in range(PIECES - 1):
        send_far(i)

    for at in range(1, len(far_list)):
        owner = far_owner(at)
        blend_owner(owner)
        swap_copy(owner * per, per, 1).start()

    await_piece(got.at[pl.ds(0, per + EDGE)], got_sem.at[0])
    join_owner(first_owner)
    send(first_owner, PIECES - 1, jnp.logical_and(first_when, jnp.logical_not(held_back)))
    join_edge(far_side)
    send_far(PIECES - 1)
    for at in range(1, len(far_list)):
        owner = far_owner(at)
        for i in range(PIECES - 1):
            if at < len(far_free):
                send(owner, i)
            else:
                send(owner, i, not_far)
                start, count, _, _ = inner(far_list[at])
                if count:
                    send(owner, i, gets_far, start, count)

    for o in near_list:
        owner = mirrored(o)
        blend_owner(owner)
        swap_copy(owner * per, per, 1).start()
    blend_edge(near_side)
    swap_copy(edge_slot(near_side), EDGE, 1).start()
    if direct:
        @pl.when(jnp.logical_not(takes_near))
        def _():
            near_recv[...] = jnp.zeros_like(near_recv)

    if detour:
        @pl.when(jnp.logical_and(relays, high))
        def _():
            await_piece(relay, relay_sem.at[0])
            pltpu.make_async_remote_copy(
                src_ref=relay, dst_ref=relay, send_sem=relay_sem.at[1], recv_sem=relay_sem.at[0],
                device_id=(g, r - n // 2), device_id_type=MESH,
            ).start()

    rec[...] = jnp.zeros_like(rec)
    for k in range(n):
        s = frame_start(k)
        totals = [0.0] * per
        for delta in (-1, 0, 1):
            group = jnp.clip(g + delta, 0, groups - 1)
            exists = jnp.where(group == g + delta, 1.0, 0.0)
            z0 = offs[0, group * n + k]
            ahead = jnp.clip(offs[1, group * n + k] - s, 0, frame - tile_rows)
            wy = table[pl.ds(PADY - ahead, frame), :]
            for j in range(per):
                z = g * GROUPZ + r * per + j - z0
                totals[j] = totals[j] + wy * (rampz_at(z) * exists)
        for j in range(per):
            rec[j, s : s + frame] = rec[j, s : s + frame] + totals[j]
    rec[...] = 1.0 / jnp.maximum(rec[...], weight_floor)

    await_piece(got.at[pl.ds(0, GROUPZ - per + EDGE)], got_sem.at[1])
    for at in range(1, len(far_list)):
        owner = far_owner(at)
        join_owner(owner)
        if at < len(far_free):
            send(owner, PIECES - 1)
        else:
            send(owner, PIECES - 1, not_far)
            start, count, _, _ = inner(far_list[at])
            if count:
                send(owner, PIECES - 1, gets_far, start, count)
    for o in near_list:
        owner = mirrored(o)
        join_owner(owner)
        for i in range(PIECES):
            send(owner, i, True if direct or o in near_free else jnp.logical_not(gets_near))
    join_edge(near_side)

    @pl.when(jnp.logical_and(has_above, low))
    def _():
        pl.semaphore_wait(above_sem, 1)

    if direct:
        @pl.when(jnp.logical_and(has_below, high))
        def _():
            pl.semaphore_wait(below_sem, 1)

    for i in range(PIECES):
        @pl.when(gets_far)
        def _():
            await_piece(far_recv.at[:, rows_of(i)], far_sem.at[i])
            add_edge(far_side, far_recv, i)
            for o in far_bound:
                _, _, start, count = inner(o)
                send(mirrored(o), i, True, start, count)

        if i == 0:
            @pl.when(sends_to(far_side))
            def _():
                await_piece(far_recv, es_sem.at[0])
                pl.semaphore_signal(
                    clear_sem, inc=1, device_id=(g, partner), device_id_type=MESH
                )
                pl.semaphore_wait(clear_sem, 1)

        send_near(i)

    if direct:
        send(first_owner, PIECES - 1, held_back)
    else:
        @pl.when(gets_near)
        def _():
            for i in range(PIECES):
                await_piece(near_recv.at[0, :, rows_of(i)], near_sem.at[i])
                add_edge(near_side, near_recv.at[0], i)
                for o in near_bound:
                    send(mirrored(o), i)

    if detour:
        @pl.when(jnp.logical_and(relays, low))
        def _():
            await_piece(relay, relay_sem.at[0])
            for i, at in enumerate(routes):
                @pl.when(g == at)
                def _():
                    part = pl.ds(MAIN - (i + 1) * DETOUR, DETOUR)
                    pltpu.make_async_remote_copy(
                        src_ref=relay, dst_ref=recv.at[source_rank, :, part],
                        send_sem=relay_sem.at[1], recv_sem=r_sem.at[2],
                        device_id=(0, 0), device_id_type=MESH,
                    ).start()

    def spans(k, i):
        solo_at = pair_start(k // 2) + (k % 2) * (SOLO + 2 * shared)
        shared_at = pair_start(k // 2) + SOLO + (k % 2) * shared
        if i < PIECES - 1:
            return [(solo_at + cut[i], solo_at + cut[i + 1], solo_at)]
        end = solo_at + SOLO - (k % 2) * trim
        return [
            (shared_at, shared_at + shared, shared_at - MAIN),
            (solo_at + MAIN, end, solo_at - shared),
        ]

    segments = [(k, i, *span) for k in range(n) for i in range(PIECES) for span in spans(k, i)]
    marks = sorted({min(end, rows) for item in segments for end in item[2:4]})
    intervals = [
        (a, b, [(k, i, at) for k, i, lo, hi, at in segments if lo < b and hi > a])
        for a, b in zip(marks[:-1], marks[1:])
    ]

    def finish(a, b, pieces, own=None, first=0):
        total = 0.0
        for k, i, at in pieces:
            total = total + recv[k, :, a - at : b - at].astype(jnp.float32)
            if k // 2 == own:
                edge = near_recv[k % 2, :, a - at : b - at].astype(jnp.float32)
                blank = [jnp.zeros((count, b - a, cols), jnp.float32) for count in (first, per - EDGE - first)]
                kept = [part for part in (blank[0], edge, blank[1]) if part.shape[0]]
                total = total + jnp.concatenate(kept, axis=0)
        value = (total * rec[:, a:b]).astype(jnp.bfloat16)
        out_ref[a:b] = jnp.swapaxes(value, 0, 1)

    if direct:
        for own in range(2):
            @pl.when(chip == own)
            def _():
                left = list(intervals)
                here = set()
                await_own()
                for i in range(PIECES):
                    @pl.when(takes_near)
                    def _():
                        await_piece(near_recv.at[:, :, rows_of(i)], near_sem.at[i])

                    for source in (own, 1 - own):
                        if source != own:
                            await_far(source, i)
                        here |= {(2 * source, i), (2 * source + 1, i)}
                        for item in list(left):
                            if all((k, j) in here for k, j, _ in item[2]):
                                left.remove(item)
                                finish(*item, own, 0 if own == 0 else per - EDGE)
    else:
        await_own()
        for away in range(1, pairs):
            for i in range(PIECES):
                await_far(lax.rem(chip + away, pairs), i)
        for item in intervals:
            finish(*item)

    if detour:
        @pl.when(relays)
        def _():
            await_piece(relay, relay_sem.at[1])

    await_piece(give, give_sem)
    for is_odd in (False, True):
        @pl.when(odd == is_odd)
        def _():
            await_piece(blend.at[pl.ds(0, n - 1), :, pl.ds(0, half - is_odd * trim)], s_sem)

    @pl.when(sends_to(near_side))
    def _():
        await_piece(far_recv, es_sem.at[1])


def solution(mesh):
    groups, n = mesh.shape["slab"], mesh.shape["tile"]
    stride = len({getattr(d, "coords", (i % 2,))[0] for i, d in enumerate(mesh.devices.flat)})

    def shards(tiles, offsets, fracs):
        _, depth, tile_rows, cols = tiles.shape
        per = GROUPZ // n
        rows = (n - 1) * STEPY + tile_rows
        reach = max(
            min(k * STEPY + JITY, rows - tile_rows) + tile_rows - frame_start(k) for k in range(n)
        )
        shared = round_up(max(reach - SOLO, 16), 16) // 2
        frame, half = SOLO + 2 * shared, SOLO + shared
        trim = min(frame - reach, SOLO - MAIN - 4) // 4 * 4
        acc_rows = round_up(max(rows, frame_start(n - 1) + frame), 16)
        head = per + 2 * JIT + 1
        lead = round_up(FIRST + frame - tile_rows + 8, 16)
        bf16, f32 = jnp.bfloat16, jnp.float32
        dma, signal = pltpu.SemaphoreType.DMA, pltpu.SemaphoreType.REGULAR
        slots = GROUPZ + 2 * EDGE
        joined = pl.pallas_call(
            functools.partial(
                kernel, groups, n, per, depth, tile_rows, shared, trim, stride
            ),
            out_shape=pltpu.VMEM((rows, per, cols), bf16),
            in_specs=[pl.BlockSpec(memory_space=pl.ANY)] * 3,
            out_specs=pl.BlockSpec(memory_space=pltpu.VMEM),
            scratch_shapes=[
                pltpu.VMEM((head, lead, cols), bf16),
                pltpu.VMEM((depth + 1, tile_rows, cols), bf16),
                pltpu.VMEM((frame, 2 * tile_rows), bf16),
                pltpu.VMEM((SOLO, 2 * lead), bf16),
                pltpu.VMEM((frame, cols), f32),
                pltpu.VMEM((frame, cols), f32),
                pltpu.VMEM((n, per, half, cols), bf16),
                pltpu.VMEM((slots, shared, cols), f32),
                pltpu.VMEM((slots, shared, cols), bf16),
                pltpu.VMEM((slots, shared, cols), bf16),
                pltpu.VMEM((2, EDGE, half, cols), bf16),
                pltpu.VMEM((EDGE, half, cols), bf16),
                pltpu.VMEM((2, EDGE, half, cols), bf16),
                pltpu.VMEM((n, per, half, cols), bf16),
                pltpu.VMEM((per, DETOUR, cols), bf16),
                pltpu.VMEM((per, acc_rows, cols), f32),
                pltpu.SMEM((offsets.shape[1], offsets.shape[0]), jnp.int32),
                pltpu.SMEM((fracs.shape[1], fracs.shape[0]), jnp.int32),
                pltpu.SMEM((depth + 2,), f32),
                pltpu.VMEM((round_up(PADY + frame + 8, 8), cols), f32),
                dma((2,)), dma((2,)), dma, dma((2,)), dma((2,)),
                dma((PIECES,)), dma((PIECES,)), dma, dma(((n // 2 - 1) * PIECES + 1,)), dma((2,)),
                signal, signal, signal,
            ],
            compiler_params=pltpu.CompilerParams(collective_id=0, has_side_effects=True),
        )(offsets.T, fracs.T, tiles)
        return jnp.transpose(joined, (1, 0, 2))

    in_specs = (P(("slab", "tile"), None, None, None), P(), P())
    out_specs = P(("slab", "tile"), None, None)
    return jax.shard_map(shards, mesh=mesh, in_specs=in_specs, out_specs=out_specs, check_vma=False)
```

```python
import functools

import jax
import jax.numpy as jnp
import numpy as np
from jax import lax
from jax.experimental import pallas as pl
from jax.experimental.pallas import tpu as pltpu
from jax.sharding import PartitionSpec as P

GROUPZ = 16
MARGIN = 2
JIT = 1
STEPY = 230
JITY = 4
RY = 26
RX = 16
QUANT = 16
EDGE = MARGIN + JIT
PADY = 32
PIECES = 3

weight_floor = 0.05
MESH = pl.DeviceIdType.MESH


def ramp(length, ramp_width):
    position = np.arange(length, dtype=np.float64)
    rising = 0.5 - 0.5 * np.cos(np.pi * (position + 1.0) / (ramp_width + 1.0))
    rising = np.where(position < ramp_width, rising, 1.0)
    return np.minimum(rising, rising[::-1])


def ramp_at(position, length, ramp_width):
    inward = jnp.minimum(position, length - 1 - position)
    t = (inward + 1).astype(jnp.float32) * float(np.pi / 2 / (ramp_width + 1.0))
    square = t * t
    sine = jnp.full(t.shape, 1.0 / 6227020800.0, jnp.float32)
    for term in (-39916800.0, 362880.0, -5040.0, 120.0, -6.0, 1.0):
        sine = sine * square + 1.0 / term
    sine = sine * t
    value = jnp.where(inward < ramp_width, sine * sine, 1.0)
    return jnp.where(inward < 0, 0.0, value)


def round_up(value, step):
    return -(-value // step) * step


SOLO = STEPY // 8 * 8
MAIN = SOLO - 8
FIRST = MAIN // 24 * 8
DETOUR = 24


def pair_start(pair):
    if isinstance(pair, int):
        return max(2 * pair * STEPY - JITY, 0) // 8 * 8
    return jnp.maximum(2 * pair * STEPY - JITY, 0) // 8 * 8


def frame_start(rank):
    return pair_start(rank // 2) + SOLO * (rank % 2)


def kernel(
    groups, n, per, depth, tile_rows, shared, trim, stride,
    offs_ref, fracs_ref, tile_ref, out_ref,
    lead, raw, coef, coef_lead, wa, wb, blend, own_sh, give, got,
    edge_send, far_recv, near_recv, recv, relay, rec,
    offs, fracs, rampz, table,
    small_sem, load_sem, give_sem, got_sem, es_sem, far_sem, near_sem, s_sem, r_sem, relay_sem,
    above_sem, below_sem, clear_sem,
):
    g = lax.axis_index("slab")
    r = lax.axis_index("tile")
    me = g * n + r
    chip = r // 2
    pairs = n // 2
    low = r < n // 2
    high = jnp.logical_not(low)
    odd = r % 2 == 1
    partner = r + 1 - 2 * (r % 2)
    cols = raw.shape[2]
    last = n - 1
    frame = SOLO + 2 * shared
    half = SOLO + shared
    rows = out_ref.shape[0]
    cut = [0, FIRST, MAIN, half]
    direct = pairs == 2

    barrier = pltpu.get_barrier_semaphore()
    has_below = g > 0
    has_above = g < groups - 1
    for i in range(1, n):
        pl.semaphore_signal(
            barrier, inc=1, device_id=(g, lax.rem(r + i, n)), device_id_type=MESH
        )

    @pl.when(has_above)
    def _():
        pl.semaphore_signal(barrier, inc=1, device_id=(g + 1, r), device_id_type=MESH)

    @pl.when(jnp.logical_and(has_below, high))
    def _():
        pl.semaphore_signal(barrier, inc=1, device_id=(g - 1, r), device_id_type=MESH)

    routes = sorted({stride, 1}, reverse=True)
    detour = direct and groups > stride
    carries = functools.reduce(jnp.logical_or, [g == at for at in routes])
    relays = jnp.logical_and(carries, odd)
    source_rank = n // 2
    source = jnp.logical_and(g == 0, r == source_rank) if detour else False
    if detour:
        @pl.when(jnp.logical_and(relays, high))
        def _():
            pl.semaphore_signal(barrier, inc=1, device_id=(0, source_rank), device_id_type=MESH)

    greeted = n - 1 + jnp.where(has_below, 1, 0) + jnp.where(jnp.logical_and(has_above, high), 1, 0)
    if detour:
        greeted = greeted + jnp.where(source, len(routes), 0)
    far_side = jnp.where(low, 1, 0)
    near_side = 1 - far_side

    def sends_to(side):
        return jnp.where(side == 0, g < groups - 1, g > 0)

    def gets_from(side):
        return jnp.where(side == 0, g > 0, g < groups - 1)

    gets_far = gets_from(far_side)
    gets_near = gets_from(near_side)

    def mirrored(owner):
        return jnp.where(low, owner, last - owner)

    edge_planes = list(range(EDGE)) + list(range(GROUPZ - EDGE, GROUPZ))
    bound = sorted({q // per for q in edge_planes}, reverse=True)
    free = [o for o in range(last, -1, -1) if o not in bound]
    far_free = [o for o in free if o >= n // 2]
    far_bound = [o for o in bound if o >= n // 2]
    near_free = [o for o in free if o < n // 2]
    near_bound = [o for o in bound if o < n // 2]
    far_list = far_free + far_bound
    near_list = near_free + near_bound
    near_owner = mirrored(near_bound[-1])
    takes_near = jnp.logical_and(gets_near, r == near_owner)

    def far_owner(i):
        return mirrored(jnp.where(gets_far, far_list[i], far_list[-1 - i]))

    offs_load = pltpu.make_async_copy(offs_ref, offs, small_sem.at[0])
    fracs_load = pltpu.make_async_copy(fracs_ref, fracs, small_sem.at[1])
    first_owner = far_owner(0)
    head_planes = lead.shape[0]
    head_start = jnp.minimum(first_owner * per + MARGIN - JIT, depth - head_planes)
    lead_rows = lead.shape[1]
    lead_start = jnp.where(odd, max(2 * shared - (frame - tile_rows), 0) // 8 * 8, 0)
    head_part = pl.ds(head_start, head_planes)
    pltpu.make_async_copy(
        tile_ref.at[0, head_part, pl.ds(pl.multiple_of(lead_start, 8), lead_rows)],
        lead, load_sem.at[0],
    ).start()
    offs_load.start()
    fracs_load.start()
    pltpu.make_async_copy(tile_ref.at[0], raw.at[pl.ds(0, depth)], load_sem.at[1]).start()

    def await_piece(part, sem):
        pltpu.make_async_copy(part, part, sem).wait()

    raw[depth] = jnp.zeros(raw.shape[1:], raw.dtype)

    for at, value in enumerate([0.0, *ramp(depth, 2 * MARGIN), 0.0]):
        rampz[at] = jnp.float32(value)
    row = lax.broadcasted_iota(jnp.int32, table.shape, 0) - PADY
    col = lax.broadcasted_iota(jnp.int32, (8, cols), 1)
    table[...] = ramp_at(row, tile_rows, RY) * ramp_at(col, cols, RX)[:1]

    def rampz_at(z):
        return rampz[jnp.clip(z, -1, depth) + 1]

    offs_load.wait()
    fracs_load.wait()
    corner = offs[0, me]
    shift = jnp.clip(offs[1, me] - frame_start(r), 0, frame - tile_rows)
    base = g * GROUPZ - corner
    fz = fracs[0, me].astype(jnp.float32) / QUANT
    fy = fracs[1, me].astype(jnp.float32) / QUANT
    fx = fracs[2, me].astype(jnp.float32) / QUANT
    start_solo = jnp.where(odd, 2 * shared, 0)
    start_own = jnp.where(odd, shared, SOLO)
    start_give = jnp.where(odd, 0, half)
    parts = [
        (0, MAIN, start_solo), (MAIN, shared, start_own),
        (MAIN + shared, SOLO - MAIN, start_solo + MAIN), (half, shared, start_give),
    ]
    def lerps(target, at, count, start, first_col, width):
        row = lax.broadcasted_iota(jnp.int32, (count, width), 0)
        col = lax.broadcasted_iota(jnp.int32, (count, width), 1)
        behind = col - row + (shift - start + first_col)
        lerp_y = jnp.where(behind == 0, 1.0 - fy, jnp.where(behind == 1, fy, 0.0))
        target[at : at + count, :width] = ((1.0 - fz) * lerp_y).astype(jnp.bfloat16)
        target[at : at + count, width:] = (fz * lerp_y).astype(jnp.bfloat16)

    def weights(at, count, start):
        weight = table[pl.ds(PADY + start - shift, count), :]
        lane = lax.broadcasted_iota(jnp.int32, (count, cols), 1)
        wa[at : at + count] = weight * (1.0 - fx)
        wb[at : at + count] = jnp.where(lane < cols - 1, weight * fx, 0.0)

    def planes(store, source, source_start, limit, factors, first, count, lo, hi):
        at = [jnp.clip(first + j, 0, depth - 1) - source_start for j in range(count)]
        at = [jnp.clip(z, 0, limit) for z in at]
        top = jnp.concatenate([source[z] for z in at], axis=1)
        bottom = jnp.concatenate([source[z + 1] for z in at], axis=1)
        mixed = jnp.dot(
            factors[lo:hi], jnp.concatenate([top, bottom], axis=0),
            preferred_element_type=jnp.float32,
        )
        for j in range(count):
            part = mixed[:, j * cols : (j + 1) * cols]
            value = part * wa[lo:hi] + pltpu.roll(part, cols - 1, 1) * wb[lo:hi]
            store(j, value * rampz_at(first + j))

    def blend_rows(target, at, start, slot, where_from, first, count, lo, hi):
        def store(j, value):
            top = min(hi, MAIN)
            if lo < top:
                target[at, start + j, lo:top] = value[: top - lo].astype(jnp.bfloat16)
            if hi > MAIN:
                own_sh[slot + j] = value[MAIN - lo : MAIN + shared - lo]
                target[at, start + j, MAIN + shared : half] = value[
                    MAIN + shared - lo : half - lo
                ].astype(jnp.bfloat16)
                give[slot + j] = value[half - lo :].astype(jnp.bfloat16)

        planes(store, *where_from, first, count, lo, hi)

    whole = (raw, 0, depth - 1, coef)

    def blend_owner(owner, lo=0, hi=frame, where_from=whole, j=0, count=per):
        first = owner * per + j
        blend_rows(blend, owner, j, first, where_from, base + first, count, lo, hi)

    def edge_slot(side):
        return GROUPZ + side * EDGE

    def blend_edge(side):
        first = base + jnp.where(side == 0, GROUPZ, -EDGE)
        blend_rows(edge_send, side, 0, edge_slot(side), whole, first, EDGE, 0, frame)

    def swap_copy(slot, count, at):
        part = pl.ds(slot, count)
        return pltpu.make_async_remote_copy(
            src_ref=give.at[part], dst_ref=got.at[part],
            send_sem=give_sem, recv_sem=got_sem.at[at],
            device_id=(g, partner), device_id_type=MESH,
        )

    def joined_rows(slot):
        return (own_sh[slot] + got[slot].astype(jnp.float32)).astype(jnp.bfloat16)

    def join_owner(owner):
        for j in range(per):
            blend[owner, j, MAIN : MAIN + shared] = joined_rows(owner * per + j)

    def join_edge(side):
        for p in range(EDGE):
            edge_send[side, p, MAIN : MAIN + shared] = joined_rows(edge_slot(side) + p)

    def rows_of(i):
        return pl.ds(cut[i], cut[i + 1] - cut[i])

    def came(source_chip, i):
        away = lax.rem(source_chip - chip + pairs, pairs)
        return jnp.where(away == 0, 0, 1 + (away - 1) * PIECES + i)

    def send(owner, i, when=True, start=0, count=per, less=0):
        there = owner // 2
        away = lax.rem(chip - there + pairs, pairs)
        at = jnp.where(away == 0, 0, 1 + (away - 1) * PIECES + i)
        shapes = [(when, less)] if i < PIECES - 1 else [
            (jnp.logical_and(when, jnp.logical_not(odd)), 0), (jnp.logical_and(when, odd), trim)
        ]
        for condition, fewer in shapes:
            part = pl.ds(cut[i], cut[i + 1] - cut[i] - fewer)
            held = blend.at[owner, pl.ds(start, count), part]
            target = recv.at[r, pl.ds(start, count), part]

            @pl.when(jnp.logical_and(condition, owner != r))
            def _():
                pltpu.make_async_remote_copy(
                    src_ref=held, dst_ref=target, send_sem=s_sem, recv_sem=r_sem.at[at],
                    device_id=(g, owner), device_id_type=MESH,
                ).start()

            @pl.when(jnp.logical_and(condition, owner == r))
            def _():
                pltpu.make_async_copy(held, target, r_sem.at[at]).start()

    def inner(o):
        taking = sum(o * per + j >= GROUPZ - EDGE for j in range(per))
        free_count = per - taking
        return jnp.where(low, 0, taking), free_count, jnp.where(low, free_count, 0), taking

    def await_far(source_chip, i):
        less = trim // 2 if i == PIECES - 1 else 0
        part = recv.at[pl.ds(2 * source_chip, 2), :, pl.ds(cut[i], cut[i + 1] - cut[i] - less)]
        pltpu.make_async_copy(part, part, r_sem.at[came(source_chip, i)]).wait()

    def await_own():
        part = recv.at[pl.ds(2 * chip, 2), :, pl.ds(0, half - trim // 2)]
        pltpu.make_async_copy(part, part, r_sem.at[0]).wait()

    def send_far(i):
        @pl.when(sends_to(far_side))
        def _():
            pltpu.make_async_remote_copy(
                src_ref=edge_send.at[far_side, :, rows_of(i)], dst_ref=far_recv.at[:, rows_of(i)],
                send_sem=es_sem.at[0], recv_sem=far_sem.at[i],
                device_id=(g + 1 - 2 * far_side, r), device_id_type=MESH,
            ).start()

    near_slot = r % 2 if direct else 0
    near_target = near_owner if direct else r

    def send_near(i):
        @pl.when(sends_to(near_side))
        def _():
            pltpu.make_async_remote_copy(
                src_ref=edge_send.at[near_side, :, rows_of(i)],
                dst_ref=near_recv.at[near_slot, :, rows_of(i)],
                send_sem=es_sem.at[1], recv_sem=near_sem.at[i],
                device_id=(g + 1 - 2 * near_side, near_target), device_id_type=MESH,
            ).start()

    def add_edge(side, source, i):
        for p in range(EDGE):
            q = p + jnp.where(side == 0, 0, GROUPZ - EDGE)
            owner, j = q // per, q % per
            a, b = cut[i], cut[i + 1]
            blend[owner, j, a:b] = (
                blend[owner, j, a:b].astype(jnp.float32) + source[p, a:b].astype(jnp.float32)
            ).astype(jnp.bfloat16)

    lerps(coef_lead, 0, cut[1], start_solo, lead_start, lead_rows)
    weights(0, cut[1], start_solo)
    for at, count, start in parts:
        lerps(coef, at, count, start, 0, tile_rows)
    weights(cut[1], MAIN - cut[1], start_solo + cut[1])
    for at, count, start in parts[1:]:
        weights(at, count, start)
    await_piece(lead, load_sem.at[0])
    not_far = jnp.logical_not(gets_far)
    first_when = True if far_free else not_far
    held_back = False
    if direct:
        holds = jnp.logical_or(odd, carries) if detour else odd
        held_back = jnp.logical_and(jnp.logical_and(high, gets_far), holds)
    blend_owner(first_owner, 0, cut[1], (lead, head_start, head_planes - 2, coef_lead))
    pl.semaphore_wait(barrier, greeted)
    send(first_owner, 0, first_when)

    @pl.when(jnp.logical_and(has_below, low))
    def _():
        pl.semaphore_signal(above_sem, inc=1, device_id=(g - 1, r), device_id_type=MESH)

    if direct:
        @pl.when(jnp.logical_and(has_above, high))
        def _():
            pl.semaphore_signal(below_sem, inc=1, device_id=(g + 1, r), device_id_type=MESH)

    await_piece(raw.at[pl.ds(0, depth)], load_sem.at[1])
    blend_owner(first_owner, cut[1], frame)
    if detour:
        @pl.when(source)
        def _():
            for i, at in enumerate(routes):
                part = pl.ds(MAIN - (i + 1) * DETOUR, DETOUR)
                pltpu.make_async_remote_copy(
                    src_ref=blend.at[first_owner, :, part], dst_ref=relay,
                    send_sem=s_sem, recv_sem=relay_sem.at[0],
                    device_id=(at, source_rank + 1), device_id_type=MESH,
                ).start()

        send(first_owner, 1, source, less=len(routes) * DETOUR)
        send(first_owner, 1, jnp.logical_not(source))
    else:
        for i in range(1, PIECES - 1):
            send(first_owner, i, first_when)
    swap_copy(first_owner * per, per, 0).start()

    blend_edge(far_side)
    swap_copy(edge_slot(far_side), EDGE, 0).start()
    for i in range(PIECES - 1):
        send_far(i)

    for at in range(1, len(far_list)):
        owner = far_owner(at)
        blend_owner(owner)
        swap_copy(owner * per, per, 1).start()

    await_piece(got.at[pl.ds(0, per + EDGE)], got_sem.at[0])
    join_owner(first_owner)
    send(first_owner, PIECES - 1, jnp.logical_and(first_when, jnp.logical_not(held_back)))
    join_edge(far_side)
    send_far(PIECES - 1)
    for at in range(1, len(far_list)):
        owner = far_owner(at)
        for i in range(PIECES - 1):
            if at < len(far_free):
                send(owner, i)
            else:
                send(owner, i, not_far)
                start, count, _, _ = inner(far_list[at])
                if count:
                    send(owner, i, gets_far, start, count)

    for o in near_list:
        owner = mirrored(o)
        blend_owner(owner)
        swap_copy(owner * per, per, 1).start()
    blend_edge(near_side)
    swap_copy(edge_slot(near_side), EDGE, 1).start()
    if direct:
        @pl.when(jnp.logical_not(takes_near))
        def _():
            near_recv[...] = jnp.zeros_like(near_recv)

    if detour:
        @pl.when(jnp.logical_and(relays, high))
        def _():
            await_piece(relay, relay_sem.at[0])
            pltpu.make_async_remote_copy(
                src_ref=relay, dst_ref=relay, send_sem=relay_sem.at[1], recv_sem=relay_sem.at[0],
                device_id=(g, r - n // 2), device_id_type=MESH,
            ).start()

    rec[...] = jnp.zeros_like(rec)
    for k in range(n):
        s = frame_start(k)
        totals = [0.0] * per
        for delta in (-1, 0, 1):
            group = jnp.clip(g + delta, 0, groups - 1)
            exists = jnp.where(group == g + delta, 1.0, 0.0)
            z0 = offs[0, group * n + k]
            ahead = jnp.clip(offs[1, group * n + k] - s, 0, frame - tile_rows)
            wy = table[pl.ds(PADY - ahead, frame), :]
            for j in range(per):
                z = g * GROUPZ + r * per + j - z0
                totals[j] = totals[j] + wy * (rampz_at(z) * exists)
        for j in range(per):
            rec[j, s : s + frame] = rec[j, s : s + frame] + totals[j]
    rec[...] = 1.0 / jnp.maximum(rec[...], weight_floor)

    await_piece(got.at[pl.ds(0, GROUPZ - per + EDGE)], got_sem.at[1])
    for at in range(1, len(far_list)):
        owner = far_owner(at)
        join_owner(owner)
        if at < len(far_free):
            send(owner, PIECES - 1)
        else:
            send(owner, PIECES - 1, not_far)
            start, count, _, _ = inner(far_list[at])
            if count:
                send(owner, PIECES - 1, gets_far, start, count)
    for o in near_list:
        owner = mirrored(o)
        join_owner(owner)
        for i in range(PIECES):
            send(owner, i, True if direct or o in near_free else jnp.logical_not(gets_near))
    join_edge(near_side)

    @pl.when(jnp.logical_and(has_above, low))
    def _():
        pl.semaphore_wait(above_sem, 1)

    if direct:
        @pl.when(jnp.logical_and(has_below, high))
        def _():
            pl.semaphore_wait(below_sem, 1)

    for i in range(PIECES):
        @pl.when(gets_far)
        def _():
            await_piece(far_recv.at[:, rows_of(i)], far_sem.at[i])
            add_edge(far_side, far_recv, i)
            for o in far_bound:
                _, _, start, count = inner(o)
                send(mirrored(o), i, True, start, count)

        if i == 0:
            @pl.when(sends_to(far_side))
            def _():
                await_piece(far_recv, es_sem.at[0])
                pl.semaphore_signal(
                    clear_sem, inc=1, device_id=(g, partner), device_id_type=MESH
                )
                pl.semaphore_wait(clear_sem, 1)

        send_near(i)

    if direct:
        send(first_owner, PIECES - 1, held_back)
    else:
        @pl.when(gets_near)
        def _():
            for i in range(PIECES):
                await_piece(near_recv.at[0, :, rows_of(i)], near_sem.at[i])
                add_edge(near_side, near_recv.at[0], i)
                for o in near_bound:
                    send(mirrored(o), i)

    if detour:
        @pl.when(jnp.logical_and(relays, low))
        def _():
            await_piece(relay, relay_sem.at[0])
            for i, at in enumerate(routes):
                @pl.when(g == at)
                def _():
                    part = pl.ds(MAIN - (i + 1) * DETOUR, DETOUR)
                    pltpu.make_async_remote_copy(
                        src_ref=relay, dst_ref=recv.at[source_rank, :, part],
                        send_sem=relay_sem.at[1], recv_sem=r_sem.at[2],
                        device_id=(0, 0), device_id_type=MESH,
                    ).start()

    def spans(k, i):
        solo_at = pair_start(k // 2) + (k % 2) * (SOLO + 2 * shared)
        shared_at = pair_start(k // 2) + SOLO + (k % 2) * shared
        if i < PIECES - 1:
            return [(solo_at + cut[i], solo_at + cut[i + 1], solo_at)]
        end = solo_at + SOLO - (k % 2) * trim
        return [
            (shared_at, shared_at + shared, shared_at - MAIN),
            (solo_at + MAIN, end, solo_at - shared),
        ]

    segments = [(k, i, *span) for k in range(n) for i in range(PIECES) for span in spans(k, i)]
    marks = sorted({min(end, rows) for item in segments for end in item[2:4]})
    intervals = [
        (a, b, [(k, i, at) for k, i, lo, hi, at in segments if lo < b and hi > a])
        for a, b in zip(marks[:-1], marks[1:])
    ]

    def finish(a, b, pieces, own=None, first=0):
        total = 0.0
        for k, i, at in pieces:
            total = total + recv[k, :, a - at : b - at].astype(jnp.float32)
            if k // 2 == own:
                edge = near_recv[k % 2, :, a - at : b - at].astype(jnp.float32)
                blank = [jnp.zeros((count, b - a, cols), jnp.float32) for count in (first, per - EDGE - first)]
                kept = [part for part in (blank[0], edge, blank[1]) if part.shape[0]]
                total = total + jnp.concatenate(kept, axis=0)
        value = (total * rec[:, a:b]).astype(jnp.bfloat16)
        out_ref[a:b] = jnp.swapaxes(value, 0, 1)

    if direct:
        for own in range(2):
            @pl.when(chip == own)
            def _():
                left = list(intervals)
                here = set()
                await_own()
                for i in range(PIECES):
                    @pl.when(takes_near)
                    def _():
                        await_piece(near_recv.at[:, :, rows_of(i)], near_sem.at[i])

                    for source in (own, 1 - own):
                        if source != own:
                            await_far(source, i)
                        here |= {(2 * source, i), (2 * source + 1, i)}
                        for item in list(left):
                            if all((k, j) in here for k, j, _ in item[2]):
                                left.remove(item)
                                finish(*item, own, 0 if own == 0 else per - EDGE)
    else:
        await_own()
        for away in range(1, pairs):
            for i in range(PIECES):
                await_far(lax.rem(chip + away, pairs), i)
        for item in intervals:
            finish(*item)

    if detour:
        @pl.when(relays)
        def _():
            await_piece(relay, relay_sem.at[1])

    await_piece(give, give_sem)
    for is_odd in (False, True):
        @pl.when(odd == is_odd)
        def _():
            await_piece(blend.at[pl.ds(0, n - 1), :, pl.ds(0, half - is_odd * trim)], s_sem)

    @pl.when(sends_to(near_side))
    def _():
        await_piece(far_recv, es_sem.at[1])


def solution(mesh):
    groups, n = mesh.shape["slab"], mesh.shape["tile"]
    stride = len({getattr(d, "coords", (i % 2,))[0] for i, d in enumerate(mesh.devices.flat)})

    def shards(tiles, offsets, fracs):
        _, depth, tile_rows, cols = tiles.shape
        per = GROUPZ // n
        rows = (n - 1) * STEPY + tile_rows
        reach = max(
            min(k * STEPY + JITY, rows - tile_rows) + tile_rows - frame_start(k) for k in range(n)
        )
        shared = round_up(max(reach - SOLO, 16), 16) // 2
        frame, half = SOLO + 2 * shared, SOLO + shared
        trim = min(frame - reach, SOLO - MAIN - 4) // 4 * 4
        acc_rows = round_up(max(rows, frame_start(n - 1) + frame), 16)
        head = per + 2 * JIT + 1
        lead = round_up(FIRST + frame - tile_rows + 8, 16)
        bf16, f32 = jnp.bfloat16, jnp.float32
        dma, signal = pltpu.SemaphoreType.DMA, pltpu.SemaphoreType.REGULAR
        slots = GROUPZ + 2 * EDGE
        joined = pl.pallas_call(
            functools.partial(
                kernel, groups, n, per, depth, tile_rows, shared, trim, stride
            ),
            out_shape=pltpu.VMEM((rows, per, cols), bf16),
            in_specs=[pl.BlockSpec(memory_space=pl.ANY)] * 3,
            out_specs=pl.BlockSpec(memory_space=pltpu.VMEM),
            scratch_shapes=[
                pltpu.VMEM((head, lead, cols), bf16),
                pltpu.VMEM((depth + 1, tile_rows, cols), bf16),
                pltpu.VMEM((frame, 2 * tile_rows), bf16),
                pltpu.VMEM((SOLO, 2 * lead), bf16),
                pltpu.VMEM((frame, cols), f32),
                pltpu.VMEM((frame, cols), f32),
                pltpu.VMEM((n, per, half, cols), bf16),
                pltpu.VMEM((slots, shared, cols), f32),
                pltpu.VMEM((slots, shared, cols), bf16),
                pltpu.VMEM((slots, shared, cols), bf16),
                pltpu.VMEM((2, EDGE, half, cols), bf16),
                pltpu.VMEM((EDGE, half, cols), bf16),
                pltpu.VMEM((2, EDGE, half, cols), bf16),
                pltpu.VMEM((n, per, half, cols), bf16),
                pltpu.VMEM((per, DETOUR, cols), bf16),
                pltpu.VMEM((per, acc_rows, cols), f32),
                pltpu.SMEM((offsets.shape[1], offsets.shape[0]), jnp.int32),
                pltpu.SMEM((fracs.shape[1], fracs.shape[0]), jnp.int32),
                pltpu.SMEM((depth + 2,), f32),
                pltpu.VMEM((round_up(PADY + frame + 8, 8), cols), f32),
                dma((2,)), dma((2,)), dma, dma((2,)), dma((2,)),
                dma((PIECES,)), dma((PIECES,)), dma, dma(((n // 2 - 1) * PIECES + 1,)), dma((2,)),
                signal, signal, signal,
            ],
            compiler_params=pltpu.CompilerParams(collective_id=0, has_side_effects=True),
        )(offsets.T, fracs.T, tiles)
        return jnp.transpose(joined, (1, 0, 2))

    in_specs = (P(("slab", "tile"), None, None, None), P(), P())
    out_specs = P(("slab", "tile"), None, None)
    return jax.shard_map(shards, mesh=mesh, in_specs=in_specs, out_specs=out_specs, check_vma=False)
```

```python
import functools

import jax
import jax.numpy as jnp
import numpy as np
from jax import lax
from jax.experimental import pallas as pl
from jax.experimental.pallas import tpu as pltpu
from jax.sharding import PartitionSpec as P

GROUPZ = 16
MARGIN = 2
JIT = 1
STEPY = 230
JITY = 4
RY = 26
RX = 16
QUANT = 16
EDGE = MARGIN + JIT
PADY = 32
PIECES = 3

weight_floor = 0.05
MESH = pl.DeviceIdType.MESH


def ramp(length, ramp_width):
    position = np.arange(length, dtype=np.float64)
    rising = 0.5 - 0.5 * np.cos(np.pi * (position + 1.0) / (ramp_width + 1.0))
    rising = np.where(position < ramp_width, rising, 1.0)
    return np.minimum(rising, rising[::-1])


def ramp_at(position, length, ramp_width):
    inward = jnp.minimum(position, length - 1 - position)
    t = (inward + 1).astype(jnp.float32) * float(np.pi / 2 / (ramp_width + 1.0))
    square = t * t
    sine = jnp.full(t.shape, 1.0 / 6227020800.0, jnp.float32)
    for term in (-39916800.0, 362880.0, -5040.0, 120.0, -6.0, 1.0):
        sine = sine * square + 1.0 / term
    sine = sine * t
    value = jnp.where(inward < ramp_width, sine * sine, 1.0)
    return jnp.where(inward < 0, 0.0, value)


def round_up(value, step):
    return -(-value // step) * step


SOLO = STEPY // 8 * 8
MAIN = SOLO - 8
FIRST = MAIN // 24 * 8
DETOUR = 24


def pair_start(pair):
    if isinstance(pair, int):
        return max(2 * pair * STEPY - JITY, 0) // 8 * 8
    return jnp.maximum(2 * pair * STEPY - JITY, 0) // 8 * 8


def frame_start(rank):
    return pair_start(rank // 2) + SOLO * (rank % 2)


def kernel(
    groups, n, per, depth, tile_rows, shared, trim, stride,
    offs_ref, fracs_ref, tile_ref, out_ref,
    lead, raw, coef, coef_lead, wa, wb, blend, own_sh, give, got,
    edge_send, far_recv, near_recv, recv, relay, rec,
    offs, fracs, rampz, table,
    small_sem, load_sem, give_sem, got_sem, es_sem, far_sem, near_sem, s_sem, r_sem, relay_sem,
    ready_sem,
):
    g = lax.axis_index("slab")
    r = lax.axis_index("tile")
    me = g * n + r
    chip = r // 2
    pairs = n // 2
    low = r < n // 2
    high = jnp.logical_not(low)
    odd = r % 2 == 1
    partner = r + 1 - 2 * (r % 2)
    cols = raw.shape[2]
    last = n - 1
    frame = SOLO + 2 * shared
    half = SOLO + shared
    rows = out_ref.shape[0]
    cut = [0, FIRST, MAIN, half]
    direct = pairs == 2

    barrier = pltpu.get_barrier_semaphore()
    has_below = g > 0
    has_above = g < groups - 1
    for i in range(1, n):
        pl.semaphore_signal(
            barrier, inc=1, device_id=(g, lax.rem(r + i, n)), device_id_type=MESH
        )

    @pl.when(has_above)
    def _():
        pl.semaphore_signal(barrier, inc=1, device_id=(g + 1, r), device_id_type=MESH)

    @pl.when(jnp.logical_and(has_below, high))
    def _():
        pl.semaphore_signal(barrier, inc=1, device_id=(g - 1, r), device_id_type=MESH)

    routes = sorted({stride, 1}, reverse=True)
    detour = direct and groups > stride
    carries = functools.reduce(jnp.logical_or, [g == at for at in routes])
    relays = jnp.logical_and(carries, odd)
    source_rank = n // 2
    source = jnp.logical_and(g == 0, r == source_rank) if detour else False
    if detour:
        @pl.when(jnp.logical_and(relays, high))
        def _():
            pl.semaphore_signal(barrier, inc=1, device_id=(0, source_rank), device_id_type=MESH)

    greeted = n - 1 + jnp.where(has_below, 1, 0) + jnp.where(jnp.logical_and(has_above, high), 1, 0)
    if detour:
        greeted = greeted + jnp.where(source, len(routes), 0)
    far_side = jnp.where(low, 1, 0)
    near_side = 1 - far_side

    def sends_to(side):
        return jnp.where(side == 0, g < groups - 1, g > 0)

    def gets_from(side):
        return jnp.where(side == 0, g > 0, g < groups - 1)

    gets_far = gets_from(far_side)
    gets_near = gets_from(near_side)

    def mirrored(owner):
        return jnp.where(low, owner, last - owner)

    edge_planes = list(range(EDGE)) + list(range(GROUPZ - EDGE, GROUPZ))
    bound = sorted({q // per for q in edge_planes}, reverse=True)
    free = [o for o in range(last, -1, -1) if o not in bound]
    far_free = [o for o in free if o >= n // 2]
    far_bound = [o for o in bound if o >= n // 2]
    near_free = [o for o in free if o < n // 2]
    near_bound = [o for o in bound if o < n // 2]
    far_list = far_free + far_bound
    near_list = near_free + near_bound
    near_owner = mirrored(near_bound[-1])
    takes_near = jnp.logical_and(gets_near, r == near_owner)

    def far_owner(i):
        return mirrored(jnp.where(gets_far, far_list[i], far_list[-1 - i]))

    offs_load = pltpu.make_async_copy(offs_ref, offs, small_sem.at[0])
    fracs_load = pltpu.make_async_copy(fracs_ref, fracs, small_sem.at[1])
    first_owner = far_owner(0)
    head_planes = lead.shape[0]
    head_start = jnp.minimum(first_owner * per + MARGIN - JIT, depth - head_planes)
    lead_rows = lead.shape[1]
    lead_start = jnp.where(odd, max(2 * shared - (frame - tile_rows), 0) // 8 * 8, 0)
    head_part = pl.ds(head_start, head_planes)
    pltpu.make_async_copy(
        tile_ref.at[0, head_part, pl.ds(pl.multiple_of(lead_start, 8), lead_rows)],
        lead, load_sem.at[0],
    ).start()
    offs_load.start()
    fracs_load.start()
    pltpu.make_async_copy(tile_ref.at[0], raw.at[pl.ds(0, depth)], load_sem.at[1]).start()

    def await_piece(part, sem):
        pltpu.make_async_copy(part, part, sem).wait()

    raw[depth] = jnp.zeros(raw.shape[1:], raw.dtype)

    for at, value in enumerate([0.0, *ramp(depth, 2 * MARGIN), 0.0]):
        rampz[at] = jnp.float32(value)
    row = lax.broadcasted_iota(jnp.int32, table.shape, 0) - PADY
    col = lax.broadcasted_iota(jnp.int32, (8, cols), 1)
    table[...] = ramp_at(row, tile_rows, RY) * ramp_at(col, cols, RX)[:1]

    def rampz_at(z):
        return rampz[jnp.clip(z, -1, depth) + 1]

    offs_load.wait()
    fracs_load.wait()
    corner = offs[0, me]
    shift = jnp.clip(offs[1, me] - frame_start(r), 0, frame - tile_rows)
    base = g * GROUPZ - corner
    fz = fracs[0, me].astype(jnp.float32) / QUANT
    fy = fracs[1, me].astype(jnp.float32) / QUANT
    fx = fracs[2, me].astype(jnp.float32) / QUANT
    start_solo = jnp.where(odd, 2 * shared, 0)
    start_own = jnp.where(odd, shared, SOLO)
    start_give = jnp.where(odd, 0, half)
    parts = [
        (0, MAIN, start_solo), (MAIN, shared, start_own),
        (MAIN + shared, SOLO - MAIN, start_solo + MAIN), (half, shared, start_give),
    ]
    def lerps(target, at, count, start, first_col, width):
        row = lax.broadcasted_iota(jnp.int32, (count, width), 0)
        col = lax.broadcasted_iota(jnp.int32, (count, width), 1)
        behind = col - row + (shift - start + first_col)
        lerp_y = jnp.where(behind == 0, 1.0 - fy, jnp.where(behind == 1, fy, 0.0))
        target[at : at + count, :width] = ((1.0 - fz) * lerp_y).astype(jnp.bfloat16)
        target[at : at + count, width:] = (fz * lerp_y).astype(jnp.bfloat16)

    def weights(at, count, start):
        weight = table[pl.ds(PADY + start - shift, count), :]
        lane = lax.broadcasted_iota(jnp.int32, (count, cols), 1)
        wa[at : at + count] = weight * (1.0 - fx)
        wb[at : at + count] = jnp.where(lane < cols - 1, weight * fx, 0.0)

    def planes(store, source, source_start, limit, factors, first, count, lo, hi):
        at = [jnp.clip(first + j, 0, depth - 1) - source_start for j in range(count)]
        at = [jnp.clip(z, 0, limit) for z in at]
        top = jnp.concatenate([source[z] for z in at], axis=1)
        bottom = jnp.concatenate([source[z + 1] for z in at], axis=1)
        mixed = jnp.dot(
            factors[lo:hi], jnp.concatenate([top, bottom], axis=0),
            preferred_element_type=jnp.float32,
        )
        for j in range(count):
            part = mixed[:, j * cols : (j + 1) * cols]
            value = part * wa[lo:hi] + pltpu.roll(part, cols - 1, 1) * wb[lo:hi]
            store(j, value * rampz_at(first + j))

    def blend_rows(target, at, start, slot, where_from, first, count, lo, hi):
        def store(j, value):
            top = min(hi, MAIN)
            if lo < top:
                target[at, start + j, lo:top] = value[: top - lo].astype(jnp.bfloat16)
            if hi > MAIN:
                own_sh[slot + j] = value[MAIN - lo : MAIN + shared - lo]
                target[at, start + j, MAIN + shared : half] = value[
                    MAIN + shared - lo : half - lo
                ].astype(jnp.bfloat16)
                give[slot + j] = value[half - lo :].astype(jnp.bfloat16)

        planes(store, *where_from, first, count, lo, hi)

    whole = (raw, 0, depth - 1, coef)

    def blend_owner(owner, lo=0, hi=frame, where_from=whole, j=0, count=per):
        first = owner * per + j
        blend_rows(blend, owner, j, first, where_from, base + first, count, lo, hi)

    def edge_slot(side):
        return GROUPZ + side * EDGE

    def blend_edge(side):
        first = base + jnp.where(side == 0, GROUPZ, -EDGE)
        blend_rows(edge_send, side, 0, edge_slot(side), whole, first, EDGE, 0, frame)

    def swap_copy(slot, count, at):
        part = pl.ds(slot, count)
        return pltpu.make_async_remote_copy(
            src_ref=give.at[part], dst_ref=got.at[part],
            send_sem=give_sem, recv_sem=got_sem.at[at],
            device_id=(g, partner), device_id_type=MESH,
        )

    def joined_rows(slot):
        return (own_sh[slot] + got[slot].astype(jnp.float32)).astype(jnp.bfloat16)

    def join_owner(owner):
        for j in range(per):
            blend[owner, j, MAIN : MAIN + shared] = joined_rows(owner * per + j)

    def join_edge(side):
        for p in range(EDGE):
            edge_send[side, p, MAIN : MAIN + shared] = joined_rows(edge_slot(side) + p)

    def rows_of(i):
        return pl.ds(cut[i], cut[i + 1] - cut[i])

    def came(source_chip, i):
        away = lax.rem(source_chip - chip + pairs, pairs)
        return jnp.where(away == 0, 0, 1 + (away - 1) * PIECES + i)

    def send(owner, i, when=True, start=0, count=per, less=0):
        there = owner // 2
        away = lax.rem(chip - there + pairs, pairs)
        at = jnp.where(away == 0, 0, 1 + (away - 1) * PIECES + i)
        shapes = [(when, less)] if i < PIECES - 1 else [
            (jnp.logical_and(when, jnp.logical_not(odd)), 0), (jnp.logical_and(when, odd), trim)
        ]
        for condition, fewer in shapes:
            part = pl.ds(cut[i], cut[i + 1] - cut[i] - fewer)
            held = blend.at[owner, pl.ds(start, count), part]
            target = recv.at[r, pl.ds(start, count), part]

            @pl.when(jnp.logical_and(condition, owner != r))
            def _():
                pltpu.make_async_remote_copy(
                    src_ref=held, dst_ref=target, send_sem=s_sem, recv_sem=r_sem.at[at],
                    device_id=(g, owner), device_id_type=MESH,
                ).start()

            @pl.when(jnp.logical_and(condition, owner == r))
            def _():
                pltpu.make_async_copy(held, target, r_sem.at[at]).start()

    def inner(o):
        taking = sum(o * per + j >= GROUPZ - EDGE for j in range(per))
        free_count = per - taking
        return jnp.where(low, 0, taking), free_count, jnp.where(low, free_count, 0), taking

    def await_far(source_chip, i):
        less = trim // 2 if i == PIECES - 1 else 0
        part = recv.at[pl.ds(2 * source_chip, 2), :, pl.ds(cut[i], cut[i + 1] - cut[i] - less)]
        pltpu.make_async_copy(part, part, r_sem.at[came(source_chip, i)]).wait()

    def await_own():
        part = recv.at[pl.ds(2 * chip, 2), :, pl.ds(0, half - trim // 2)]
        pltpu.make_async_copy(part, part, r_sem.at[0]).wait()

    def send_far(i):
        @pl.when(sends_to(far_side))
        def _():
            pltpu.make_async_remote_copy(
                src_ref=edge_send.at[far_side, :, rows_of(i)], dst_ref=far_recv.at[:, rows_of(i)],
                send_sem=es_sem.at[0], recv_sem=far_sem.at[i],
                device_id=(g + 1 - 2 * far_side, r), device_id_type=MESH,
            ).start()

    near_slot = r % 2 if direct else 0
    near_target = near_owner if direct else r

    def send_near(i):
        @pl.when(sends_to(near_side))
        def _():
            pltpu.make_async_remote_copy(
                src_ref=edge_send.at[near_side, :, rows_of(i)],
                dst_ref=near_recv.at[near_slot, :, rows_of(i)],
                send_sem=es_sem.at[1], recv_sem=near_sem.at[i],
                device_id=(g + 1 - 2 * near_side, near_target), device_id_type=MESH,
            ).start()

    def add_edge(side, source, i):
        for p in range(EDGE):
            q = p + jnp.where(side == 0, 0, GROUPZ - EDGE)
            owner, j = q // per, q % per
            a, b = cut[i], cut[i + 1]
            blend[owner, j, a:b] = (
                blend[owner, j, a:b].astype(jnp.float32) + source[p, a:b].astype(jnp.float32)
            ).astype(jnp.bfloat16)

    lerps(coef_lead, 0, cut[1], start_solo, lead_start, lead_rows)
    weights(0, cut[1], start_solo)
    for at, count, start in parts:
        lerps(coef, at, count, start, 0, tile_rows)
    weights(cut[1], MAIN - cut[1], start_solo + cut[1])
    for at, count, start in parts[1:]:
        weights(at, count, start)
    await_piece(lead, load_sem.at[0])
    not_far = jnp.logical_not(gets_far)
    first_when = True if far_free else not_far
    held_back = False
    if direct:
        holds = jnp.logical_or(odd, carries) if detour else odd
        held_back = jnp.logical_and(jnp.logical_and(high, gets_far), holds)
    blend_owner(first_owner, 0, cut[1], (lead, head_start, head_planes - 2, coef_lead))
    pl.semaphore_wait(barrier, greeted)
    send(first_owner, 0, first_when)

    @pl.when(jnp.logical_and(has_below, low))
    def _():
        pl.semaphore_signal(ready_sem, inc=1, device_id=(g - 1, r), device_id_type=MESH)

    if direct:
        @pl.when(jnp.logical_and(has_above, high))
        def _():
            pl.semaphore_signal(ready_sem, inc=1, device_id=(g + 1, r), device_id_type=MESH)

    await_piece(raw.at[pl.ds(0, depth)], load_sem.at[1])
    blend_owner(first_owner, cut[1], frame)
    if detour:
        @pl.when(source)
        def _():
            for i, at in enumerate(routes):
                part = pl.ds(MAIN - (i + 1) * DETOUR, DETOUR)
                pltpu.make_async_remote_copy(
                    src_ref=blend.at[first_owner, :, part], dst_ref=relay,
                    send_sem=s_sem, recv_sem=relay_sem.at[0],
                    device_id=(at, source_rank + 1), device_id_type=MESH,
                ).start()

        send(first_owner, 1, source, less=len(routes) * DETOUR)
        send(first_owner, 1, jnp.logical_not(source))
    else:
        for i in range(1, PIECES - 1):
            send(first_owner, i, first_when)
    swap_copy(first_owner * per, per, 0).start()

    blend_edge(far_side)
    swap_copy(edge_slot(far_side), EDGE, 0).start()
    for i in range(PIECES - 1):
        send_far(i)

    for at in range(1, len(far_list)):
        owner = far_owner(at)
        blend_owner(owner)
        swap_copy(owner * per, per, 1).start()

    await_piece(got.at[pl.ds(0, per + EDGE)], got_sem.at[0])
    join_owner(first_owner)
    send(first_owner, PIECES - 1, jnp.logical_and(first_when, jnp.logical_not(held_back)))
    join_edge(far_side)
    send_far(PIECES - 1)
    for at in range(1, len(far_list)):
        owner = far_owner(at)
        for i in range(PIECES - 1):
            if at < len(far_free):
                send(owner, i)
            else:
                send(owner, i, not_far)
                start, count, _, _ = inner(far_list[at])
                if count:
                    send(owner, i, gets_far, start, count)

    for o in near_list:
        owner = mirrored(o)
        blend_owner(owner)
        swap_copy(owner * per, per, 1).start()
    blend_edge(near_side)
    swap_copy(edge_slot(near_side), EDGE, 1).start()
    if direct:
        @pl.when(jnp.logical_not(takes_near))
        def _():
            near_recv[...] = jnp.zeros_like(near_recv)

    if detour:
        @pl.when(jnp.logical_and(relays, high))
        def _():
            await_piece(relay, relay_sem.at[0])
            pltpu.make_async_remote_copy(
                src_ref=relay, dst_ref=relay, send_sem=relay_sem.at[1], recv_sem=relay_sem.at[0],
                device_id=(g, r - n // 2), device_id_type=MESH,
            ).start()

    rec[...] = jnp.zeros_like(rec)
    for k in range(n):
        s = frame_start(k)
        totals = [0.0] * per
        for delta in (-1, 0, 1):
            group = jnp.clip(g + delta, 0, groups - 1)
            exists = jnp.where(group == g + delta, 1.0, 0.0)
            z0 = offs[0, group * n + k]
            ahead = jnp.clip(offs[1, group * n + k] - s, 0, frame - tile_rows)
            wy = table[pl.ds(PADY - ahead, frame), :]
            for j in range(per):
                z = g * GROUPZ + r * per + j - z0
                totals[j] = totals[j] + wy * (rampz_at(z) * exists)
        for j in range(per):
            rec[j, s : s + frame] = rec[j, s : s + frame] + totals[j]
    rec[...] = 1.0 / jnp.maximum(rec[...], weight_floor)

    await_piece(got.at[pl.ds(0, GROUPZ - per + EDGE)], got_sem.at[1])
    for at in range(1, len(far_list)):
        owner = far_owner(at)
        join_owner(owner)
        if at < len(far_free):
            send(owner, PIECES - 1)
        else:
            send(owner, PIECES - 1, not_far)
            start, count, _, _ = inner(far_list[at])
            if count:
                send(owner, PIECES - 1, gets_far, start, count)
    for o in near_list:
        owner = mirrored(o)
        join_owner(owner)
        for i in range(PIECES):
            send(owner, i, True if direct or o in near_free else jnp.logical_not(gets_near))
    join_edge(near_side)

    for i in range(PIECES):
        @pl.when(gets_far)
        def _():
            await_piece(far_recv.at[:, rows_of(i)], far_sem.at[i])
            add_edge(far_side, far_recv, i)
            for o in far_bound:
                _, _, start, count = inner(o)
                send(mirrored(o), i, True, start, count)

        if i == 0:
            @pl.when(sends_to(far_side))
            def _():
                await_piece(far_recv, es_sem.at[0])
                pl.semaphore_signal(
                    ready_sem, inc=1, device_id=(g, partner), device_id_type=MESH
                )

            ready = jnp.where(jnp.logical_and(has_above, low), 1, 0)
            if direct:
                ready = ready + jnp.where(jnp.logical_and(has_below, high), 1, 0)
            pl.semaphore_wait(ready_sem, ready + jnp.where(sends_to(far_side), 1, 0))

        send_near(i)

    if direct:
        send(first_owner, PIECES - 1, held_back)
    else:
        @pl.when(gets_near)
        def _():
            for i in range(PIECES):
                await_piece(near_recv.at[0, :, rows_of(i)], near_sem.at[i])
                add_edge(near_side, near_recv.at[0], i)
                for o in near_bound:
                    send(mirrored(o), i)

    if detour:
        @pl.when(jnp.logical_and(relays, low))
        def _():
            await_piece(relay, relay_sem.at[0])
            for i, at in enumerate(routes):
                @pl.when(g == at)
                def _():
                    part = pl.ds(MAIN - (i + 1) * DETOUR, DETOUR)
                    pltpu.make_async_remote_copy(
                        src_ref=relay, dst_ref=recv.at[source_rank, :, part],
                        send_sem=relay_sem.at[1], recv_sem=r_sem.at[2],
                        device_id=(0, 0), device_id_type=MESH,
                    ).start()

    def spans(k, i):
        solo_at = pair_start(k // 2) + (k % 2) * (SOLO + 2 * shared)
        shared_at = pair_start(k // 2) + SOLO + (k % 2) * shared
        if i < PIECES - 1:
            return [(solo_at + cut[i], solo_at + cut[i + 1], solo_at)]
        end = solo_at + SOLO - (k % 2) * trim
        return [
            (shared_at, shared_at + shared, shared_at - MAIN),
            (solo_at + MAIN, end, solo_at - shared),
        ]

    segments = [(k, i, *span) for k in range(n) for i in range(PIECES) for span in spans(k, i)]
    marks = sorted({min(end, rows) for item in segments for end in item[2:4]})
    intervals = [
        (a, b, [(k, i, at) for k, i, lo, hi, at in segments if lo < b and hi > a])
        for a, b in zip(marks[:-1], marks[1:])
    ]

    def finish(a, b, pieces, own=None, first=0):
        total = 0.0
        for k, i, at in pieces:
            total = total + recv[k, :, a - at : b - at].astype(jnp.float32)
            if k // 2 == own:
                edge = near_recv[k % 2, :, a - at : b - at].astype(jnp.float32)
                blank = [jnp.zeros((count, b - a, cols), jnp.float32) for count in (first, per - EDGE - first)]
                kept = [part for part in (blank[0], edge, blank[1]) if part.shape[0]]
                total = total + jnp.concatenate(kept, axis=0)
        value = (total * rec[:, a:b]).astype(jnp.bfloat16)
        out_ref[a:b] = jnp.swapaxes(value, 0, 1)

    if direct:
        for own in range(2):
            @pl.when(chip == own)
            def _():
                left = list(intervals)
                here = set()
                await_own()
                for i in range(PIECES):
                    @pl.when(takes_near)
                    def _():
                        await_piece(near_recv.at[:, :, rows_of(i)], near_sem.at[i])

                    for source in (own, 1 - own):
                        if source != own:
                            await_far(source, i)
                        here |= {(2 * source, i), (2 * source + 1, i)}
                        for item in list(left):
                            if all((k, j) in here for k, j, _ in item[2]):
                                left.remove(item)
                                finish(*item, own, 0 if own == 0 else per - EDGE)
    else:
        await_own()
        for away in range(1, pairs):
            for i in range(PIECES):
                await_far(lax.rem(chip + away, pairs), i)
        for item in intervals:
            finish(*item)

    if detour:
        @pl.when(relays)
        def _():
            await_piece(relay, relay_sem.at[1])

    await_piece(give, give_sem)
    for is_odd in (False, True):
        @pl.when(odd == is_odd)
        def _():
            await_piece(blend.at[pl.ds(0, n - 1), :, pl.ds(0, half - is_odd * trim)], s_sem)

    @pl.when(sends_to(near_side))
    def _():
        await_piece(far_recv, es_sem.at[1])


def solution(mesh):
    groups, n = mesh.shape["slab"], mesh.shape["tile"]
    stride = len({getattr(d, "coords", (i % 2,))[0] for i, d in enumerate(mesh.devices.flat)})

    def shards(tiles, offsets, fracs):
        _, depth, tile_rows, cols = tiles.shape
        per = GROUPZ // n
        rows = (n - 1) * STEPY + tile_rows
        reach = max(
            min(k * STEPY + JITY, rows - tile_rows) + tile_rows - frame_start(k) for k in range(n)
        )
        shared = round_up(max(reach - SOLO, 16), 16) // 2
        frame, half = SOLO + 2 * shared, SOLO + shared
        trim = min(frame - reach, SOLO - MAIN - 4) // 4 * 4
        acc_rows = round_up(max(rows, frame_start(n - 1) + frame), 16)
        head = per + 2 * JIT + 1
        lead = round_up(FIRST + frame - tile_rows + 8, 16)
        bf16, f32 = jnp.bfloat16, jnp.float32
        dma, signal = pltpu.SemaphoreType.DMA, pltpu.SemaphoreType.REGULAR
        slots = GROUPZ + 2 * EDGE
        joined = pl.pallas_call(
            functools.partial(
                kernel, groups, n, per, depth, tile_rows, shared, trim, stride
            ),
            out_shape=pltpu.VMEM((rows, per, cols), bf16),
            in_specs=[pl.BlockSpec(memory_space=pl.ANY)] * 3,
            out_specs=pl.BlockSpec(memory_space=pltpu.VMEM),
            scratch_shapes=[
                pltpu.VMEM((head, lead, cols), bf16),
                pltpu.VMEM((depth + 1, tile_rows, cols), bf16),
                pltpu.VMEM((frame, 2 * tile_rows), bf16),
                pltpu.VMEM((SOLO, 2 * lead), bf16),
                pltpu.VMEM((frame, cols), f32),
                pltpu.VMEM((frame, cols), f32),
                pltpu.VMEM((n, per, half, cols), bf16),
                pltpu.VMEM((slots, shared, cols), f32),
                pltpu.VMEM((slots, shared, cols), bf16),
                pltpu.VMEM((slots, shared, cols), bf16),
                pltpu.VMEM((2, EDGE, half, cols), bf16),
                pltpu.VMEM((EDGE, half, cols), bf16),
                pltpu.VMEM((2, EDGE, half, cols), bf16),
                pltpu.VMEM((n, per, half, cols), bf16),
                pltpu.VMEM((per, DETOUR, cols), bf16),
                pltpu.VMEM((per, acc_rows, cols), f32),
                pltpu.SMEM((offsets.shape[1], offsets.shape[0]), jnp.int32),
                pltpu.SMEM((fracs.shape[1], fracs.shape[0]), jnp.int32),
                pltpu.SMEM((depth + 2,), f32),
                pltpu.VMEM((round_up(PADY + frame + 8, 8), cols), f32),
                dma((2,)), dma((2,)), dma, dma((2,)), dma((2,)),
                dma((PIECES,)), dma((PIECES,)), dma, dma(((n // 2 - 1) * PIECES + 1,)), dma((2,)),
                signal,
            ],
            compiler_params=pltpu.CompilerParams(collective_id=0, has_side_effects=True),
        )(offsets.T, fracs.T, tiles)
        return jnp.transpose(joined, (1, 0, 2))

    in_specs = (P(("slab", "tile"), None, None, None), P(), P())
    out_specs = P(("slab", "tile"), None, None)
    return jax.shard_map(shards, mesh=mesh, in_specs=in_specs, out_specs=out_specs, check_vma=False)
```
